32 devices in a mesh: fsdp: 32 (over z, y, x, core).
Axes of the slice: x: 2, y: 2, z: 4, core: 2. Of those that a mesh axis runs over, the one named last changes fastest.
Arguments:
- act_in: bfloat16 [512, 196, 512], P('fsdp')
- labels: int32 [512], P('fsdp')
- layer_p: float32 [2, 2203648], P(None, 'fsdp')
- head_w: float32 [512, 1000], P('fsdp')
- small_p: float32 [4096], P('fsdp')
- layer_m: float32 [2, 2203648], P(None, 'fsdp')
- head_m: float32 [512, 1000], P('fsdp')
- small_m: float32 [4096], P('fsdp')
- layer_v: float32 [2, 2203648], P(None, 'fsdp')
- head_v: float32 [512, 1000], P('fsdp')
- small_v: float32 [4096], P('fsdp')
Outputs:
- output 1: float32 [], replicated
- output 2: float32 [2, 2203648], P(None, 'fsdp')
- output 3: float32 [512, 1000], P('fsdp')
- output 4: float32 [4096], P('fsdp')
- output 5: float32 [2, 2203648], P(None, 'fsdp')
- output 6: float32 [512, 1000], P('fsdp')
- output 7: float32 [4096], P('fsdp')
- output 8: float32 [2, 2203648], P(None, 'fsdp')
- output 9: float32 [512, 1000], P('fsdp')
- output 10: float32 [4096], P('fsdp')
All inputs are finite; a program needn't handle non-finite values.
Results may differ from the reference program's by a relative error of at most 0.00106585.
Values are sent between devices in bfloat16 or wider.
A program may use at most 1 GiB of HBM per device.

```python
import jax
import jax.numpy as jnp
from jax import lax

CHANNELS = 512
TOKENS = 196
TOKEN_HID = 256
CHAN_HID = 2048
CLASSES = 1000
BATCH_DEV = 16
FSDP_DEVS = 32
ADAM_STEP = 10

GLOBAL_BATCH = BATCH_DEV * FSDP_DEVS
PAD_UNIT = 128 * FSDP_DEVS
MAT_LEN = 2 * TOKENS * TOKEN_HID + 2 * CHANNELS * CHAN_HID
LAYER_LEN = MAT_LEN + 5 * CHANNELS + TOKEN_HID + TOKENS + CHAN_HID
LAYER_PAD = (LAYER_LEN + PAD_UNIT - 1) // PAD_UNIT * PAD_UNIT
SMALL_LEN = 2 * CHANNELS + CLASSES
SMALL_PAD = (SMALL_LEN + PAD_UNIT - 1) // PAD_UNIT * PAD_UNIT
PIECE_SIZES = (TOKENS * TOKEN_HID, TOKEN_HID * TOKENS, CHANNELS * CHAN_HID, CHAN_HID * CHANNELS, CHANNELS, CHANNELS, TOKEN_HID, TOKENS, CHANNELS, CHANNELS, CHAN_HID, CHANNELS)
LN_EPS = 1e-6
LEARN_RATE = 0.003
BETA_ONE = 0.9
BETA_TWO = 0.999
ADAM_EPS = 1e-8
WEIGHT_DECAY = 0.03


def unpack_layer(flat):
    pieces = []
    piece_start = 0
    for piece_len in PIECE_SIZES:
        pieces.append(flat[piece_start:piece_start + piece_len])
        piece_start = piece_start + piece_len
    w_tok1 = pieces[0].reshape(TOKENS, TOKEN_HID)
    w_tok2 = pieces[1].reshape(TOKEN_HID, TOKENS)
    w_ch1 = pieces[2].reshape(CHANNELS, CHAN_HID)
    w_ch2 = pieces[3].reshape(CHAN_HID, CHANNELS)
    return [w_tok1, w_tok2, w_ch1, w_ch2] + pieces[4:12]


def layer_norm(x_in, ln_gain, ln_shift):
    x_f = x_in.astype(jnp.float32)
    mean_val = jnp.mean(x_f, axis=-1, keepdims=True)
    var_val = jnp.mean(jnp.square(x_f - mean_val), axis=-1, keepdims=True)
    normed = (x_f - mean_val) * lax.rsqrt(var_val + LN_EPS)
    return (normed * ln_gain.astype(jnp.float32) + ln_shift.astype(jnp.float32)).astype(jnp.bfloat16)


def mixer_layer(x_in, flat):
    w_tok1, w_tok2, w_ch1, w_ch2, ln1_g, ln1_b, b_tok1, b_tok2, ln2_g, ln2_b, b_ch1, b_ch2 = unpack_layer(flat)
    normed = layer_norm(x_in, ln1_g, ln1_b)
    hid_tok = jnp.einsum('bsc,sj->bcj', normed.astype(jnp.float32), w_tok1.astype(jnp.float32)) + b_tok1.astype(jnp.float32)
    act_tok = jax.nn.gelu(hid_tok).astype(jnp.bfloat16)
    tok_out = jnp.einsum('bcj,js->bsc', act_tok.astype(jnp.float32), w_tok2.astype(jnp.float32)) + b_tok2.astype(jnp.float32)[:, None]
    after_tok = (x_in.astype(jnp.float32) + tok_out).astype(jnp.bfloat16)
    normed2 = layer_norm(after_tok, ln2_g, ln2_b)
    hid_ch = jnp.einsum('bsc,cd->bsd', normed2.astype(jnp.float32), w_ch1.astype(jnp.float32)) + b_ch1.astype(jnp.float32)
    act_ch = jax.nn.gelu(hid_ch).astype(jnp.bfloat16)
    ch_out = jnp.einsum('bsd,dc->bsc', act_ch.astype(jnp.float32), w_ch2.astype(jnp.float32)) + b_ch2.astype(jnp.float32)
    return (after_tok.astype(jnp.float32) + ch_out).astype(jnp.bfloat16)


def block_loss(layer_p, head_w, small_p, x_block, label_block):
    layers_bf = layer_p.astype(jnp.bfloat16)
    hidden = x_block
    for layer_idx in range(2):
        hidden = mixer_layer(hidden, layers_bf[layer_idx])
    small_bf = small_p.astype(jnp.bfloat16)
    lnf_g = small_bf[:CHANNELS]
    lnf_b = small_bf[CHANNELS:2 * CHANNELS]
    head_b = small_bf[2 * CHANNELS:2 * CHANNELS + CLASSES]
    normed = layer_norm(hidden, lnf_g, lnf_b)
    pooled = jnp.mean(normed.astype(jnp.float32), axis=1).astype(jnp.bfloat16)
    logits = jnp.dot(pooled, head_w.astype(jnp.bfloat16), preferred_element_type=jnp.float32) + head_b.astype(jnp.float32)
    log_norm = jax.nn.logsumexp(logits, axis=-1)
    is_label = jnp.arange(CLASSES)[None, :] == label_block[:, None]
    picked = jnp.sum(jnp.where(is_label, logits, 0.0), axis=-1)
    return jnp.sum(log_norm - picked) / GLOBAL_BATCH


def loss_and_grads(act_in, labels, layer_p, head_w, small_p):
    x_blocks = act_in.reshape(FSDP_DEVS, BATCH_DEV, TOKENS, CHANNELS)
    label_blocks = labels.reshape(FSDP_DEVS, BATCH_DEV)
    grad_fn = jax.value_and_grad(block_loss, argnums=(0, 1, 2))

    def scan_body(running, block_pair):
        loss_part, grad_parts = grad_fn(layer_p, head_w, small_p, block_pair[0], block_pair[1])
        return (running[0] + loss_part, running[1] + grad_parts[0], running[2] + grad_parts[1], running[3] + grad_parts[2]), None

    start_val = (jnp.zeros((), jnp.float32), jnp.zeros_like(layer_p), jnp.zeros_like(head_w), jnp.zeros_like(small_p))
    totals, _ = lax.scan(scan_body, start_val, (x_blocks, label_blocks))
    return totals


def adam_update(master, gradient, moment, second, decay_rate):
    moment_new = BETA_ONE * moment + (1.0 - BETA_ONE) * gradient
    second_new = BETA_TWO * second + (1.0 - BETA_TWO) * gradient * gradient
    m_hat = moment_new / (1.0 - BETA_ONE ** ADAM_STEP)
    v_hat = second_new / (1.0 - BETA_TWO ** ADAM_STEP)
    master_new = master - LEARN_RATE * (m_hat / (jnp.sqrt(v_hat) + ADAM_EPS) + decay_rate * master)
    return master_new, moment_new, second_new


def draw_layer(key):
    subkeys = jax.random.split(key, 13)
    normal = jax.random.normal
    pieces = [
        normal(subkeys[0], (TOKENS * TOKEN_HID,), jnp.float32) * TOKENS ** -0.5,
        normal(subkeys[1], (TOKEN_HID * TOKENS,), jnp.float32) * TOKEN_HID ** -0.5,
        normal(subkeys[2], (CHANNELS * CHAN_HID,), jnp.float32) * CHANNELS ** -0.5,
        normal(subkeys[3], (CHAN_HID * CHANNELS,), jnp.float32) * CHAN_HID ** -0.5,
        1.0 + 0.2 * normal(subkeys[4], (CHANNELS,), jnp.float32),
        0.2 * normal(subkeys[5], (CHANNELS,), jnp.float32),
        0.3 * normal(subkeys[6], (TOKEN_HID,), jnp.float32),
        0.3 * normal(subkeys[7], (TOKENS,), jnp.float32),
        1.0 + 0.2 * normal(subkeys[8], (CHANNELS,), jnp.float32),
        0.2 * normal(subkeys[9], (CHANNELS,), jnp.float32),
        0.3 * normal(subkeys[10], (CHAN_HID,), jnp.float32),
        0.3 * normal(subkeys[11], (CHANNELS,), jnp.float32),
        0.02 * normal(subkeys[12], (LAYER_PAD - LAYER_LEN,), jnp.float32),
    ]
    return jnp.concatenate(pieces)


def setup_inputs(seed: int = 0) -> dict:
    keys = jax.random.split(jax.random.key(seed), 12)
    normal = jax.random.normal
    base = normal(keys[0], (GLOBAL_BATCH, 1, CHANNELS), jnp.float32)
    noise = normal(keys[1], (GLOBAL_BATCH, TOKENS, CHANNELS), jnp.float32)
    act_in = (base + noise).astype(jnp.bfloat16)
    labels = jax.random.randint(keys[2], (GLOBAL_BATCH,), 0, CLASSES, jnp.int32)
    layer_p = jnp.stack([draw_layer(keys[3]), draw_layer(keys[4])])
    head_w = normal(keys[5], (CHANNELS, CLASSES), jnp.float32) * CHANNELS ** -0.5
    small_p = jnp.concatenate([
        2.0 + 0.3 * normal(keys[6], (CHANNELS,), jnp.float32),
        0.3 * normal(keys[7], (CHANNELS,), jnp.float32),
        normal(keys[8], (CLASSES,), jnp.float32),
        0.02 * normal(keys[9], (SMALL_PAD - SMALL_LEN,), jnp.float32),
    ])
    _, g_layer, g_head, g_small = loss_and_grads(act_in, labels, layer_p, head_w, small_p)
    layer_rms = jnp.sqrt(jnp.mean(jnp.square(g_layer), axis=1, keepdims=True))
    head_rms = jnp.sqrt(jnp.mean(jnp.square(g_head)))
    small_rms = jnp.sqrt(jnp.mean(jnp.square(g_small)))
    mkeys = jax.random.split(keys[10], 6)
    uniform = jax.random.uniform
    layer_m = 0.3 * layer_rms * normal(mkeys[0], layer_p.shape, jnp.float32)
    head_m = 0.3 * head_rms * normal(mkeys[1], head_w.shape, jnp.float32)
    small_m = 0.3 * small_rms * normal(mkeys[2], small_p.shape, jnp.float32)
    layer_v = 0.01 * jnp.square(layer_rms) * uniform(mkeys[3], layer_p.shape, jnp.float32, 0.5, 2.0)
    head_v = 0.01 * jnp.square(head_rms) * uniform(mkeys[4], head_w.shape, jnp.float32, 0.5, 2.0)
    small_v = 0.01 * jnp.square(small_rms) * uniform(mkeys[5], small_p.shape, jnp.float32, 0.5, 2.0)
    return {'act_in': act_in, 'labels': labels, 'layer_p': layer_p, 'head_w': head_w, 'small_p': small_p, 'layer_m': layer_m, 'head_m': head_m, 'small_m': small_m, 'layer_v': layer_v, 'head_v': head_v, 'small_v': small_v}


def reference(act_in, labels, layer_p, head_w, small_p, layer_m, head_m, small_m, layer_v, head_v, small_v):
    loss_value, g_layer, g_head, g_small = loss_and_grads(act_in, labels, layer_p, head_w, small_p)
    sq_total = jnp.sum(jnp.square(g_layer)) + jnp.sum(jnp.square(g_head)) + jnp.sum(jnp.square(g_small))
    clip_scale = 1.0 / jnp.maximum(1.0, jnp.sqrt(sq_total))
    layer_decay = jnp.where(jnp.arange(LAYER_PAD) < MAT_LEN, WEIGHT_DECAY, 0.0)[None, :]
    new_lp, new_lm, new_lv = adam_update(layer_p, g_layer * clip_scale, layer_m, layer_v, layer_decay)
    new_hw, new_hm, new_hv = adam_update(head_w, g_head * clip_scale, head_m, head_v, WEIGHT_DECAY)
    new_sp, new_sm, new_sv = adam_update(small_p, g_small * clip_scale, small_m, small_v, 0.0)
    return (loss_value, new_lp, new_hw, new_sp, new_lm, new_hm, new_sm, new_lv, new_hv, new_sv)
```

```python
import math
import jax
import jax.numpy as jnp
from jax import lax
from jax.experimental import pallas as pl
from jax.experimental.pallas import tpu as pltpu
from jax.sharding import PartitionSpec as P

LN_EPS = 1e-6
LEARN_RATE = 0.003
BETA_ONE = 0.9
BETA_TWO = 0.999
ADAM_EPS = 1e-8
WEIGHT_DECAY = 0.03
ADAM_STEP = 10
AXIS = 'fsdp'
GROUP = 32
ROWS = 8
LANES = 128
TILE = ROWS * LANES
HEAD_PAD = 1024

BIT_CORE, BIT_X, BIT_Y, BIT_Z0, BIT_Z1 = 0, 1, 2, 3, 4


def swap_bit(val, bit):
    return lax.ppermute(val, AXIS, [(dev, dev ^ (1 << bit)) for dev in range(GROUP)])


def my_bit(bit):
    return (lax.axis_index(AXIS) // (1 << bit)) % 2


def spread(block, bit, axis):
    other = swap_bit(block, bit)
    is_high = my_bit(bit) == 1
    return jnp.stack([jnp.where(is_high, other, block), jnp.where(is_high, block, other)], axis=axis)


def gather_colour(block, order):
    block = spread(block, BIT_Z0, 0)
    block = spread(block, BIT_Z1, 0)
    if order == 'yx':
        block = spread(block, BIT_Y, 2)
        block = spread(block, BIT_X, 3)
    else:
        block = spread(block, BIT_X, 2)
        block = spread(block, BIT_Y, 2)
    block = spread(block, BIT_CORE, 4)
    return block.reshape((GROUP,) + block.shape[5:])


def gather_tiles(tiles):
    half = tiles.shape[0] // 2
    part_a = gather_colour(tiles[:half], 'yx')
    part_b = gather_colour(tiles[half:], 'xy')
    return jnp.concatenate([part_a, part_b], axis=1)


def fold(block, bit, axis):
    low = lax.index_in_dim(block, 0, axis, keepdims=False)
    high = lax.index_in_dim(block, 1, axis, keepdims=False)
    is_high = my_bit(bit) == 1
    sent = jnp.where(is_high, low, high)
    kept = jnp.where(is_high, high, low)
    return kept + swap_bit(sent, bit)


def scatter_colour(block, order):
    block = block.reshape((2, 2, 2, 2, 2) + block.shape[1:])
    block = fold(block, BIT_CORE, 4)
    if order == 'xy':
        block = fold(block, BIT_X, 3)
        block = fold(block, BIT_Y, 2)
    else:
        block = fold(block, BIT_Y, 2)
        block = fold(block, BIT_X, 2)
    block = fold(block, BIT_Z1, 0)
    return fold(block, BIT_Z0, 0)


def scatter_tiles(blocks):
    half = blocks.shape[1] // 2
    part_a = scatter_colour(blocks[:, :half], 'xy')
    part_b = scatter_colour(blocks[:, half:], 'yx')
    return jnp.concatenate([part_a, part_b], axis=0)


def row_offset(share_rows):
    return (lax.axis_index(AXIS) * share_rows) % ROWS


def share_to_window(share):
    share_rows = share.shape[0] // LANES
    num_tiles = -(-(share_rows + ROWS - 2) // ROWS)
    window = jnp.zeros((num_tiles * ROWS, LANES), share.dtype)
    window = lax.dynamic_update_slice(window, share.reshape(share_rows, LANES), (row_offset(share_rows), 0))
    return window.reshape(num_tiles, ROWS, LANES)


def window_to_share(window, share_len):
    share_rows = share_len // LANES
    rows = window.reshape(-1, LANES)
    return lax.dynamic_slice(rows, (row_offset(share_rows), 0), (share_rows, LANES)).reshape(share_len)


def window_starts(share_rows):
    period = 4
    return [share_rows * dev // ROWS for dev in range(period)], share_rows * period // ROWS


def windows_to_tiles(windows, share_len):
    share_rows = share_len // LANES
    starts, period_tiles = window_starts(share_rows)
    num_tiles = windows.shape[1]
    grouped = windows.reshape((GROUP // 4, 4) + windows.shape[1:])
    pieces = []
    fresh = 0
    for dev in range(4):
        end = starts[dev] + num_tiles
        shared_end = dev < 3 and starts[dev + 1] < end
        last = num_tiles - 1 if shared_end else num_tiles
        pieces.append(grouped[:, dev, fresh:last])
        fresh = 0
        if shared_end:
            pieces.append(grouped[:, dev, last:] + grouped[:, dev + 1, :1])
            fresh = 1
    tiles = jnp.concatenate(pieces, axis=1)
    return tiles.reshape((GROUP // 4 * period_tiles,) + tiles.shape[2:])


def tiles_to_windows(tiles, share_len, num_tiles):
    starts, period_tiles = window_starts(share_len // LANES)
    grouped = tiles.reshape((GROUP // 4, period_tiles) + tiles.shape[1:])
    windows = jnp.stack([grouped[:, start:start + num_tiles] for start in starts], axis=1)
    return windows.reshape((GROUP, num_tiles) + tiles.shape[1:])


def piece_shapes(num_tokens, num_chans):
    tok_hid = num_chans // 2
    ch_hid = 4 * num_chans
    return [(num_tokens, tok_hid), (tok_hid, num_tokens), (num_chans, ch_hid), (ch_hid, num_chans), (num_chans,), (num_chans,), (tok_hid,), (num_tokens,), (num_chans,), (num_chans,), (ch_hid,), (num_chans,)]


def unpack_tiles(tiles, num_tokens, num_chans):
    pieces = []
    start = 0
    shapes = piece_shapes(num_tokens, num_chans)
    for shape_one in shapes[:4]:
        count = math.prod(shape_one) // TILE
        pieces.append(tiles[start:start + count].reshape(shape_one))
        start = start + count
    flat = tiles[start:].reshape(-1)
    start = 0
    for shape_one in shapes[4:]:
        pieces.append(flat[start:start + shape_one[0]])
        start = start + shape_one[0]
    return pieces


def pack_tiles(grads, flat_len):
    pieces = [grad.reshape(-1, ROWS, LANES) for grad in grads[:4]]
    used = sum(piece.shape[0] for piece in pieces) * TILE
    vectors = jnp.concatenate(grads[4:])
    vectors = jnp.pad(vectors, (0, flat_len - used - vectors.shape[0]))
    pieces.append(vectors.reshape(-1, ROWS, LANES))
    return jnp.concatenate(pieces, axis=0)


def head_to_tiles(head):
    rows = head.shape[0]
    head = jnp.pad(head, ((0, 0), (0, HEAD_PAD - head.shape[1])))
    return head.reshape(rows // ROWS, ROWS, HEAD_PAD // LANES, LANES).transpose(0, 2, 1, 3).reshape(-1, ROWS, LANES)


def tiles_to_head(tiles, rows):
    tiles = tiles.reshape(rows // ROWS, HEAD_PAD // LANES, ROWS, LANES)
    return tiles.transpose(0, 2, 1, 3).reshape(rows, HEAD_PAD)


def sum_kernel(x_ref, out_ref, held, local_sem, send_sems, recv_sems):
    me = lax.axis_index(AXIS)
    barrier = pltpu.get_barrier_semaphore()
    for step in range(1, GROUP):
        pl.semaphore_signal(barrier, inc=1, device_id=((me + step) % GROUP,), device_id_type=pl.DeviceIdType.MESH)
    own = pltpu.make_async_copy(x_ref, held.at[me], local_sem)
    own.start()
    pl.semaphore_wait(barrier, GROUP - 1)
    sends = []
    for step in range(1, GROUP):
        copy = pltpu.make_async_remote_copy(
            src_ref=x_ref, dst_ref=held.at[me], send_sem=send_sems.at[step], recv_sem=recv_sems.at[me],
            device_id=((me + step) % GROUP,), device_id_type=pl.DeviceIdType.MESH)
        copy.start()
        sends.append(copy)
    own.wait()
    for step in range(1, GROUP):
        peer = (me + step) % GROUP
        pltpu.make_async_remote_copy(
            src_ref=x_ref, dst_ref=held.at[peer], send_sem=send_sems.at[step], recv_sem=recv_sems.at[peer],
            device_id=(peer,), device_id_type=pl.DeviceIdType.MESH).wait_recv()
    for copy in sends:
        copy.wait_send()
    out_ref[...] = jnp.sum(held[...], axis=0)


def sum_over_devices(values):
    block = jnp.zeros((ROWS, LANES), jnp.float32)
    for pos, value in enumerate(values):
        block = block.at[0, pos].set(value)
    total = pl.pallas_call(
        sum_kernel,
        out_shape=jax.ShapeDtypeStruct((ROWS, LANES), jnp.float32),
        in_specs=[pl.BlockSpec(memory_space=pltpu.VMEM)],
        out_specs=pl.BlockSpec(memory_space=pltpu.VMEM),
        scratch_shapes=[
            pltpu.VMEM((GROUP, ROWS, LANES), jnp.float32),
            pltpu.SemaphoreType.DMA,
            pltpu.SemaphoreType.DMA((GROUP,)),
            pltpu.SemaphoreType.DMA((GROUP,)),
        ],
        compiler_params=pltpu.CompilerParams(collective_id=0, has_side_effects=True),
        name='sum_over_devices',
    )(block)
    return [total[0, pos] for pos in range(len(values))]


def layer_norm(x_in, ln_gain, ln_shift):
    x_f = x_in.astype(jnp.float32)
    mean_val = jnp.mean(x_f, axis=-1, keepdims=True)
    var_val = jnp.mean(jnp.square(x_f - mean_val), axis=-1, keepdims=True)
    normed = (x_f - mean_val) * lax.rsqrt(var_val + LN_EPS)
    return (normed * ln_gain.astype(jnp.float32) + ln_shift.astype(jnp.float32)).astype(jnp.bfloat16)


def gelu_both(hidden):
    scale = math.sqrt(2.0 / math.pi)
    square = hidden * hidden
    tanh_val = jnp.tanh(hidden * (scale + (scale * 0.044715) * square))
    cdf = 0.5 + 0.5 * tanh_val
    slope = cdf + (0.5 * hidden) * (1.0 - tanh_val * tanh_val) * (scale + (3.0 * scale * 0.044715) * square)
    return (hidden * cdf).astype(jnp.bfloat16), slope


def norm_grad(x_in, ln_gain, ln_shift, d_normed):
    _, pullback = jax.vjp(layer_norm, x_in, ln_gain.astype(jnp.float32), ln_shift.astype(jnp.float32))
    d_x, d_gain, d_shift = pullback(d_normed.astype(jnp.bfloat16))
    return d_x.astype(jnp.float32), d_gain, d_shift


def layer_forward(x_in, weights):
    w_tok1, w_tok2, w_ch1, w_ch2, ln1_g, ln1_b, b_tok1, b_tok2, ln2_g, ln2_b, b_ch1, b_ch2 = weights
    normed = layer_norm(x_in, ln1_g, ln1_b)
    hid_tok = jnp.einsum('bsc,sj->bcj', normed, w_tok1, preferred_element_type=jnp.float32) + b_tok1.astype(jnp.float32)
    act_tok, slope_tok = gelu_both(hid_tok)
    tok_out = jnp.einsum('bcj,js->bsc', act_tok, w_tok2, preferred_element_type=jnp.float32) + b_tok2.astype(jnp.float32)[:, None]
    after_tok = (x_in.astype(jnp.float32) + tok_out).astype(jnp.bfloat16)
    normed2 = layer_norm(after_tok, ln2_g, ln2_b)
    hid_ch = jnp.einsum('bsc,cd->bsd', normed2, w_ch1, preferred_element_type=jnp.float32) + b_ch1.astype(jnp.float32)
    act_ch, slope_ch = gelu_both(hid_ch)
    ch_out = jnp.einsum('bsd,dc->bsc', act_ch, w_ch2, preferred_element_type=jnp.float32) + b_ch2.astype(jnp.float32)
    layer_out = (after_tok.astype(jnp.float32) + ch_out).astype(jnp.bfloat16)
    return layer_out, (x_in, normed, slope_tok, act_tok, after_tok, normed2, slope_ch, act_ch)


def layer_backward(d_out, weights, cache):
    w_tok1, w_tok2, w_ch1, w_ch2, ln1_g, ln1_b, b_tok1, b_tok2, ln2_g, ln2_b, b_ch1, b_ch2 = weights
    x_in, normed, slope_tok, act_tok, after_tok, normed2, slope_ch, act_ch = cache
    d_out_bf = d_out.astype(jnp.bfloat16)
    g_b_ch2 = jnp.sum(d_out, axis=(0, 1))
    g_w_ch2 = jnp.einsum('bsd,bsc->dc', act_ch, d_out_bf, preferred_element_type=jnp.float32)
    d_act_ch = jnp.einsum('bsc,dc->bsd', d_out_bf, w_ch2, preferred_element_type=jnp.float32)
    d_hid_ch = d_act_ch.astype(jnp.bfloat16).astype(jnp.float32) * slope_ch
    d_hid_ch_bf = d_hid_ch.astype(jnp.bfloat16)
    g_b_ch1 = jnp.sum(d_hid_ch, axis=(0, 1))
    g_w_ch1 = jnp.einsum('bsc,bsd->cd', normed2, d_hid_ch_bf, preferred_element_type=jnp.float32)
    d_normed2 = jnp.einsum('bsd,cd->bsc', d_hid_ch_bf, w_ch1, preferred_element_type=jnp.float32)
    d_after_ln, g_ln2_g, g_ln2_b = norm_grad(after_tok, ln2_g, ln2_b, d_normed2)
    d_after = d_after_ln + d_out
    d_after_bf = d_after.astype(jnp.bfloat16)
    g_b_tok2 = jnp.sum(d_after, axis=(0, 2))
    g_w_tok2 = jnp.einsum('bcj,bsc->js', act_tok, d_after_bf, preferred_element_type=jnp.float32)
    d_act_tok = jnp.einsum('bsc,js->bcj', d_after_bf, w_tok2, preferred_element_type=jnp.float32)
    d_hid_tok = d_act_tok.astype(jnp.bfloat16).astype(jnp.float32) * slope_tok
    d_hid_tok_bf = d_hid_tok.astype(jnp.bfloat16)
    g_b_tok1 = jnp.sum(d_hid_tok, axis=(0, 1))
    g_w_tok1 = jnp.einsum('bsc,bcj->sj', normed, d_hid_tok_bf, preferred_element_type=jnp.float32)
    d_normed = jnp.einsum('bcj,sj->bsc', d_hid_tok_bf, w_tok1, preferred_element_type=jnp.float32)
    d_in_ln, g_ln1_g, g_ln1_b = norm_grad(x_in, ln1_g, ln1_b, d_normed)
    d_in = d_in_ln + d_after
    return d_in, [g_w_tok1, g_w_tok2, g_w_ch1, g_w_ch2, g_ln1_g, g_ln1_b, g_b_tok1, g_b_tok2, g_ln2_g, g_ln2_b, g_b_ch1, g_b_ch2]


def head_step(hidden, labels, small_full, head_full, num_classes, global_b):
    num_tokens = hidden.shape[1]
    num_chans = hidden.shape[2]
    lnf_g = small_full[:num_chans]
    lnf_b = small_full[num_chans:2 * num_chans]
    head_b = small_full[2 * num_chans:2 * num_chans + num_classes]
    normed = layer_norm(hidden, lnf_g, lnf_b)
    pooled = (jnp.sum(normed, axis=1, dtype=jnp.float32) / num_tokens).astype(jnp.bfloat16)
    is_class = jnp.arange(HEAD_PAD)[None, :] < num_classes
    logits = jnp.dot(pooled, head_full, preferred_element_type=jnp.float32) + jnp.pad(head_b.astype(jnp.float32), (0, HEAD_PAD - num_classes))
    logits = jnp.where(is_class, logits, -jnp.inf)
    log_norm = jax.nn.logsumexp(logits, axis=-1)
    is_label = jnp.arange(HEAD_PAD)[None, :] == labels[:, None]
    picked = jnp.sum(jnp.where(is_label, logits, 0.0), axis=-1)
    loss_sum = jnp.sum(log_norm - picked)
    d_logits = (jnp.exp(logits - log_norm[:, None]) - is_label.astype(jnp.float32)) / global_b
    d_logits_bf = d_logits.astype(jnp.bfloat16)
    g_head_b = jnp.sum(d_logits, axis=0)[:num_classes]
    g_head_w = jnp.einsum('bc,bk->ck', pooled, d_logits_bf, preferred_element_type=jnp.float32)
    d_pooled = jnp.einsum('bk,ck->bc', d_logits_bf, head_full, preferred_element_type=jnp.float32)
    d_normed = jnp.broadcast_to((d_pooled / num_tokens)[:, None, :], normed.shape)
    d_hidden, g_lnf_g, g_lnf_b = norm_grad(hidden, lnf_g, lnf_b, d_normed)
    g_small = jnp.concatenate([g_lnf_g, g_lnf_b, g_head_b])
    return loss_sum, d_hidden, g_head_w, g_small


def adam_update(master, gradient, moment, second, decay_rate):
    moment_new = BETA_ONE * moment + (1.0 - BETA_ONE) * gradient
    second_new = BETA_TWO * second + (1.0 - BETA_TWO) * gradient * gradient
    m_hat = moment_new / (1.0 - BETA_ONE ** ADAM_STEP)
    v_hat = second_new / (1.0 - BETA_TWO ** ADAM_STEP)
    master_new = master - LEARN_RATE * (m_hat / (jnp.sqrt(v_hat) + ADAM_EPS) + decay_rate * master)
    return master_new, moment_new, second_new


def solution(mesh):
    row_spec = P(AXIS)
    layer_spec = P(None, AXIS)
    in_specs = (row_spec, row_spec, layer_spec, row_spec, row_spec, layer_spec, row_spec, row_spec, layer_spec, row_spec, row_spec)
    out_specs = (P(),) + in_specs[2:]

    def device_step(act_in, labels, layer_p, head_w, small_p, layer_m, head_m, small_m, layer_v, head_v, small_v):
        local_b, num_tokens, num_chans = act_in.shape
        global_b = local_b * GROUP
        num_layers, share_len = layer_p.shape
        flat_len = share_len * GROUP
        head_rows, num_classes = head_w.shape
        small_len = small_p.shape[0]
        mat_len = 2 * num_tokens * (num_chans // 2) + 8 * num_chans * num_chans

        windows = [share_to_window(layer_p[layer_idx].astype(jnp.bfloat16)) for layer_idx in range(num_layers)]
        win_tiles = windows[0].shape[0]
        head_tiles = head_to_tiles(head_w.astype(jnp.bfloat16))
        small_tile = jnp.pad(small_p.astype(jnp.bfloat16).reshape(1, 1, small_len), ((0, 0), (0, ROWS - 1), (0, 0)))
        windows[-1] = jnp.concatenate([windows[-1], head_tiles, small_tile], axis=0)
        num_head = head_tiles.shape[0]

        weights = []
        caches = []
        hidden = act_in
        gathered = []
        for layer_idx in range(num_layers):
            own = windows[layer_idx]
            if layer_idx:
                own, gathered[-1] = lax.optimization_barrier((own, gathered[-1]))
            gathered.append(gather_tiles(own))
        for layer_idx in range(num_layers):
            tiles = windows_to_tiles(gathered[layer_idx][:, :win_tiles], share_len)
            weights.append(unpack_tiles(tiles, num_tokens, num_chans))
            hidden, cache = layer_forward(hidden, weights[layer_idx])
            caches.append(cache)
        extra = gathered[-1][:, win_tiles:]
        head_full = tiles_to_head(extra[:, :num_head], head_rows * GROUP)
        small_full = extra[:, num_head, 0].reshape(-1)
        loss_sum, d_hidden, g_head_w, g_small = head_step(hidden, labels, small_full, head_full, num_classes, global_b)

        head_blocks = head_to_tiles(g_head_w).reshape(GROUP, num_head, ROWS, LANES)
        g_small = jnp.pad(g_small, (0, small_len * GROUP - g_small.shape[0])).reshape(GROUP, 1, 1, small_len)
        small_blocks = jnp.pad(g_small, ((0, 0), (0, 0), (0, ROWS - 1), (0, 0)))
        layer_shares = [None] * num_layers
        for layer_idx in reversed(range(num_layers)):
            d_hidden, grads = layer_backward(d_hidden, weights[layer_idx], caches[layer_idx])
            blocks = tiles_to_windows(pack_tiles(grads, flat_len), share_len, win_tiles)
            if layer_idx == num_layers - 1:
                blocks = jnp.concatenate([blocks, head_blocks, small_blocks], axis=1)
            summed = scatter_tiles(blocks)
            layer_shares[layer_idx] = window_to_share(summed[:win_tiles], share_len)
            if layer_idx == num_layers - 1:
                head_g = tiles_to_head(summed[win_tiles:win_tiles + num_head], head_rows)[:, :num_classes]
                small_g = summed[win_tiles + num_head, 0]
        layer_g = jnp.stack(layer_shares)

        sq_local = jnp.sum(jnp.square(layer_g)) + jnp.sum(jnp.square(head_g)) + jnp.sum(jnp.square(small_g))
        loss_total, sq_total = sum_over_devices([loss_sum, sq_local])
        loss_value = loss_total / global_b
        clip_scale = 1.0 / jnp.maximum(1.0, jnp.sqrt(sq_total))
        flat_pos = lax.axis_index(AXIS) * share_len + jnp.arange(share_len)
        layer_decay = jnp.where(flat_pos < mat_len, WEIGHT_DECAY, 0.0)[None, :]
        new_lp, new_lm, new_lv = adam_update(layer_p, layer_g * clip_scale, layer_m, layer_v, layer_decay)
        new_hw, new_hm, new_hv = adam_update(head_w, head_g * clip_scale, head_m, head_v, WEIGHT_DECAY)
        new_sp, new_sm, new_sv = adam_update(small_p, small_g * clip_scale, small_m, small_v, 0.0)
        return (loss_value, new_lp, new_hw, new_sp, new_lm, new_hm, new_sm, new_lv, new_hv, new_sv)

    return jax.shard_map(device_step, mesh=mesh, in_specs=in_specs, out_specs=out_specs, check_vma=False)
```

```python
import math
import jax
import jax.numpy as jnp
from jax import lax
from jax.experimental import pallas as pl
from jax.experimental.pallas import tpu as pltpu
from jax.sharding import PartitionSpec as P

LN_EPS = 1e-6
LEARN_RATE = 0.003
BETA_ONE = 0.9
BETA_TWO = 0.999
ADAM_EPS = 1e-8
WEIGHT_DECAY = 0.03
ADAM_STEP = 10
AXIS = 'fsdp'
GROUP = 32
ROWS = 8
LANES = 128
TILE = ROWS * LANES
HEAD_PAD = 1024

def row_offset(share_rows):
    return (lax.axis_index(AXIS) * share_rows) % ROWS


def share_to_window(share):
    share_rows = share.shape[0] // LANES
    num_tiles = -(-(share_rows + ROWS - 2) // ROWS)
    window = jnp.zeros((num_tiles * ROWS, LANES), share.dtype)
    window = lax.dynamic_update_slice(window, share.reshape(share_rows, LANES), (row_offset(share_rows), 0))
    return window.reshape(num_tiles, ROWS, LANES)


def window_to_share(window, share_len):
    share_rows = share_len // LANES
    rows = window.reshape(-1, LANES)
    return lax.dynamic_slice(rows, (row_offset(share_rows), 0), (share_rows, LANES)).reshape(share_len)


def piece_shapes(num_tokens, num_chans):
    tok_hid = num_chans // 2
    ch_hid = 4 * num_chans
    return [(num_tokens, tok_hid), (tok_hid, num_tokens), (num_chans, ch_hid), (ch_hid, num_chans), (num_chans,), (num_chans,), (tok_hid,), (num_tokens,), (num_chans,), (num_chans,), (ch_hid,), (num_chans,)]


def unpack_tiles(tiles, num_tokens, num_chans):
    pieces = []
    start = 0
    shapes = piece_shapes(num_tokens, num_chans)
    for shape_one in shapes[:4]:
        count = math.prod(shape_one) // TILE
        pieces.append(tiles[start:start + count].reshape(shape_one))
        start = start + count
    flat = tiles[start:].reshape(-1)
    start = 0
    for shape_one in shapes[4:]:
        pieces.append(flat[start:start + shape_one[0]])
        start = start + shape_one[0]
    return pieces


def pack_tiles(grads, flat_len):
    pieces = [grad.reshape(-1, ROWS, LANES) for grad in grads[:4]]
    used = sum(piece.shape[0] for piece in pieces) * TILE
    vectors = jnp.concatenate(grads[4:])
    vectors = jnp.pad(vectors, (0, flat_len - used - vectors.shape[0]))
    pieces.append(vectors.reshape(-1, ROWS, LANES))
    return jnp.concatenate(pieces, axis=0)


def head_to_tiles(head):
    rows = head.shape[0]
    head = jnp.pad(head, ((0, 0), (0, HEAD_PAD - head.shape[1])))
    return head.reshape(rows // ROWS, ROWS, HEAD_PAD // LANES, LANES).transpose(0, 2, 1, 3).reshape(-1, ROWS, LANES)


def tiles_to_head(tiles, rows):
    tiles = tiles.reshape(rows // ROWS, HEAD_PAD // LANES, ROWS, LANES)
    return tiles.transpose(0, 2, 1, 3).reshape(rows, HEAD_PAD)


MASK_CORE, MASK_X, MASK_Y, MASK_Z = 1, 2, 4, 8
PARTNERS = (MASK_CORE, MASK_X, MASK_Y, MASK_Z, 2 * MASK_Z, 3 * MASK_Z)
PERIOD = 4


class Peers:
    def __init__(self, me):
        self.bits = []
        for bit in range(5):
            val = lax.rem(lax.div(me, 1 << bit), 2)
            self.bits.append((val, 1 - val))
        self.known = {}

    def split(self, rel):
        if rel not in self.known:
            vals = [self.bits[bit][(rel >> bit) & 1] for bit in range(5)]
            pos = vals[0] + 2 * vals[1]
            group = vals[2] + 2 * vals[3] + 4 * vals[4]
            self.known[rel] = (group * PERIOD + pos, group, pos)
        return self.known[rel]

    def device(self, rel):
        return self.split(rel)[0]


def meet_partners(peers):
    barrier = pltpu.get_barrier_semaphore()
    for mask in PARTNERS:
        pl.semaphore_signal(barrier, inc=1, device_id=(peers.device(mask),), device_id_type=pl.DeviceIdType.MESH)
    pl.semaphore_wait(barrier, len(PARTNERS))


def gather_kernel(inner0_ref, inner1_ref, misc_ref, flat0_ref, flat1_ref, extra_ref, misc_all, bound, local_sems, send_sems, recv_sems):
    peers = Peers(lax.axis_index(AXIS))
    inner = inner0_ref.shape[0]
    stride = inner + 1
    own_refs = (inner0_ref, inner1_ref, misc_ref)
    colours = ((MASK_Y, MASK_X), (MASK_X, MASK_Y), (MASK_X, MASK_Y))

    def place(arr, rel):
        dev, group, pos = peers.split(rel)
        if arr == 2:
            return misc_all.at[dev]
        flat = (flat0_ref, flat1_ref)[arr]
        return flat.at[group, pl.ds(stride * pos + 1, inner)]

    own_copies = [pltpu.make_async_copy(own_refs[arr], place(arr, 0), local_sems.at[arr]) for arr in range(3)]
    for copy in own_copies:
        copy.start()
    meet_partners(peers)
    sends = []

    def send(arr, rel, mask):
        here = place(arr, rel)
        copy = pltpu.make_async_remote_copy(
            src_ref=own_refs[arr] if rel == 0 else here, dst_ref=here,
            send_sem=send_sems.at[arr, rel ^ mask], recv_sem=recv_sems.at[arr, rel ^ mask],
            device_id=(peers.device(mask),), device_id_type=pl.DeviceIdType.MESH)
        copy.start()
        sends.append(copy)

    def receive(arr, rel):
        here = place(arr, rel)
        pltpu.make_async_remote_copy(
            src_ref=here, dst_ref=here, send_sem=send_sems.at[arr, rel], recv_sem=recv_sems.at[arr, rel],
            device_id=(peers.device(0),), device_id_type=pl.DeviceIdType.MESH).wait_recv()

    for mask_pos in range(6):
        for arr in range(3):
            first, second = colours[arr]
            send(arr, 0, (MASK_Z, first, second, 2 * MASK_Z, 3 * MASK_Z, MASK_CORE)[mask_pos])
    for dist, use_first, use_second in ((0, 1, 0), (1, 0, 0), (0, 0, 1), (1, 1, 0), (0, 1, 1), (2, 0, 0), (1, 0, 1), (2, 1, 0),
                                        (1, 1, 1), (3, 0, 0), (2, 0, 1), (3, 1, 0), (2, 1, 1), (3, 0, 1), (3, 1, 1)):
        for arr in range(3):
            first, second = colours[arr]
            rel = dist * MASK_Z + use_first * first + use_second * second
            receive(arr, rel)
            if not use_second:
                if not use_first:
                    send(arr, rel, first)
                send(arr, rel, second)
            send(arr, rel, MASK_CORE)
    for rel in range(MASK_CORE, GROUP, 2):
        for arr in range(3):
            receive(arr, rel)
    for copy in own_copies:
        copy.wait()
    for copy in sends:
        copy.wait_send()

    for layer_idx in range(2):
        for group in range(GROUP // PERIOD):
            for pos in range(PERIOD + 1):
                tile = None
                if pos < PERIOD:
                    tile = misc_all[group * PERIOD + pos, 2 * layer_idx]
                if pos > 0:
                    left = misc_all[group * PERIOD + pos - 1, 2 * layer_idx + 1]
                    tile = left if tile is None else tile + left
                bound[layer_idx, pos, group, 0] = tile
    extra_ref[...] = misc_all[:, 4:]
    edges = []
    for layer_idx in range(2):
        flat = (flat0_ref, flat1_ref)[layer_idx]
        for pos in range(PERIOD + 1):
            edges.append(pltpu.make_async_copy(bound.at[layer_idx, pos], flat.at[:, pl.ds(stride * pos, 1)], local_sems.at[3 + layer_idx * (PERIOD + 1) + pos]))
    for copy in edges:
        copy.start()
    for copy in edges:
        copy.wait()


def gather_shares(window0, window1, extra):
    num_tiles = window0.shape[0]
    num_extra = extra.shape[0]
    inner = num_tiles - 2
    misc = jnp.concatenate([window0[:1], window0[-1:], window1[:1], window1[-1:], extra], axis=0)
    flat = (GROUP // PERIOD, PERIOD * (num_tiles - 1) + 1, ROWS, LANES)
    vmem = pl.BlockSpec(memory_space=pltpu.VMEM)
    hbm = pl.BlockSpec(memory_space=pl.ANY)
    dtype = window0.dtype
    return pl.pallas_call(
        gather_kernel,
        out_shape=(jax.ShapeDtypeStruct(flat, dtype), jax.ShapeDtypeStruct(flat, dtype), jax.ShapeDtypeStruct((GROUP, num_extra, ROWS, LANES), dtype)),
        in_specs=[vmem] * 3,
        out_specs=(hbm, hbm, vmem),
        scratch_shapes=[
            pltpu.VMEM((GROUP, num_extra + 4, ROWS, LANES), dtype),
            pltpu.VMEM((2, PERIOD + 1, GROUP // PERIOD, 1, ROWS, LANES), dtype),
            pltpu.SemaphoreType.DMA((3 + 2 * (PERIOD + 1),)),
            pltpu.SemaphoreType.DMA((3, GROUP)),
            pltpu.SemaphoreType.DMA((3, GROUP)),
        ],
        compiler_params=pltpu.CompilerParams(collective_id=1, has_side_effects=True),
        name='gather_shares',
    )(window0[1:-1], window1[1:-1], misc)


def scatter_kernel(grad0_ref, grad1_ref, extra_ref, out0_ref, out1_ref, own0, own1, core0, core1, first0, first1, second0, second1, far0, far1,
                   load_sems, send_sems, core_sems, first_sems, second_sems, far_sems):
    peers = Peers(lax.axis_index(AXIS))
    num_tiles = out0_ref.shape[0]
    num_extra = extra_ref.shape[1]
    own, near, first_in, second_in, far_in = (own0, own1), (core0, core1), (first0, first1), (second0, second1), (far0, far1)
    colours = ((MASK_X, MASK_Y), (MASK_Y, MASK_X))
    dists = (3, 2, 1, 0)
    sends = []

    def source(part, rel):
        dev, group, pos = peers.split(rel)
        if part == 2:
            return extra_ref.at[dev]
        grad = (grad0_ref, grad1_ref)[part]
        return grad.at[group, pl.ds((num_tiles - 1) * pos, num_tiles)]

    def slot(part, buffers, pos):
        if part == 2:
            return buffers[1].at[pos, pl.ds(num_tiles, num_extra)]
        return buffers[part].at[pos, pl.ds(0, num_tiles)]

    def post(src, dst, send_sem, recv_sem, mask):
        copy = pltpu.make_async_remote_copy(src_ref=src, dst_ref=dst, send_sem=send_sem, recv_sem=recv_sem,
                                            device_id=(peers.device(mask),), device_id_type=pl.DeviceIdType.MESH)
        copy.start()
        sends.append(copy)

    def expect(dst, send_sem, recv_sem):
        pltpu.make_async_remote_copy(src_ref=dst, dst_ref=dst, send_sem=send_sem, recv_sem=recv_sem,
                                     device_id=(peers.device(0),), device_id_type=pl.DeviceIdType.MESH).wait_recv()

    def targets(dist):
        return [(dist * 4 + pos, dist * MASK_Z + pos * MASK_X) for pos in (3, 2, 1, 0)]

    loads = {}
    for dist in dists:
        for pos, rel in targets(dist):
            for part in range(3):
                loads[part, pos] = pltpu.make_async_copy(source(part, rel), slot(part, own, pos), load_sems.at[part, pos])
                loads[part, pos].start()
    meet_partners(peers)
    for dist in dists:
        for pos, rel in targets(dist):
            for part in range(3):
                post(source(part, rel | MASK_CORE), slot(part, near, pos), send_sems.at[part, pos], core_sems.at[part, pos], MASK_CORE)

    def fold_core(dist):
        for pos, rel in targets(dist):
            for part in range(3):
                loads[part, pos].wait()
                expect(slot(part, near, pos), send_sems.at[part, pos], core_sems.at[part, pos])
            for side in range(2):
                own[side][pos] += near[side][pos]
        for side in range(2):
            mask, other = colours[side]
            for which in (1, 0):
                pos = dist * 4 + (mask + which * other) // MASK_X
                index = dist * 2 + which
                post(own[side].at[pos], first_in[side].at[index], send_sems.at[3 + side, index], first_sems.at[side, index], mask)

    def fold_first(dist):
        for side in range(2):
            mask, other = colours[side]
            for which in (1, 0):
                pos = dist * 4 + which * other // MASK_X
                index = dist * 2 + which
                expect(first_in[side].at[index], send_sems.at[3 + side, index], first_sems.at[side, index])
                own[side][pos] += first_in[side][index]
        for side in range(2):
            mask, other = colours[side]
            post(own[side].at[dist * 4 + other // MASK_X], second_in[side].at[dist], send_sems.at[3 + side, 8 + dist], second_sems.at[side, dist], other)

    def fold_second(dist):
        for side in range(2):
            expect(second_in[side].at[dist], send_sems.at[3 + side, 8 + dist], second_sems.at[side, dist])
            own[side][dist * 4] += second_in[side][dist]
        if dist:
            for side in range(2):
                post(own[side].at[dist * 4], far_in[side].at[dist - 1], send_sems.at[3 + side, 12 + dist], far_sems.at[side, dist - 1], dist * MASK_Z)

    for dist in dists:
        fold_core(dist)
    fold_first(3)
    fold_first(2)
    fold_second(3)
    fold_first(1)
    fold_second(2)
    fold_first(0)
    fold_second(1)
    fold_second(0)
    for side in range(2):
        total = own[side][0]
        for dist in (3, 2, 1):
            expect(far_in[side].at[dist - 1], send_sems.at[3 + side, 12 + dist], far_sems.at[side, dist - 1])
            total = total + far_in[side][dist - 1]
        (out0_ref, out1_ref)[side][...] = total
    for copy in sends:
        copy.wait_send()


def scatter_grads(grad0, grad1, extra, num_tiles):
    num_extra = extra.shape[1]
    sizes = (num_tiles, num_tiles + num_extra)
    vmem = pl.BlockSpec(memory_space=pltpu.VMEM)
    hbm = pl.BlockSpec(memory_space=pl.ANY)

    def buffers(count):
        return [pltpu.VMEM((count, size, ROWS, LANES), jnp.float32) for size in sizes]

    return pl.pallas_call(
        scatter_kernel,
        out_shape=tuple(jax.ShapeDtypeStruct((size, ROWS, LANES), jnp.float32) for size in sizes),
        in_specs=[hbm] * 3,
        out_specs=(vmem, vmem),
        scratch_shapes=buffers(16) + buffers(16) + buffers(8) + buffers(4) + buffers(3) + [
            pltpu.SemaphoreType.DMA((3, 16)),
            pltpu.SemaphoreType.DMA((5, 16)),
            pltpu.SemaphoreType.DMA((3, 16)),
            pltpu.SemaphoreType.DMA((2, 8)),
            pltpu.SemaphoreType.DMA((2, 4)),
            pltpu.SemaphoreType.DMA((2, 3)),
        ],
        compiler_params=pltpu.CompilerParams(collective_id=2, has_side_effects=True),
        name='scatter_grads',
    )(grad0, grad1, extra)


def sum_kernel(x_ref, out_ref, held, local_sem, send_sems, recv_sems):
    me = lax.axis_index(AXIS)
    barrier = pltpu.get_barrier_semaphore()
    for step in range(1, GROUP):
        pl.semaphore_signal(barrier, inc=1, device_id=((me + step) % GROUP,), device_id_type=pl.DeviceIdType.MESH)
    own = pltpu.make_async_copy(x_ref, held.at[me], local_sem)
    own.start()
    pl.semaphore_wait(barrier, GROUP - 1)
    sends = []
    for step in range(1, GROUP):
        copy = pltpu.make_async_remote_copy(
            src_ref=x_ref, dst_ref=held.at[me], send_sem=send_sems.at[step], recv_sem=recv_sems.at[me],
            device_id=((me + step) % GROUP,), device_id_type=pl.DeviceIdType.MESH)
        copy.start()
        sends.append(copy)
    own.wait()
    for step in range(1, GROUP):
        peer = (me + step) % GROUP
        pltpu.make_async_remote_copy(
            src_ref=x_ref, dst_ref=held.at[peer], send_sem=send_sems.at[step], recv_sem=recv_sems.at[peer],
            device_id=(peer,), device_id_type=pl.DeviceIdType.MESH).wait_recv()
    for copy in sends:
        copy.wait_send()
    out_ref[...] = jnp.sum(held[...], axis=0)


def sum_over_devices(values):
    block = jnp.zeros((ROWS, LANES), jnp.float32)
    for pos, value in enumerate(values):
        block = block.at[0, pos].set(value)
    total = pl.pallas_call(
        sum_kernel,
        out_shape=jax.ShapeDtypeStruct((ROWS, LANES), jnp.float32),
        in_specs=[pl.BlockSpec(memory_space=pltpu.VMEM)],
        out_specs=pl.BlockSpec(memory_space=pltpu.VMEM),
        scratch_shapes=[
            pltpu.VMEM((GROUP, ROWS, LANES), jnp.float32),
            pltpu.SemaphoreType.DMA,
            pltpu.SemaphoreType.DMA((GROUP,)),
            pltpu.SemaphoreType.DMA((GROUP,)),
        ],
        compiler_params=pltpu.CompilerParams(collective_id=0, has_side_effects=True),
        name='sum_over_devices',
    )(block)
    return [total[0, pos] for pos in range(len(values))]


def layer_norm(x_in, ln_gain, ln_shift):
    x_f = x_in.astype(jnp.float32)
    mean_val = jnp.mean(x_f, axis=-1, keepdims=True)
    var_val = jnp.mean(jnp.square(x_f - mean_val), axis=-1, keepdims=True)
    normed = (x_f - mean_val) * lax.rsqrt(var_val + LN_EPS)
    return (normed * ln_gain.astype(jnp.float32) + ln_shift.astype(jnp.float32)).astype(jnp.bfloat16)


def gelu_both(hidden):
    scale = math.sqrt(2.0 / math.pi)
    square = hidden * hidden
    tanh_val = jnp.tanh(hidden * (scale + (scale * 0.044715) * square))
    cdf = 0.5 + 0.5 * tanh_val
    slope = cdf + (0.5 * hidden) * (1.0 - tanh_val * tanh_val) * (scale + (3.0 * scale * 0.044715) * square)
    return (hidden * cdf).astype(jnp.bfloat16), slope


def norm_grad(x_in, ln_gain, ln_shift, d_normed):
    _, pullback = jax.vjp(layer_norm, x_in, ln_gain.astype(jnp.float32), ln_shift.astype(jnp.float32))
    d_x, d_gain, d_shift = pullback(d_normed.astype(jnp.bfloat16))
    return d_x.astype(jnp.float32), d_gain, d_shift


def scoped(tag, spec, lhs, rhs, **kwargs):
    with jax.named_scope(tag):
        return jnp.einsum(spec, lhs, rhs, **kwargs)


def layer_forward(x_in, weights, tag):
    w_tok1, w_tok2, w_ch1, w_ch2, ln1_g, ln1_b, b_tok1, b_tok2, ln2_g, ln2_b, b_ch1, b_ch2 = weights
    normed = layer_norm(x_in, ln1_g, ln1_b)
    hid_tok = scoped(tag + '_tok1', 'bsc,sj->bcj', normed, w_tok1, preferred_element_type=jnp.float32) + b_tok1.astype(jnp.float32)
    act_tok, slope_tok = gelu_both(hid_tok)
    with jax.named_scope(tag + '_tok2'):
        tok_out = jnp.einsum('bcj,js->bsc', act_tok, w_tok2, preferred_element_type=jnp.float32) + b_tok2.astype(jnp.float32)[:, None]
        after_tok = (x_in.astype(jnp.float32) + tok_out).astype(jnp.bfloat16)
    normed2 = layer_norm(after_tok, ln2_g, ln2_b)
    hid_ch = scoped(tag + '_ch1', 'bsc,cd->bsd', normed2, w_ch1, preferred_element_type=jnp.float32) + b_ch1.astype(jnp.float32)
    act_ch, slope_ch = gelu_both(hid_ch)
    with jax.named_scope(tag + '_ch2'):
        ch_out = jnp.einsum('bsd,dc->bsc', act_ch, w_ch2, preferred_element_type=jnp.float32) + b_ch2.astype(jnp.float32)
        layer_out = (after_tok.astype(jnp.float32) + ch_out).astype(jnp.bfloat16)
    return layer_out, (x_in, normed, slope_tok, act_tok, after_tok, normed2, slope_ch, act_ch)


def layer_backward(d_out, weights, cache, tag):
    w_tok1, w_tok2, w_ch1, w_ch2, ln1_g, ln1_b, b_tok1, b_tok2, ln2_g, ln2_b, b_ch1, b_ch2 = weights
    x_in, normed, slope_tok, act_tok, after_tok, normed2, slope_ch, act_ch = cache
    d_out_bf = d_out.astype(jnp.bfloat16)
    g_b_ch2 = jnp.sum(d_out, axis=(0, 1))
    g_w_ch2 = scoped(tag + '_gw2', 'bsd,bsc->dc', act_ch, d_out_bf, preferred_element_type=jnp.float32)
    with jax.named_scope(tag + '_dact'):
        d_act_ch = jnp.einsum('bsc,dc->bsd', d_out_bf, w_ch2, preferred_element_type=jnp.float32)
        d_hid_ch = d_act_ch.astype(jnp.bfloat16).astype(jnp.float32) * slope_ch
        d_hid_ch_bf = d_hid_ch.astype(jnp.bfloat16)
        g_b_ch1 = jnp.sum(d_hid_ch, axis=(0, 1))
    g_w_ch1 = scoped(tag + '_gw1', 'bsc,bsd->cd', normed2, d_hid_ch_bf, preferred_element_type=jnp.float32)
    d_normed2 = scoped(tag + '_dnorm2', 'bsd,cd->bsc', d_hid_ch_bf, w_ch1, preferred_element_type=jnp.float32)
    with jax.named_scope(tag + '_ln2'):
        d_after_ln, g_ln2_g, g_ln2_b = norm_grad(after_tok, ln2_g, ln2_b, d_normed2)
    d_after = d_after_ln + d_out
    d_after_bf = d_after.astype(jnp.bfloat16)
    g_b_tok2 = jnp.sum(d_after, axis=(0, 2))
    g_w_tok2 = scoped(tag + '_gt2', 'bcj,bsc->js', act_tok, d_after_bf, preferred_element_type=jnp.float32)
    with jax.named_scope(tag + '_dtok'):
        d_act_tok = jnp.einsum('bsc,js->bcj', d_after_bf, w_tok2, preferred_element_type=jnp.float32)
        d_hid_tok = d_act_tok.astype(jnp.bfloat16).astype(jnp.float32) * slope_tok
        d_hid_tok_bf = d_hid_tok.astype(jnp.bfloat16)
        g_b_tok1 = jnp.sum(d_hid_tok, axis=(0, 1))
    g_w_tok1 = scoped(tag + '_gt1', 'bsc,bcj->sj', normed, d_hid_tok_bf, preferred_element_type=jnp.float32)
    d_normed = scoped(tag + '_dnt', 'bcj,sj->bsc', d_hid_tok_bf, w_tok1, preferred_element_type=jnp.float32)
    d_in_ln, g_ln1_g, g_ln1_b = norm_grad(x_in, ln1_g, ln1_b, d_normed)
    d_in = d_in_ln + d_after
    return d_in, [g_w_tok1, g_w_tok2, g_w_ch1, g_w_ch2, g_ln1_g, g_ln1_b, g_b_tok1, g_b_tok2, g_ln2_g, g_ln2_b, g_b_ch1, g_b_ch2]


def head_step(hidden, labels, small_full, head_full, num_classes, global_b):
    num_tokens = hidden.shape[1]
    num_chans = hidden.shape[2]
    lnf_g = small_full[:num_chans]
    lnf_b = small_full[num_chans:2 * num_chans]
    head_b = small_full[2 * num_chans:2 * num_chans + num_classes]
    normed = layer_norm(hidden, lnf_g, lnf_b)
    pooled = (jnp.sum(normed, axis=1, dtype=jnp.float32) / num_tokens).astype(jnp.bfloat16)
    is_class = jnp.arange(HEAD_PAD)[None, :] < num_classes
    logits = jnp.dot(pooled, head_full, preferred_element_type=jnp.float32) + jnp.pad(head_b.astype(jnp.float32), (0, HEAD_PAD - num_classes))
    logits = jnp.where(is_class, logits, -jnp.inf)
    log_norm = jax.nn.logsumexp(logits, axis=-1)
    is_label = jnp.arange(HEAD_PAD)[None, :] == labels[:, None]
    picked = jnp.sum(jnp.where(is_label, logits, 0.0), axis=-1)
    loss_sum = jnp.sum(log_norm - picked)
    d_logits = (jnp.exp(logits - log_norm[:, None]) - is_label.astype(jnp.float32)) / global_b
    d_logits_bf = d_logits.astype(jnp.bfloat16)
    g_head_b = jnp.sum(d_logits, axis=0)[:num_classes]
    g_head_w = jnp.einsum('bc,bk->ck', pooled, d_logits_bf, preferred_element_type=jnp.float32)
    d_pooled = jnp.einsum('bk,ck->bc', d_logits_bf, head_full, preferred_element_type=jnp.float32)
    d_normed = jnp.broadcast_to((d_pooled / num_tokens)[:, None, :], normed.shape)
    d_hidden, g_lnf_g, g_lnf_b = norm_grad(hidden, lnf_g, lnf_b, d_normed)
    g_small = jnp.concatenate([g_lnf_g, g_lnf_b, g_head_b])
    return loss_sum, d_hidden, g_head_w, g_small


def adam_update(master, gradient, moment, second, decay_rate):
    moment_new = BETA_ONE * moment + (1.0 - BETA_ONE) * gradient
    second_new = BETA_TWO * second + (1.0 - BETA_TWO) * gradient * gradient
    m_hat = moment_new / (1.0 - BETA_ONE ** ADAM_STEP)
    v_hat = second_new / (1.0 - BETA_TWO ** ADAM_STEP)
    master_new = master - LEARN_RATE * (m_hat / (jnp.sqrt(v_hat) + ADAM_EPS) + decay_rate * master)
    return master_new, moment_new, second_new


def solution(mesh):
    row_spec = P(AXIS)
    layer_spec = P(None, AXIS)
    in_specs = (row_spec, row_spec, layer_spec, row_spec, row_spec, layer_spec, row_spec, row_spec, layer_spec, row_spec, row_spec)
    out_specs = (P(),) + in_specs[2:]

    def device_step(act_in, labels, layer_p, head_w, small_p, layer_m, head_m, small_m, layer_v, head_v, small_v):
        local_b, num_tokens, num_chans = act_in.shape
        global_b = local_b * GROUP
        num_layers, share_len = layer_p.shape
        flat_len = share_len * GROUP
        head_rows, num_classes = head_w.shape
        small_len = small_p.shape[0]
        mat_len = 2 * num_tokens * (num_chans // 2) + 8 * num_chans * num_chans

        windows = [share_to_window(layer_p[layer_idx].astype(jnp.bfloat16)) for layer_idx in range(num_layers)]
        win_tiles = windows[0].shape[0]
        head_tiles = head_to_tiles(head_w.astype(jnp.bfloat16))
        small_tile = jnp.pad(small_p.astype(jnp.bfloat16).reshape(1, 1, small_len), ((0, 0), (0, ROWS - 1), (0, 0)))
        num_head = head_tiles.shape[0]
        flat0, flat1, extra = gather_shares(windows[0], windows[1], jnp.concatenate([head_tiles, small_tile], axis=0))

        weights = []
        caches = []
        hidden = act_in
        for layer_idx, flat in enumerate((flat0, flat1)):
            weights.append(unpack_tiles(flat.reshape(-1, ROWS, LANES), num_tokens, num_chans))
            hidden, cache = layer_forward(hidden, weights[layer_idx], f'f{layer_idx}')
            caches.append(cache)
        head_full = tiles_to_head(extra[:, :num_head], head_rows * GROUP)
        small_full = extra[:, num_head, 0].reshape(-1)
        loss_sum, d_hidden, g_head_w, g_small = head_step(hidden, labels, small_full, head_full, num_classes, global_b)

        head_blocks = head_to_tiles(g_head_w).reshape(GROUP, num_head, ROWS, LANES)
        g_small = jnp.pad(g_small, (0, small_len * GROUP - g_small.shape[0])).reshape(GROUP, 1, 1, small_len)
        small_blocks = jnp.pad(g_small, ((0, 0), (0, 0), (0, ROWS - 1), (0, 0)))
        packed = [None] * num_layers
        for layer_idx in reversed(range(num_layers)):
            d_hidden, grads = layer_backward(d_hidden, weights[layer_idx], caches[layer_idx], f'b{layer_idx}')
            packed[layer_idx] = pack_tiles(grads, flat_len).reshape(flat0.shape)
        summed0, summed1 = scatter_grads(packed[0], packed[1], jnp.concatenate([head_blocks, small_blocks], axis=1), win_tiles)
        layer_g = jnp.stack([window_to_share(summed0, share_len), window_to_share(summed1[:win_tiles], share_len)])
        head_g = tiles_to_head(summed1[win_tiles:win_tiles + num_head], head_rows)[:, :num_classes]
        small_g = summed1[win_tiles + num_head, 0]

        sq_local = jnp.sum(jnp.square(layer_g)) + jnp.sum(jnp.square(head_g)) + jnp.sum(jnp.square(small_g))
        loss_total, sq_total = sum_over_devices([loss_sum, sq_local])
        loss_value = loss_total / global_b
        clip_scale = 1.0 / jnp.maximum(1.0, jnp.sqrt(sq_total))
        flat_pos = lax.axis_index(AXIS) * share_len + jnp.arange(share_len)
        layer_decay = jnp.where(flat_pos < mat_len, WEIGHT_DECAY, 0.0)[None, :]
        new_lp, new_lm, new_lv = adam_update(layer_p, layer_g * clip_scale, layer_m, layer_v, layer_decay)
        new_hw, new_hm, new_hv = adam_update(head_w, head_g * clip_scale, head_m, head_v, WEIGHT_DECAY)
        new_sp, new_sm, new_sv = adam_update(small_p, small_g * clip_scale, small_m, small_v, 0.0)
        return (loss_value, new_lp, new_hw, new_sp, new_lm, new_hm, new_sm, new_lv, new_hv, new_sv)

    return jax.shard_map(device_step, mesh=mesh, in_specs=in_specs, out_specs=out_specs, check_vma=False)
```

```python
import functools
import math
import jax
import jax.numpy as jnp
from jax import lax
from jax.experimental import pallas as pl
from jax.experimental.pallas import tpu as pltpu
from jax.sharding import PartitionSpec as P

LN_EPS = 1e-6
LEARN_RATE = 0.003
BETA_ONE = 0.9
BETA_TWO = 0.999
ADAM_EPS = 1e-8
WEIGHT_DECAY = 0.03
ADAM_STEP = 10
AXIS = 'fsdp'
GROUP = 32
ROWS = 8
LANES = 128
TILE = ROWS * LANES
HEAD_PAD = 1024

def row_offset(share_rows):
    return (lax.axis_index(AXIS) * share_rows) % ROWS


def share_to_window(share):
    share_rows = share.shape[0] // LANES
    num_tiles = -(-(share_rows + ROWS - 2) // ROWS)
    window = jnp.zeros((num_tiles * ROWS, LANES), share.dtype)
    window = lax.dynamic_update_slice(window, share.reshape(share_rows, LANES), (row_offset(share_rows), 0))
    return window.reshape(num_tiles, ROWS, LANES)


def window_to_share(window, share_len):
    share_rows = share_len // LANES
    rows = window.reshape(-1, LANES)
    return lax.dynamic_slice(rows, (row_offset(share_rows), 0), (share_rows, LANES)).reshape(share_len)


def piece_shapes(num_tokens, num_chans):
    tok_hid = num_chans // 2
    ch_hid = 4 * num_chans
    return [(num_tokens, tok_hid), (tok_hid, num_tokens), (num_chans, ch_hid), (ch_hid, num_chans), (num_chans,), (num_chans,), (tok_hid,), (num_tokens,), (num_chans,), (num_chans,), (ch_hid,), (num_chans,)]


def unpack_tiles(tiles, num_tokens, num_chans):
    pieces = []
    start = 0
    shapes = piece_shapes(num_tokens, num_chans)
    for shape_one in shapes[:4]:
        count = math.prod(shape_one) // TILE
        pieces.append(tiles[start:start + count].reshape(shape_one))
        start = start + count
    flat = tiles[start:].reshape(-1)
    start = 0
    for shape_one in shapes[4:]:
        pieces.append(flat[start:start + shape_one[0]])
        start = start + shape_one[0]
    return pieces


def head_to_tiles(head):
    rows = head.shape[0]
    head = jnp.pad(head, ((0, 0), (0, HEAD_PAD - head.shape[1])))
    return head.reshape(rows // ROWS, ROWS, HEAD_PAD // LANES, LANES).transpose(0, 2, 1, 3).reshape(-1, ROWS, LANES)


def tiles_to_head(tiles, rows):
    tiles = tiles.reshape(rows // ROWS, HEAD_PAD // LANES, ROWS, LANES)
    return tiles.transpose(0, 2, 1, 3).reshape(rows, HEAD_PAD)


MASK_CORE, MASK_X, MASK_Y, MASK_Z = 1, 2, 4, 8
PARTNERS = (MASK_CORE, MASK_X, MASK_Y, MASK_Z, 2 * MASK_Z, 3 * MASK_Z)
PERIOD = 4


class Peers:
    def __init__(self, me):
        self.bits = []
        for bit in range(5):
            val = lax.rem(lax.div(me, 1 << bit), 2)
            self.bits.append((val, 1 - val))
        self.known = {}

    def split(self, rel):
        if rel not in self.known:
            vals = [self.bits[bit][(rel >> bit) & 1] for bit in range(5)]
            pos = vals[0] + 2 * vals[1]
            group = vals[2] + 2 * vals[3] + 4 * vals[4]
            self.known[rel] = (group * PERIOD + pos, group, pos)
        return self.known[rel]

    def device(self, rel):
        return self.split(rel)[0]


def meet_partners(peers):
    barrier = pltpu.get_barrier_semaphore()
    for mask in PARTNERS:
        pl.semaphore_signal(barrier, inc=1, device_id=(peers.device(mask),), device_id_type=pl.DeviceIdType.MESH)
    pl.semaphore_wait(barrier, len(PARTNERS))


def gather_kernel(inner0_ref, inner1_ref, misc_ref, flat0_ref, flat1_ref, extra_ref, misc_all, bound, local_sems, send_sems, recv_sems):
    peers = Peers(lax.axis_index(AXIS))
    inner = inner0_ref.shape[0]
    stride = inner + 1
    own_refs = (inner0_ref, inner1_ref, misc_ref)
    colours = ((MASK_Y, MASK_X), (MASK_X, MASK_Y), (MASK_X, MASK_Y))

    def place(arr, rel):
        dev, group, pos = peers.split(rel)
        if arr == 2:
            return misc_all.at[dev]
        flat = (flat0_ref, flat1_ref)[arr]
        return flat.at[group, pl.ds(stride * pos + 1, inner)]

    own_copies = [pltpu.make_async_copy(own_refs[arr], place(arr, 0), local_sems.at[arr]) for arr in range(3)]
    for copy in own_copies:
        copy.start()
    meet_partners(peers)
    sends = []

    def send(arr, rel, mask):
        here = place(arr, rel)
        copy = pltpu.make_async_remote_copy(
            src_ref=own_refs[arr] if rel == 0 else here, dst_ref=here,
            send_sem=send_sems.at[arr, rel ^ mask], recv_sem=recv_sems.at[arr, rel ^ mask],
            device_id=(peers.device(mask),), device_id_type=pl.DeviceIdType.MESH)
        copy.start()
        sends.append(copy)

    def receive(arr, rel):
        here = place(arr, rel)
        pltpu.make_async_remote_copy(
            src_ref=here, dst_ref=here, send_sem=send_sems.at[arr, rel], recv_sem=recv_sems.at[arr, rel],
            device_id=(peers.device(0),), device_id_type=pl.DeviceIdType.MESH).wait_recv()

    for mask_pos in range(6):
        for arr in range(3):
            first, second = colours[arr]
            send(arr, 0, (MASK_Z, first, second, 2 * MASK_Z, 3 * MASK_Z, MASK_CORE)[mask_pos])
    for dist, use_first, use_second in ((0, 1, 0), (1, 0, 0), (0, 0, 1), (1, 1, 0), (0, 1, 1), (2, 0, 0), (1, 0, 1), (2, 1, 0),
                                        (1, 1, 1), (3, 0, 0), (2, 0, 1), (3, 1, 0), (2, 1, 1), (3, 0, 1), (3, 1, 1)):
        for arr in range(3):
            first, second = colours[arr]
            rel = dist * MASK_Z + use_first * first + use_second * second
            receive(arr, rel)
            if not use_second:
                if not use_first:
                    send(arr, rel, first)
                send(arr, rel, second)
            send(arr, rel, MASK_CORE)
    for rel in range(MASK_CORE, GROUP, 2):
        for arr in range(3):
            receive(arr, rel)
    for copy in own_copies:
        copy.wait()
    for copy in sends:
        copy.wait_send()

    for layer_idx in range(2):
        for group in range(GROUP // PERIOD):
            for pos in range(PERIOD + 1):
                tile = None
                if pos < PERIOD:
                    tile = misc_all[group * PERIOD + pos, 2 * layer_idx]
                if pos > 0:
                    left = misc_all[group * PERIOD + pos - 1, 2 * layer_idx + 1]
                    tile = left if tile is None else tile + left
                bound[layer_idx, pos, group, 0] = tile
    extra_ref[...] = misc_all[:, 4:]
    edges = []
    for layer_idx in range(2):
        flat = (flat0_ref, flat1_ref)[layer_idx]
        for pos in range(PERIOD + 1):
            edges.append(pltpu.make_async_copy(bound.at[layer_idx, pos], flat.at[:, pl.ds(stride * pos, 1)], local_sems.at[3 + layer_idx * (PERIOD + 1) + pos]))
    for copy in edges:
        copy.start()
    for copy in edges:
        copy.wait()


def gather_shares(window0, window1, extra):
    num_tiles = window0.shape[0]
    num_extra = extra.shape[0]
    inner = num_tiles - 2
    misc = jnp.concatenate([window0[:1], window0[-1:], window1[:1], window1[-1:], extra], axis=0)
    flat = (GROUP // PERIOD, PERIOD * (num_tiles - 1) + 1, ROWS, LANES)
    vmem = pl.BlockSpec(memory_space=pltpu.VMEM)
    hbm = pl.BlockSpec(memory_space=pl.ANY)
    dtype = window0.dtype
    return pl.pallas_call(
        gather_kernel,
        out_shape=(jax.ShapeDtypeStruct(flat, dtype), jax.ShapeDtypeStruct(flat, dtype), jax.ShapeDtypeStruct((GROUP, num_extra, ROWS, LANES), dtype)),
        in_specs=[vmem] * 3,
        out_specs=(hbm, hbm, vmem),
        scratch_shapes=[
            pltpu.VMEM((GROUP, num_extra + 4, ROWS, LANES), dtype),
            pltpu.VMEM((2, PERIOD + 1, GROUP // PERIOD, 1, ROWS, LANES), dtype),
            pltpu.SemaphoreType.DMA((3 + 2 * (PERIOD + 1),)),
            pltpu.SemaphoreType.DMA((3, GROUP)),
            pltpu.SemaphoreType.DMA((3, GROUP)),
        ],
        compiler_params=pltpu.CompilerParams(collective_id=1, has_side_effects=True),
        name='gather_shares',
    )(window0[1:-1], window1[1:-1], misc)


def scatter_kernel(grad0_ref, grad1_ref, extra_ref, out0_ref, out1_ref, own0, own1, core0, core1, first0, first1, second0, second1, far0, far1,
                   load_sems, send_sems, core_sems, first_sems, second_sems, far_sems):
    peers = Peers(lax.axis_index(AXIS))
    num_tiles = out0_ref.shape[0]
    num_extra = extra_ref.shape[1]
    own, near, first_in, second_in, far_in = (own0, own1), (core0, core1), (first0, first1), (second0, second1), (far0, far1)
    colours = ((MASK_X, MASK_Y), (MASK_Y, MASK_X))
    dists = (3, 2, 1, 0)
    sends = []

    def source(part, rel):
        dev, group, pos = peers.split(rel)
        if part == 2:
            return extra_ref.at[dev]
        grad = (grad0_ref, grad1_ref)[part]
        return grad.at[group, pl.ds((num_tiles - 1) * pos, num_tiles)]

    def slot(part, buffers, pos):
        if part == 2:
            return buffers[1].at[pos, pl.ds(num_tiles, num_extra)]
        return buffers[part].at[pos, pl.ds(0, num_tiles)]

    def post(src, dst, send_sem, recv_sem, mask):
        copy = pltpu.make_async_remote_copy(src_ref=src, dst_ref=dst, send_sem=send_sem, recv_sem=recv_sem,
                                            device_id=(peers.device(mask),), device_id_type=pl.DeviceIdType.MESH)
        copy.start()
        sends.append(copy)

    def expect(dst, send_sem, recv_sem):
        pltpu.make_async_remote_copy(src_ref=dst, dst_ref=dst, send_sem=send_sem, recv_sem=recv_sem,
                                     device_id=(peers.device(0),), device_id_type=pl.DeviceIdType.MESH).wait_recv()

    def targets(dist):
        return [(dist * 4 + pos, dist * MASK_Z + pos * MASK_X) for pos in (3, 2, 1, 0)]

    loads = {}
    for dist in dists:
        for pos, rel in targets(dist):
            for part in range(3):
                loads[part, pos] = pltpu.make_async_copy(source(part, rel), slot(part, own, pos), load_sems.at[part, pos])
                loads[part, pos].start()
    meet_partners(peers)
    for dist in dists:
        for pos, rel in targets(dist):
            for part in range(3):
                post(source(part, rel | MASK_CORE), slot(part, near, pos), send_sems.at[part, pos], core_sems.at[part, pos], MASK_CORE)

    def fold_core(dist):
        for pos, rel in targets(dist):
            for part in range(3):
                loads[part, pos].wait()
                expect(slot(part, near, pos), send_sems.at[part, pos], core_sems.at[part, pos])
            for side in range(2):
                own[side][pos] += near[side][pos]
        for side in range(2):
            mask, other = colours[side]
            for which in (1, 0):
                pos = dist * 4 + (mask + which * other) // MASK_X
                index = dist * 2 + which
                post(own[side].at[pos], first_in[side].at[index], send_sems.at[3 + side, index], first_sems.at[side, index], mask)

    def fold_first(dist):
        for side in range(2):
            mask, other = colours[side]
            for which in (1, 0):
                pos = dist * 4 + which * other // MASK_X
                index = dist * 2 + which
                expect(first_in[side].at[index], send_sems.at[3 + side, index], first_sems.at[side, index])
                own[side][pos] += first_in[side][index]
        for side in range(2):
            mask, other = colours[side]
            post(own[side].at[dist * 4 + other // MASK_X], second_in[side].at[dist], send_sems.at[3 + side, 8 + dist], second_sems.at[side, dist], other)

    def fold_second(dist):
        for side in range(2):
            expect(second_in[side].at[dist], send_sems.at[3 + side, 8 + dist], second_sems.at[side, dist])
            own[side][dist * 4] += second_in[side][dist]
        if dist:
            for side in range(2):
                post(own[side].at[dist * 4], far_in[side].at[dist - 1], send_sems.at[3 + side, 12 + dist], far_sems.at[side, dist - 1], dist * MASK_Z)

    fold_core(3)
    fold_core(2)
    fold_first(3)
    fold_core(1)
    fold_first(2)
    fold_second(3)
    fold_core(0)
    fold_first(1)
    fold_second(2)
    fold_first(0)
    fold_second(1)
    fold_second(0)
    for side in range(2):
        total = own[side][0]
        for dist in (3, 2, 1):
            expect(far_in[side].at[dist - 1], send_sems.at[3 + side, 12 + dist], far_sems.at[side, dist - 1])
            total = total + far_in[side][dist - 1]
        (out0_ref, out1_ref)[side][...] = total
    for copy in sends:
        copy.wait_send()


def scatter_grads(grad0, grad1, extra, num_tiles):
    num_extra = extra.shape[1]
    sizes = (num_tiles, num_tiles + num_extra)
    vmem = pl.BlockSpec(memory_space=pltpu.VMEM)
    hbm = pl.BlockSpec(memory_space=pl.ANY)

    def buffers(count):
        return [pltpu.VMEM((count, size, ROWS, LANES), jnp.float32) for size in sizes]

    return pl.pallas_call(
        scatter_kernel,
        out_shape=tuple(jax.ShapeDtypeStruct((size, ROWS, LANES), jnp.float32) for size in sizes),
        in_specs=[hbm] * 3,
        out_specs=(vmem, vmem),
        scratch_shapes=buffers(16) + buffers(16) + buffers(8) + buffers(4) + buffers(3) + [
            pltpu.SemaphoreType.DMA((3, 16)),
            pltpu.SemaphoreType.DMA((5, 16)),
            pltpu.SemaphoreType.DMA((3, 16)),
            pltpu.SemaphoreType.DMA((2, 8)),
            pltpu.SemaphoreType.DMA((2, 4)),
            pltpu.SemaphoreType.DMA((2, 3)),
        ],
        compiler_params=pltpu.CompilerParams(collective_id=2, has_side_effects=True),
        name='scatter_grads',
    )(grad0, grad1, extra)


NT_DIMS = (((1,), (1,)), ((), ()))
NN_DIMS = (((1,), (0,)), ((), ()))
HID_CHUNK = 512


def mlp_grad_kernel(d_out_ref, act_ref, slope_ref, normed_ref, w1_ref, w2_ref, d_normed_ref, bias_ref, flat_ref, acc1, acc2, staged, sems, *, row1, row2):
    step = pl.program_id(0)
    chans, hid = acc1.shape

    @pl.when(step == 0)
    def _():
        acc1[...] = jnp.zeros_like(acc1)
        acc2[...] = jnp.zeros_like(acc2)
        bias_ref[...] = jnp.zeros_like(bias_ref)

    d_out = d_out_ref[...]
    d_out_t = d_out.T
    normed_t = normed_ref[...].T
    d_normed = None
    for start in range(0, hid, HID_CHUNK):
        cols = pl.ds(start, HID_CHUNK)
        d_act = lax.dot_general(d_out, w2_ref[cols, :], NT_DIMS, preferred_element_type=jnp.float32)
        acc2[:, cols] += lax.dot_general(d_out_t, act_ref[:, cols], NN_DIMS, preferred_element_type=jnp.float32)
        d_hid = d_act.astype(jnp.bfloat16).astype(jnp.float32) * slope_ref[:, cols]
        bias_ref[:, cols] += jnp.sum(d_hid.reshape(-1, ROWS, HID_CHUNK), axis=0)
        d_hid_bf = d_hid.astype(jnp.bfloat16)
        acc1[:, cols] += lax.dot_general(normed_t, d_hid_bf, NN_DIMS, preferred_element_type=jnp.float32)
        part = lax.dot_general(d_hid_bf, w1_ref[:, cols], NT_DIMS, preferred_element_type=jnp.float32)
        d_normed = part if d_normed is None else d_normed + part
    d_normed_ref[...] = d_normed.astype(d_normed_ref.dtype)

    @pl.when(step == pl.num_programs(0) - 1)
    def _():
        wide = hid // LANES
        for col in range(wide):
            staged[0, pl.ds(col, chans, stride=wide), :] = acc1[:, col * LANES:(col + 1) * LANES]
        first = pltpu.make_async_copy(staged.at[0], flat_ref.at[pl.ds(row1, chans * wide)], sems.at[0])
        first.start()
        narrow = chans // LANES
        for col in range(narrow):
            staged[1, pl.ds(col, hid, stride=narrow), :] = acc2[col * LANES:(col + 1) * LANES, :].T
        second = pltpu.make_async_copy(staged.at[1], flat_ref.at[pl.ds(row2, chans * wide)], sems.at[1])
        second.start()
        first.wait()
        second.wait()


def mlp_grad(d_out, act, slope, normed, w1, w2, flat_rows, row1, row2, block):
    tokens, chans = d_out.shape
    hid = act.shape[1]

    def by_block(width):
        return pl.BlockSpec((block, width), lambda step: (step, 0))

    def whole(shape):
        return pl.BlockSpec(shape, lambda step: (0, 0), pipeline_mode=pl.Buffered(1))

    mat_rows = chans * hid // LANES
    return pl.pallas_call(
        functools.partial(mlp_grad_kernel, row1=row1, row2=row2),
        grid=(tokens // block,),
        out_shape=(
            jax.ShapeDtypeStruct((tokens, chans), jnp.bfloat16),
            jax.ShapeDtypeStruct((ROWS, hid), jnp.float32),
            jax.ShapeDtypeStruct((flat_rows, LANES), jnp.float32),
        ),
        in_specs=[by_block(chans), by_block(hid), by_block(hid), by_block(chans), whole(w1.shape), whole(w2.shape)],
        out_specs=(by_block(chans), pl.BlockSpec((ROWS, hid), lambda step: (0, 0)), pl.BlockSpec(memory_space=pl.ANY)),
        scratch_shapes=[
            pltpu.VMEM((chans, hid), jnp.float32),
            pltpu.VMEM((chans, hid), jnp.float32),
            pltpu.VMEM((2, mat_rows, LANES), jnp.float32),
            pltpu.SemaphoreType.DMA((2,)),
        ],
        compiler_params=pltpu.CompilerParams(dimension_semantics=('arbitrary',), vmem_limit_bytes=60 * 1024 * 1024),
        cost_estimate=pl.CostEstimate(flops=8 * tokens * chans * hid, bytes_accessed=6 * tokens * hid + 6 * tokens * chans + 12 * chans * hid, transcendentals=0),
        name='mlp_grad',
    )(d_out, act, slope, normed, w1, w2)


def sum_kernel(x_ref, out_ref, held, local_sem, send_sems, recv_sems):
    me = lax.axis_index(AXIS)
    barrier = pltpu.get_barrier_semaphore()
    for step in range(1, GROUP):
        pl.semaphore_signal(barrier, inc=1, device_id=((me + step) % GROUP,), device_id_type=pl.DeviceIdType.MESH)
    own = pltpu.make_async_copy(x_ref, held.at[me], local_sem)
    own.start()
    pl.semaphore_wait(barrier, GROUP - 1)
    sends = []
    for step in range(1, GROUP):
        copy = pltpu.make_async_remote_copy(
            src_ref=x_ref, dst_ref=held.at[me], send_sem=send_sems.at[step], recv_sem=recv_sems.at[me],
            device_id=((me + step) % GROUP,), device_id_type=pl.DeviceIdType.MESH)
        copy.start()
        sends.append(copy)
    own.wait()
    for step in range(1, GROUP):
        peer = (me + step) % GROUP
        pltpu.make_async_remote_copy(
            src_ref=x_ref, dst_ref=held.at[peer], send_sem=send_sems.at[step], recv_sem=recv_sems.at[peer],
            device_id=(peer,), device_id_type=pl.DeviceIdType.MESH).wait_recv()
    for copy in sends:
        copy.wait_send()
    out_ref[...] = jnp.sum(held[...], axis=0)


def sum_over_devices(values):
    block = jnp.zeros((ROWS, LANES), jnp.float32)
    for pos, value in enumerate(values):
        block = block.at[0, pos].set(value)
    total = pl.pallas_call(
        sum_kernel,
        out_shape=jax.ShapeDtypeStruct((ROWS, LANES), jnp.float32),
        in_specs=[pl.BlockSpec(memory_space=pltpu.VMEM)],
        out_specs=pl.BlockSpec(memory_space=pltpu.VMEM),
        scratch_shapes=[
            pltpu.VMEM((GROUP, ROWS, LANES), jnp.float32),
            pltpu.SemaphoreType.DMA,
            pltpu.SemaphoreType.DMA((GROUP,)),
            pltpu.SemaphoreType.DMA((GROUP,)),
        ],
        compiler_params=pltpu.CompilerParams(collective_id=0, has_side_effects=True),
        name='sum_over_devices',
    )(block)
    return [total[0, pos] for pos in range(len(values))]


def layer_norm(x_in, ln_gain, ln_shift):
    x_f = x_in.astype(jnp.float32)
    mean_val = jnp.mean(x_f, axis=-1, keepdims=True)
    var_val = jnp.mean(jnp.square(x_f - mean_val), axis=-1, keepdims=True)
    normed = (x_f - mean_val) * lax.rsqrt(var_val + LN_EPS)
    return (normed * ln_gain.astype(jnp.float32) + ln_shift.astype(jnp.float32)).astype(jnp.bfloat16)


def gelu_both(hidden):
    scale = math.sqrt(2.0 / math.pi)
    square = hidden * hidden
    tanh_val = jnp.tanh(hidden * (scale + (scale * 0.044715) * square))
    cdf = 0.5 + 0.5 * tanh_val
    slope = cdf + (0.5 * hidden) * (1.0 - tanh_val * tanh_val) * (scale + (3.0 * scale * 0.044715) * square)
    return (hidden * cdf).astype(jnp.bfloat16), slope


def norm_grad(x_in, ln_gain, ln_shift, d_normed):
    _, pullback = jax.vjp(layer_norm, x_in, ln_gain.astype(jnp.float32), ln_shift.astype(jnp.float32))
    d_x, d_gain, d_shift = pullback(d_normed.astype(jnp.bfloat16))
    return d_x.astype(jnp.float32), d_gain, d_shift


def scoped(tag, spec, lhs, rhs, **kwargs):
    with jax.named_scope(tag):
        return jnp.einsum(spec, lhs, rhs, **kwargs)


def layer_forward(x_in, weights, tag):
    w_tok1, w_tok2, w_ch1, w_ch2, ln1_g, ln1_b, b_tok1, b_tok2, ln2_g, ln2_b, b_ch1, b_ch2 = weights
    normed = layer_norm(x_in, ln1_g, ln1_b)
    hid_tok = scoped(tag + '_tok1', 'bsc,sj->bcj', normed, w_tok1, preferred_element_type=jnp.float32) + b_tok1.astype(jnp.float32)
    act_tok, slope_tok = gelu_both(hid_tok)
    with jax.named_scope(tag + '_tok2'):
        tok_out = jnp.einsum('bcj,js->bsc', act_tok, w_tok2, preferred_element_type=jnp.float32) + b_tok2.astype(jnp.float32)[:, None]
        after_tok = (x_in.astype(jnp.float32) + tok_out).astype(jnp.bfloat16)
    normed2 = layer_norm(after_tok, ln2_g, ln2_b)
    hid_ch = scoped(tag + '_ch1', 'bsc,cd->bsd', normed2, w_ch1, preferred_element_type=jnp.float32) + b_ch1.astype(jnp.float32)
    act_ch, slope_ch = gelu_both(hid_ch)
    with jax.named_scope(tag + '_ch2'):
        ch_out = jnp.einsum('bsd,dc->bsc', act_ch, w_ch2, preferred_element_type=jnp.float32) + b_ch2.astype(jnp.float32)
        layer_out = (after_tok.astype(jnp.float32) + ch_out).astype(jnp.bfloat16)
    return layer_out, (x_in, normed, slope_tok, act_tok, after_tok, normed2, slope_ch, act_ch)


def layer_backward(d_out, weights, cache, tag, flat_len):
    num_tokens, num_chans = d_out.shape[1:]
    w_tok1, w_tok2, w_ch1, w_ch2, ln1_g, ln1_b, b_tok1, b_tok2, ln2_g, ln2_b, b_ch1, b_ch2 = weights
    x_in, normed, slope_tok, act_tok, after_tok, normed2, slope_ch, act_ch = cache
    d_out_bf = d_out.astype(jnp.bfloat16)
    g_b_ch2 = jnp.sum(d_out, axis=(0, 1))
    tokens = d_out.shape[0] * num_tokens
    mat_tiles = [math.prod(shape_one) // LANES for shape_one in piece_shapes(num_tokens, num_chans)[:4]]
    row1 = mat_tiles[0] + mat_tiles[1]
    d_normed2, bias_rows, flat_grad = mlp_grad(
        d_out_bf.reshape(tokens, num_chans), act_ch.reshape(tokens, -1), slope_ch.reshape(tokens, -1), normed2.reshape(tokens, num_chans),
        w_ch1, w_ch2, flat_len // LANES, row1, row1 + mat_tiles[2], tokens // 7)
    g_b_ch1 = jnp.sum(bias_rows, axis=0)
    d_normed2 = d_normed2.reshape(d_out.shape)
    with jax.named_scope(tag + '_ln2'):
        d_after_ln, g_ln2_g, g_ln2_b = norm_grad(after_tok, ln2_g, ln2_b, d_normed2)
    d_after = d_after_ln + d_out
    d_after_bf = d_after.astype(jnp.bfloat16)
    g_b_tok2 = jnp.sum(d_after, axis=(0, 2))
    g_w_tok2 = scoped(tag + '_gt2', 'bcj,bsc->js', act_tok, d_after_bf, preferred_element_type=jnp.float32)
    with jax.named_scope(tag + '_dtok'):
        d_act_tok = jnp.einsum('bsc,js->bcj', d_after_bf, w_tok2, preferred_element_type=jnp.float32)
        d_hid_tok = d_act_tok.astype(jnp.bfloat16).astype(jnp.float32) * slope_tok
        d_hid_tok_bf = d_hid_tok.astype(jnp.bfloat16)
        g_b_tok1 = jnp.sum(d_hid_tok, axis=(0, 1))
    g_w_tok1 = scoped(tag + '_gt1', 'bsc,bcj->sj', normed, d_hid_tok_bf, preferred_element_type=jnp.float32)
    d_normed = scoped(tag + '_dnt', 'bcj,sj->bsc', d_hid_tok_bf, w_tok1, preferred_element_type=jnp.float32)
    d_in_ln, g_ln1_g, g_ln1_b = norm_grad(x_in, ln1_g, ln1_b, d_normed)
    d_in = d_in_ln + d_after
    vectors = jnp.concatenate([g_ln1_g, g_ln1_b, g_b_tok1, g_b_tok2, g_ln2_g, g_ln2_b, g_b_ch1, g_b_ch2])
    last_row = row1 + mat_tiles[2] + mat_tiles[3]
    vectors = jnp.pad(vectors, (0, flat_len - last_row * LANES - vectors.shape[0])).reshape(-1, LANES)
    tok_rows = jnp.concatenate([g_w_tok1.reshape(-1, LANES), g_w_tok2.reshape(-1, LANES)], axis=0)
    flat_grad = lax.dynamic_update_slice(flat_grad, tok_rows, (0, 0))
    flat_grad = lax.dynamic_update_slice(flat_grad, vectors, (last_row, 0))
    return d_in, flat_grad


def head_step(hidden, labels, small_full, head_full, num_classes, global_b):
    num_tokens = hidden.shape[1]
    num_chans = hidden.shape[2]
    lnf_g = small_full[:num_chans]
    lnf_b = small_full[num_chans:2 * num_chans]
    head_b = small_full[2 * num_chans:2 * num_chans + num_classes]
    normed = layer_norm(hidden, lnf_g, lnf_b)
    pooled = (jnp.sum(normed, axis=1, dtype=jnp.float32) / num_tokens).astype(jnp.bfloat16)
    is_class = jnp.arange(HEAD_PAD)[None, :] < num_classes
    logits = jnp.dot(pooled, head_full, preferred_element_type=jnp.float32) + jnp.pad(head_b.astype(jnp.float32), (0, HEAD_PAD - num_classes))
    logits = jnp.where(is_class, logits, -jnp.inf)
    log_norm = jax.nn.logsumexp(logits, axis=-1)
    is_label = jnp.arange(HEAD_PAD)[None, :] == labels[:, None]
    picked = jnp.sum(jnp.where(is_label, logits, 0.0), axis=-1)
    loss_sum = jnp.sum(log_norm - picked)
    d_logits = (jnp.exp(logits - log_norm[:, None]) - is_label.astype(jnp.float32)) / global_b
    d_logits_bf = d_logits.astype(jnp.bfloat16)
    g_head_b = jnp.sum(d_logits, axis=0)[:num_classes]
    g_head_w = jnp.einsum('bc,bk->ck', pooled, d_logits_bf, preferred_element_type=jnp.float32)
    d_pooled = jnp.einsum('bk,ck->bc', d_logits_bf, head_full, preferred_element_type=jnp.float32)
    d_normed = jnp.broadcast_to((d_pooled / num_tokens)[:, None, :], normed.shape)
    d_hidden, g_lnf_g, g_lnf_b = norm_grad(hidden, lnf_g, lnf_b, d_normed)
    g_small = jnp.concatenate([g_lnf_g, g_lnf_b, g_head_b])
    return loss_sum, d_hidden, g_head_w, g_small


def adam_update(master, gradient, moment, second, decay_rate):
    moment_new = BETA_ONE * moment + (1.0 - BETA_ONE) * gradient
    second_new = BETA_TWO * second + (1.0 - BETA_TWO) * gradient * gradient
    m_hat = moment_new / (1.0 - BETA_ONE ** ADAM_STEP)
    v_hat = second_new / (1.0 - BETA_TWO ** ADAM_STEP)
    master_new = master - LEARN_RATE * (m_hat / (jnp.sqrt(v_hat) + ADAM_EPS) + decay_rate * master)
    return master_new, moment_new, second_new


def solution(mesh):
    row_spec = P(AXIS)
    layer_spec = P(None, AXIS)
    in_specs = (row_spec, row_spec, layer_spec, row_spec, row_spec, layer_spec, row_spec, row_spec, layer_spec, row_spec, row_spec)
    out_specs = (P(),) + in_specs[2:]

    def device_step(act_in, labels, layer_p, head_w, small_p, layer_m, head_m, small_m, layer_v, head_v, small_v):
        local_b, num_tokens, num_chans = act_in.shape
        global_b = local_b * GROUP
        num_layers, share_len = layer_p.shape
        flat_len = share_len * GROUP
        head_rows, num_classes = head_w.shape
        small_len = small_p.shape[0]
        mat_len = 2 * num_tokens * (num_chans // 2) + 8 * num_chans * num_chans

        windows = [share_to_window(layer_p[layer_idx].astype(jnp.bfloat16)) for layer_idx in range(num_layers)]
        win_tiles = windows[0].shape[0]
        head_tiles = head_to_tiles(head_w.astype(jnp.bfloat16))
        small_tile = jnp.pad(small_p.astype(jnp.bfloat16).reshape(1, 1, small_len), ((0, 0), (0, ROWS - 1), (0, 0)))
        num_head = head_tiles.shape[0]
        flat0, flat1, extra = gather_shares(windows[0], windows[1], jnp.concatenate([head_tiles, small_tile], axis=0))

        weights = []
        caches = []
        hidden = act_in
        for layer_idx, flat in enumerate((flat0, flat1)):
            weights.append(unpack_tiles(flat.reshape(-1, ROWS, LANES), num_tokens, num_chans))
            hidden, cache = layer_forward(hidden, weights[layer_idx], f'f{layer_idx}')
            caches.append(cache)
        head_full = tiles_to_head(extra[:, :num_head], head_rows * GROUP)
        small_full = extra[:, num_head, 0].reshape(-1)
        loss_sum, d_hidden, g_head_w, g_small = head_step(hidden, labels, small_full, head_full, num_classes, global_b)

        head_blocks = head_to_tiles(g_head_w).reshape(GROUP, num_head, ROWS, LANES)
        g_small = jnp.pad(g_small, (0, small_len * GROUP - g_small.shape[0])).reshape(GROUP, 1, 1, small_len)
        small_blocks = jnp.pad(g_small, ((0, 0), (0, 0), (0, ROWS - 1), (0, 0)))
        packed = [None] * num_layers
        for layer_idx in reversed(range(num_layers)):
            d_hidden, flat_grad = layer_backward(d_hidden, weights[layer_idx], caches[layer_idx], f'b{layer_idx}', flat_len)
            packed[layer_idx] = flat_grad.reshape(flat0.shape)
        summed0, summed1 = scatter_grads(packed[0], packed[1], jnp.concatenate([head_blocks, small_blocks], axis=1), win_tiles)
        layer_g = jnp.stack([window_to_share(summed0, share_len), window_to_share(summed1[:win_tiles], share_len)])
        head_g = tiles_to_head(summed1[win_tiles:win_tiles + num_head], head_rows)[:, :num_classes]
        small_g = summed1[win_tiles + num_head, 0]

        sq_local = jnp.sum(jnp.square(layer_g)) + jnp.sum(jnp.square(head_g)) + jnp.sum(jnp.square(small_g))
        loss_total, sq_total = sum_over_devices([loss_sum, sq_local])
        loss_value = loss_total / global_b
        clip_scale = 1.0 / jnp.maximum(1.0, jnp.sqrt(sq_total))
        flat_pos = lax.axis_index(AXIS) * share_len + jnp.arange(share_len)
        layer_decay = jnp.where(flat_pos < mat_len, WEIGHT_DECAY, 0.0)[None, :]
        new_lp, new_lm, new_lv = adam_update(layer_p, layer_g * clip_scale, layer_m, layer_v, layer_decay)
        new_hw, new_hm, new_hv = adam_update(head_w, head_g * clip_scale, head_m, head_v, WEIGHT_DECAY)
        new_sp, new_sm, new_sv = adam_update(small_p, small_g * clip_scale, small_m, small_v, 0.0)
        return (loss_value, new_lp, new_hw, new_sp, new_lm, new_hm, new_sm, new_lv, new_hv, new_sv)

    return jax.shard_map(device_step, mesh=mesh, in_specs=in_specs, out_specs=out_specs, check_vma=False)
```

```python
import functools
import math
import jax
import jax.numpy as jnp
from jax import lax
from jax.experimental import pallas as pl
from jax.experimental.pallas import tpu as pltpu
from jax.sharding import PartitionSpec as P

LN_EPS = 1e-6
LEARN_RATE = 0.003
BETA_ONE = 0.9
BETA_TWO = 0.999
ADAM_EPS = 1e-8
WEIGHT_DECAY = 0.03
ADAM_STEP = 10
AXIS = 'fsdp'
GROUP = 32
ROWS = 8
LANES = 128
TILE = ROWS * LANES
HEAD_PAD = 1024
IMAGE_ROWS = 8

def row_offset(share_rows):
    return (lax.axis_index(AXIS) * share_rows) % ROWS


def share_to_window(share):
    share_rows = share.shape[0] // LANES
    num_tiles = -(-(share_rows + ROWS - 2) // ROWS)
    window = jnp.zeros((num_tiles * ROWS, LANES), share.dtype)
    window = lax.dynamic_update_slice(window, share.reshape(share_rows, LANES), (row_offset(share_rows), 0))
    return window.reshape(num_tiles, ROWS, LANES)


def window_to_share(window, share_len):
    share_rows = share_len // LANES
    rows = window.reshape(-1, LANES)
    return lax.dynamic_slice(rows, (row_offset(share_rows), 0), (share_rows, LANES)).reshape(share_len)


def piece_shapes(num_tokens, num_chans):
    tok_hid = num_chans // 2
    ch_hid = 4 * num_chans
    return [(num_tokens, tok_hid), (tok_hid, num_tokens), (num_chans, ch_hid), (ch_hid, num_chans), (num_chans,), (num_chans,), (tok_hid,), (num_tokens,), (num_chans,), (num_chans,), (ch_hid,), (num_chans,)]


def pad_tokens(val, axis, num_tokens):
    widths = [(0, 0)] * val.ndim
    widths[axis] = (0, -num_tokens % IMAGE_ROWS)
    return jnp.pad(val, widths)


def unpack_tiles(tiles, num_tokens, num_chans):
    pieces = []
    start = 0
    shapes = piece_shapes(num_tokens, num_chans)
    for shape_one in shapes[:4]:
        count = math.prod(shape_one) // TILE
        pieces.append(tiles[start:start + count].reshape(shape_one))
        start = start + count
    flat = tiles[start:].reshape(-1)
    start = 0
    for shape_one in shapes[4:]:
        pieces.append(flat[start:start + shape_one[0]])
        start = start + shape_one[0]
    pieces[0] = pad_tokens(pieces[0], 0, num_tokens)
    pieces[1] = pad_tokens(pieces[1], 1, num_tokens)
    pieces[2], pieces[3] = lax.optimization_barrier((pieces[2], pieces[3]))
    pieces[7] = pad_tokens(pieces[7], 0, num_tokens)
    return pieces


def head_to_tiles(head):
    rows = head.shape[0]
    head = jnp.pad(head, ((0, 0), (0, HEAD_PAD - head.shape[1])))
    return head.reshape(rows // ROWS, ROWS, HEAD_PAD // LANES, LANES).transpose(0, 2, 1, 3).reshape(-1, ROWS, LANES)


def tiles_to_head(tiles, rows):
    tiles = tiles.reshape(rows // ROWS, HEAD_PAD // LANES, ROWS, LANES)
    return tiles.transpose(0, 2, 1, 3).reshape(rows, HEAD_PAD)


MASK_CORE, MASK_X, MASK_Y, MASK_Z = 1, 2, 4, 8
PARTNERS = (MASK_CORE, MASK_X, MASK_Y, MASK_Z, 2 * MASK_Z, 3 * MASK_Z)
PERIOD = 4


class Peers:
    def __init__(self, me):
        self.bits = []
        for bit in range(5):
            val = lax.rem(lax.div(me, 1 << bit), 2)
            self.bits.append((val, 1 - val))
        self.known = {}

    def split(self, rel):
        if rel not in self.known:
            vals = [self.bits[bit][(rel >> bit) & 1] for bit in range(5)]
            pos = vals[0] + 2 * vals[1]
            group = vals[2] + 2 * vals[3] + 4 * vals[4]
            self.known[rel] = (group * PERIOD + pos, group, pos)
        return self.known[rel]

    def device(self, rel):
        return self.split(rel)[0]


def meet_partners(peers):
    barrier = pltpu.get_barrier_semaphore()
    for mask in PARTNERS:
        pl.semaphore_signal(barrier, inc=1, device_id=(peers.device(mask),), device_id_type=pl.DeviceIdType.MESH)
    pl.semaphore_wait(barrier, len(PARTNERS))


def gather_kernel(inner0_ref, inner1_ref, misc_ref, flat0_ref, flat1_ref, extra_ref, misc_all, bound, local_sems, send_sems, recv_sems):
    peers = Peers(lax.axis_index(AXIS))
    inner = inner0_ref.shape[0]
    stride = inner + 1
    own_refs = (inner0_ref, inner1_ref, misc_ref)
    colours = ((MASK_Y, MASK_X), (MASK_X, MASK_Y), (MASK_X, MASK_Y))

    def place(arr, rel):
        dev, group, pos = peers.split(rel)
        if arr == 2:
            return misc_all.at[dev]
        flat = (flat0_ref, flat1_ref)[arr]
        return flat.at[group, pl.ds(stride * pos + 1, inner)]

    own_copies = [pltpu.make_async_copy(own_refs[arr], place(arr, 0), local_sems.at[arr]) for arr in range(3)]
    for copy in own_copies:
        copy.start()
    meet_partners(peers)
    sends = []

    def send(arr, rel, mask):
        here = place(arr, rel)
        copy = pltpu.make_async_remote_copy(
            src_ref=own_refs[arr] if rel == 0 else here, dst_ref=here,
            send_sem=send_sems.at[arr, rel ^ mask], recv_sem=recv_sems.at[arr, rel ^ mask],
            device_id=(peers.device(mask),), device_id_type=pl.DeviceIdType.MESH)
        copy.start()
        sends.append(copy)

    def receive(arr, rel):
        here = place(arr, rel)
        pltpu.make_async_remote_copy(
            src_ref=here, dst_ref=here, send_sem=send_sems.at[arr, rel], recv_sem=recv_sems.at[arr, rel],
            device_id=(peers.device(0),), device_id_type=pl.DeviceIdType.MESH).wait_recv()

    for mask_pos in range(6):
        for arr in range(3):
            first, second = colours[arr]
            send(arr, 0, (MASK_Z, first, second, 2 * MASK_Z, 3 * MASK_Z, MASK_CORE)[mask_pos])
    for dist, use_first, use_second in ((0, 1, 0), (1, 0, 0), (0, 0, 1), (1, 1, 0), (0, 1, 1), (2, 0, 0), (1, 0, 1), (2, 1, 0),
                                        (1, 1, 1), (3, 0, 0), (2, 0, 1), (3, 1, 0), (2, 1, 1), (3, 0, 1), (3, 1, 1)):
        for arr in range(3):
            first, second = colours[arr]
            rel = dist * MASK_Z + use_first * first + use_second * second
            receive(arr, rel)
            if not use_second:
                if not use_first:
                    send(arr, rel, first)
                send(arr, rel, second)
            send(arr, rel, MASK_CORE)
    for rel in range(MASK_CORE, GROUP, 2):
        for arr in range(3):
            receive(arr, rel)
    for copy in own_copies:
        copy.wait()
    for copy in sends:
        copy.wait_send()

    for layer_idx in range(2):
        for group in range(GROUP // PERIOD):
            for pos in range(PERIOD + 1):
                tile = None
                if pos < PERIOD:
                    tile = misc_all[group * PERIOD + pos, 2 * layer_idx]
                if pos > 0:
                    left = misc_all[group * PERIOD + pos - 1, 2 * layer_idx + 1]
                    tile = left if tile is None else tile + left
                bound[layer_idx, pos, group, 0] = tile
    extra_ref[...] = misc_all[:, 4:]
    edges = []
    for layer_idx in range(2):
        flat = (flat0_ref, flat1_ref)[layer_idx]
        for pos in range(PERIOD + 1):
            edges.append(pltpu.make_async_copy(bound.at[layer_idx, pos], flat.at[:, pl.ds(stride * pos, 1)], local_sems.at[3 + layer_idx * (PERIOD + 1) + pos]))
    for copy in edges:
        copy.start()
    for copy in edges:
        copy.wait()


def gather_shares(window0, window1, extra):
    num_tiles = window0.shape[0]
    num_extra = extra.shape[0]
    inner = num_tiles - 2
    misc = jnp.concatenate([window0[:1], window0[-1:], window1[:1], window1[-1:], extra], axis=0)
    flat = (GROUP // PERIOD, PERIOD * (num_tiles - 1) + 1, ROWS, LANES)
    vmem = pl.BlockSpec(memory_space=pltpu.VMEM)
    hbm = pl.BlockSpec(memory_space=pl.ANY)
    dtype = window0.dtype
    return pl.pallas_call(
        gather_kernel,
        out_shape=(jax.ShapeDtypeStruct(flat, dtype), jax.ShapeDtypeStruct(flat, dtype), jax.ShapeDtypeStruct((GROUP, num_extra, ROWS, LANES), dtype)),
        in_specs=[vmem] * 3,
        out_specs=(hbm, hbm, vmem),
        scratch_shapes=[
            pltpu.VMEM((GROUP, num_extra + 4, ROWS, LANES), dtype),
            pltpu.VMEM((2, PERIOD + 1, GROUP // PERIOD, 1, ROWS, LANES), dtype),
            pltpu.SemaphoreType.DMA((3 + 2 * (PERIOD + 1),)),
            pltpu.SemaphoreType.DMA((3, GROUP)),
            pltpu.SemaphoreType.DMA((3, GROUP)),
        ],
        compiler_params=pltpu.CompilerParams(collective_id=1, has_side_effects=True),
        name='gather_shares',
    )(window0[1:-1], window1[1:-1], misc)


def scatter_kernel(grad0_ref, grad1_ref, extra_ref, out0_ref, out1_ref, own0, own1, core0, core1, first0, first1, second0, second1, far0, far1,
                   load_sems, send_sems, core_sems, first_sems, second_sems, far_sems):
    peers = Peers(lax.axis_index(AXIS))
    num_tiles = out0_ref.shape[0]
    num_extra = extra_ref.shape[1]
    own, near, first_in, second_in, far_in = (own0, own1), (core0, core1), (first0, first1), (second0, second1), (far0, far1)
    colours = ((MASK_X, MASK_Y), (MASK_Y, MASK_X))
    dists = (3, 2, 1, 0)
    sends = []

    def source(part, rel):
        dev, group, pos = peers.split(rel)
        if part == 2:
            return extra_ref.at[dev]
        grad = (grad0_ref, grad1_ref)[part]
        return grad.at[group, pl.ds((num_tiles - 1) * pos, num_tiles)]

    def slot(part, buffers, pos):
        if part == 2:
            return buffers[1].at[pos, pl.ds(num_tiles, num_extra)]
        return buffers[part].at[pos, pl.ds(0, num_tiles)]

    def post(src, dst, send_sem, recv_sem, mask):
        copy = pltpu.make_async_remote_copy(src_ref=src, dst_ref=dst, send_sem=send_sem, recv_sem=recv_sem,
                                            device_id=(peers.device(mask),), device_id_type=pl.DeviceIdType.MESH)
        copy.start()
        sends.append(copy)

    def expect(dst, send_sem, recv_sem):
        pltpu.make_async_remote_copy(src_ref=dst, dst_ref=dst, send_sem=send_sem, recv_sem=recv_sem,
                                     device_id=(peers.device(0),), device_id_type=pl.DeviceIdType.MESH).wait_recv()

    def targets(dist):
        return [(dist * 4 + pos, dist * MASK_Z + pos * MASK_X) for pos in (3, 2, 1, 0)]

    loads = {}
    for dist in dists:
        for pos, rel in targets(dist):
            for part in range(3):
                loads[part, pos] = pltpu.make_async_copy(source(part, rel), slot(part, own, pos), load_sems.at[part, pos])
                loads[part, pos].start()
    meet_partners(peers)
    for dist in dists:
        for pos, rel in targets(dist):
            for part in range(3):
                post(source(part, rel | MASK_CORE), slot(part, near, pos), send_sems.at[part, pos], core_sems.at[part, pos], MASK_CORE)

    def fold_core(dist):
        for pos, rel in targets(dist):
            for part in range(3):
                loads[part, pos].wait()
                expect(slot(part, near, pos), send_sems.at[part, pos], core_sems.at[part, pos])
            for side in range(2):
                own[side][pos] += near[side][pos]
        for side in range(2):
            mask, other = colours[side]
            for which in (1, 0):
                pos = dist * 4 + (mask + which * other) // MASK_X
                index = dist * 2 + which
                post(own[side].at[pos], first_in[side].at[index], send_sems.at[3 + side, index], first_sems.at[side, index], mask)

    def fold_first(dist):
        for side in range(2):
            mask, other = colours[side]
            for which in (1, 0):
                pos = dist * 4 + which * other // MASK_X
                index = dist * 2 + which
                expect(first_in[side].at[index], send_sems.at[3 + side, index], first_sems.at[side, index])
                own[side][pos] += first_in[side][index]
        for side in range(2):
            mask, other = colours[side]
            post(own[side].at[dist * 4 + other // MASK_X], second_in[side].at[dist], send_sems.at[3 + side, 8 + dist], second_sems.at[side, dist], other)

    def fold_second(dist):
        for side in range(2):
            expect(second_in[side].at[dist], send_sems.at[3 + side, 8 + dist], second_sems.at[side, dist])
            own[side][dist * 4] += second_in[side][dist]
        if dist:
            for side in range(2):
                post(own[side].at[dist * 4], far_in[side].at[dist - 1], send_sems.at[3 + side, 12 + dist], far_sems.at[side, dist - 1], dist * MASK_Z)

    fold_core(3)
    fold_core(2)
    fold_first(3)
    fold_core(1)
    fold_first(2)
    fold_second(3)
    fold_core(0)
    fold_first(1)
    fold_second(2)
    fold_first(0)
    fold_second(1)
    fold_second(0)
    for side in range(2):
        total = own[side][0]
        for dist in (3, 2, 1):
            expect(far_in[side].at[dist - 1], send_sems.at[3 + side, 12 + dist], far_sems.at[side, dist - 1])
            total = total + far_in[side][dist - 1]
        (out0_ref, out1_ref)[side][...] = total
    for copy in sends:
        copy.wait_send()


def scatter_grads(grad0, grad1, extra, num_tiles):
    num_extra = extra.shape[1]
    sizes = (num_tiles, num_tiles + num_extra)
    vmem = pl.BlockSpec(memory_space=pltpu.VMEM)
    hbm = pl.BlockSpec(memory_space=pl.ANY)

    def buffers(count):
        return [pltpu.VMEM((count, size, ROWS, LANES), jnp.float32) for size in sizes]

    return pl.pallas_call(
        scatter_kernel,
        out_shape=tuple(jax.ShapeDtypeStruct((size, ROWS, LANES), jnp.float32) for size in sizes),
        in_specs=[hbm] * 3,
        out_specs=(vmem, vmem),
        scratch_shapes=buffers(16) + buffers(16) + buffers(8) + buffers(4) + buffers(3) + [
            pltpu.SemaphoreType.DMA((3, 16)),
            pltpu.SemaphoreType.DMA((5, 16)),
            pltpu.SemaphoreType.DMA((3, 16)),
            pltpu.SemaphoreType.DMA((2, 8)),
            pltpu.SemaphoreType.DMA((2, 4)),
            pltpu.SemaphoreType.DMA((2, 3)),
        ],
        compiler_params=pltpu.CompilerParams(collective_id=2, has_side_effects=True),
        name='scatter_grads',
    )(grad0, grad1, extra)


NT_DIMS = (((1,), (1,)), ((), ()))
NN_DIMS = (((1,), (0,)), ((), ()))
HID_CHUNK = 512


def mlp_grad_kernel(d_out_ref, act_ref, slope_ref, normed_ref, w1_ref, w2_ref, d_normed_ref, bias_ref, flat_ref, acc1, acc2, staged, sems, *, row1, row2):
    step = pl.program_id(0)
    chans, hid = acc1.shape

    @pl.when(step == 0)
    def _():
        acc1[...] = jnp.zeros_like(acc1)
        acc2[...] = jnp.zeros_like(acc2)
        bias_ref[...] = jnp.zeros_like(bias_ref)

    d_out = d_out_ref[...]
    d_out_t = d_out.T
    normed_t = normed_ref[...].T
    d_normed = None
    for start in range(0, hid, HID_CHUNK):
        cols = pl.ds(start, HID_CHUNK)
        d_act = lax.dot_general(d_out, w2_ref[cols, :], NT_DIMS, preferred_element_type=jnp.float32)
        acc2[:, cols] += lax.dot_general(d_out_t, act_ref[:, cols], NN_DIMS, preferred_element_type=jnp.float32)
        d_hid = d_act.astype(jnp.bfloat16).astype(jnp.float32) * slope_ref[:, cols]
        bias_ref[:, cols] += jnp.sum(d_hid.reshape(-1, ROWS, HID_CHUNK), axis=0)
        d_hid_bf = d_hid.astype(jnp.bfloat16)
        acc1[:, cols] += lax.dot_general(normed_t, d_hid_bf, NN_DIMS, preferred_element_type=jnp.float32)
        part = lax.dot_general(d_hid_bf, w1_ref[:, cols], NT_DIMS, preferred_element_type=jnp.float32)
        d_normed = part if d_normed is None else d_normed + part
    d_normed_ref[...] = d_normed.astype(d_normed_ref.dtype)

    @pl.when(step == pl.num_programs(0) - 1)
    def _():
        wide = hid // LANES
        for col in range(wide):
            staged[0, pl.ds(col, chans, stride=wide), :] = acc1[:, col * LANES:(col + 1) * LANES]
        first = pltpu.make_async_copy(staged.at[0], flat_ref.at[pl.ds(row1, chans * wide)], sems.at[0])
        first.start()
        narrow = chans // LANES
        for col in range(narrow):
            staged[1, pl.ds(col, hid, stride=narrow), :] = acc2[col * LANES:(col + 1) * LANES, :].T
        second = pltpu.make_async_copy(staged.at[1], flat_ref.at[pl.ds(row2, chans * wide)], sems.at[1])
        second.start()
        first.wait()
        second.wait()


def mlp_grad(d_out, act, slope, normed, w1, w2, flat_rows, row1, row2, block):
    tokens, chans = d_out.shape
    hid = act.shape[1]

    def by_block(width):
        return pl.BlockSpec((block, width), lambda step: (step, 0))

    def whole(shape):
        return pl.BlockSpec(shape, lambda step: (0, 0), pipeline_mode=pl.Buffered(1))

    mat_rows = chans * hid // LANES
    return pl.pallas_call(
        functools.partial(mlp_grad_kernel, row1=row1, row2=row2),
        grid=(tokens // block,),
        out_shape=(
            jax.ShapeDtypeStruct((tokens, chans), jnp.bfloat16),
            jax.ShapeDtypeStruct((ROWS, hid), jnp.float32),
            jax.ShapeDtypeStruct((flat_rows, LANES), jnp.float32),
        ),
        in_specs=[by_block(chans), by_block(hid), by_block(hid), by_block(chans), whole(w1.shape), whole(w2.shape)],
        out_specs=(by_block(chans), pl.BlockSpec((ROWS, hid), lambda step: (0, 0)), pl.BlockSpec(memory_space=pl.ANY)),
        scratch_shapes=[
            pltpu.VMEM((chans, hid), jnp.float32),
            pltpu.VMEM((chans, hid), jnp.float32),
            pltpu.VMEM((2, mat_rows, LANES), jnp.float32),
            pltpu.SemaphoreType.DMA((2,)),
        ],
        compiler_params=pltpu.CompilerParams(dimension_semantics=('arbitrary',), vmem_limit_bytes=60 * 1024 * 1024),
        cost_estimate=pl.CostEstimate(flops=8 * tokens * chans * hid, bytes_accessed=6 * tokens * hid + 6 * tokens * chans + 12 * chans * hid, transcendentals=0),
        name='mlp_grad',
    )(d_out, act, slope, normed, w1, w2)


def sum_kernel(x_ref, out_ref, held, local_sem, send_sems, recv_sems):
    me = lax.axis_index(AXIS)
    barrier = pltpu.get_barrier_semaphore()
    for step in range(1, GROUP):
        pl.semaphore_signal(barrier, inc=1, device_id=((me + step) % GROUP,), device_id_type=pl.DeviceIdType.MESH)
    own = pltpu.make_async_copy(x_ref, held.at[me], local_sem)
    own.start()
    pl.semaphore_wait(barrier, GROUP - 1)
    sends = []
    for step in range(1, GROUP):
        copy = pltpu.make_async_remote_copy(
            src_ref=x_ref, dst_ref=held.at[me], send_sem=send_sems.at[step], recv_sem=recv_sems.at[me],
            device_id=((me + step) % GROUP,), device_id_type=pl.DeviceIdType.MESH)
        copy.start()
        sends.append(copy)
    own.wait()
    for step in range(1, GROUP):
        peer = (me + step) % GROUP
        pltpu.make_async_remote_copy(
            src_ref=x_ref, dst_ref=held.at[peer], send_sem=send_sems.at[step], recv_sem=recv_sems.at[peer],
            device_id=(peer,), device_id_type=pl.DeviceIdType.MESH).wait_recv()
    for copy in sends:
        copy.wait_send()
    out_ref[...] = jnp.sum(held[...], axis=0)


def sum_over_devices(values):
    block = jnp.zeros((ROWS, LANES), jnp.float32)
    for pos, value in enumerate(values):
        block = block.at[0, pos].set(value)
    total = pl.pallas_call(
        sum_kernel,
        out_shape=jax.ShapeDtypeStruct((ROWS, LANES), jnp.float32),
        in_specs=[pl.BlockSpec(memory_space=pltpu.VMEM)],
        out_specs=pl.BlockSpec(memory_space=pltpu.VMEM),
        scratch_shapes=[
            pltpu.VMEM((GROUP, ROWS, LANES), jnp.float32),
            pltpu.SemaphoreType.DMA,
            pltpu.SemaphoreType.DMA((GROUP,)),
            pltpu.SemaphoreType.DMA((GROUP,)),
        ],
        compiler_params=pltpu.CompilerParams(collective_id=0, has_side_effects=True),
        name='sum_over_devices',
    )(block)
    return [total[0, pos] for pos in range(len(values))]


def layer_norm(x_in, ln_gain, ln_shift):
    x_f = x_in.astype(jnp.float32)
    mean_val = jnp.mean(x_f, axis=-1, keepdims=True)
    var_val = jnp.mean(jnp.square(x_f - mean_val), axis=-1, keepdims=True)
    normed = (x_f - mean_val) * lax.rsqrt(var_val + LN_EPS)
    return (normed * ln_gain.astype(jnp.float32) + ln_shift.astype(jnp.float32)).astype(jnp.bfloat16)


def gelu_both(hidden):
    scale = math.sqrt(2.0 / math.pi)
    square = hidden * hidden
    tanh_val = jnp.tanh(hidden * (scale + (scale * 0.044715) * square))
    cdf = 0.5 + 0.5 * tanh_val
    slope = cdf + (0.5 * hidden) * (1.0 - tanh_val * tanh_val) * (scale + (3.0 * scale * 0.044715) * square)
    return (hidden * cdf).astype(jnp.bfloat16), slope


def norm_grad(x_in, ln_gain, ln_shift, d_normed):
    _, pullback = jax.vjp(layer_norm, x_in, ln_gain.astype(jnp.float32), ln_shift.astype(jnp.float32))
    d_x, d_gain, d_shift = pullback(d_normed.astype(jnp.bfloat16))
    return d_x.astype(jnp.float32), d_gain, d_shift


def scoped(tag, spec, lhs, rhs, **kwargs):
    with jax.named_scope(tag):
        return jnp.einsum(spec, lhs, rhs, **kwargs)


def layer_forward(x_in, weights, tag):
    w_tok1, w_tok2, w_ch1, w_ch2, ln1_g, ln1_b, b_tok1, b_tok2, ln2_g, ln2_b, b_ch1, b_ch2 = weights
    normed = layer_norm(x_in, ln1_g, ln1_b)
    hid_tok = scoped(tag + '_tok1', 'bsc,sj->bcj', normed, w_tok1, preferred_element_type=jnp.float32) + b_tok1.astype(jnp.float32)
    act_tok, slope_tok = gelu_both(hid_tok)
    with jax.named_scope(tag + '_tok2'):
        tok_out = jnp.einsum('bcj,js->bsc', act_tok, w_tok2, preferred_element_type=jnp.float32) + b_tok2.astype(jnp.float32)[:, None]
        after_tok = (x_in.astype(jnp.float32) + tok_out).astype(jnp.bfloat16)
    normed2 = layer_norm(after_tok, ln2_g, ln2_b)
    hid_ch = scoped(tag + '_ch1', 'bsc,cd->bsd', normed2, w_ch1, preferred_element_type=jnp.float32) + b_ch1.astype(jnp.float32)
    act_ch, slope_ch = gelu_both(hid_ch)
    with jax.named_scope(tag + '_ch2'):
        ch_out = jnp.einsum('bsd,dc->bsc', act_ch, w_ch2, preferred_element_type=jnp.float32) + b_ch2.astype(jnp.float32)
        layer_out = (after_tok.astype(jnp.float32) + ch_out).astype(jnp.bfloat16)
    return layer_out, (x_in, normed, slope_tok, act_tok, after_tok, normed2, slope_ch, act_ch)


def layer_backward(d_out, weights, cache, tag, flat_len, num_tokens):
    num_chans = d_out.shape[2]
    w_tok1, w_tok2, w_ch1, w_ch2, ln1_g, ln1_b, b_tok1, b_tok2, ln2_g, ln2_b, b_ch1, b_ch2 = weights
    x_in, normed, slope_tok, act_tok, after_tok, normed2, slope_ch, act_ch = cache
    d_out_bf = d_out.astype(jnp.bfloat16)
    g_b_ch2 = jnp.sum(d_out, axis=(0, 1))
    tokens = d_out.shape[0] * d_out.shape[1]
    mat_tiles = [math.prod(shape_one) // LANES for shape_one in piece_shapes(num_tokens, num_chans)[:4]]
    row1 = mat_tiles[0] + mat_tiles[1]
    d_normed2, bias_rows, flat_grad = mlp_grad(
        d_out_bf.reshape(tokens, num_chans), act_ch.reshape(tokens, -1), slope_ch.reshape(tokens, -1), normed2.reshape(tokens, num_chans),
        w_ch1, w_ch2, flat_len // LANES, row1, row1 + mat_tiles[2], tokens // 5)
    g_b_ch1 = jnp.sum(bias_rows, axis=0)
    d_normed2 = d_normed2.reshape(d_out.shape)
    with jax.named_scope(tag + '_ln2'):
        d_after_ln, g_ln2_g, g_ln2_b = norm_grad(after_tok, ln2_g, ln2_b, d_normed2)
    d_after = d_after_ln + d_out
    d_after_bf = d_after.astype(jnp.bfloat16)
    g_b_tok2 = jnp.sum(d_after, axis=(0, 2))
    g_w_tok2 = scoped(tag + '_gt2', 'bcj,bsc->js', act_tok, d_after_bf, preferred_element_type=jnp.float32)
    with jax.named_scope(tag + '_dtok'):
        d_act_tok = jnp.einsum('bsc,js->bcj', d_after_bf, w_tok2, preferred_element_type=jnp.float32)
        d_hid_tok = d_act_tok.astype(jnp.bfloat16).astype(jnp.float32) * slope_tok
        d_hid_tok_bf = d_hid_tok.astype(jnp.bfloat16)
        g_b_tok1 = jnp.sum(d_hid_tok, axis=(0, 1))
    g_w_tok1 = scoped(tag + '_gt1', 'bsc,bcj->sj', normed, d_hid_tok_bf, preferred_element_type=jnp.float32)
    d_normed = scoped(tag + '_dnt', 'bcj,sj->bsc', d_hid_tok_bf, w_tok1, preferred_element_type=jnp.float32)
    d_in_ln, g_ln1_g, g_ln1_b = norm_grad(x_in, ln1_g, ln1_b, d_normed)
    d_in = d_in_ln + d_after
    vectors = jnp.concatenate([g_ln1_g, g_ln1_b, g_b_tok1, g_b_tok2[:num_tokens], g_ln2_g, g_ln2_b, g_b_ch1, g_b_ch2])
    last_row = row1 + mat_tiles[2] + mat_tiles[3]
    vectors = jnp.pad(vectors, (0, flat_len - last_row * LANES - vectors.shape[0])).reshape(-1, LANES)
    tok_rows = jnp.concatenate([g_w_tok1[:num_tokens].reshape(-1, LANES), g_w_tok2[:, :num_tokens].reshape(-1, LANES)], axis=0)
    flat_grad = lax.dynamic_update_slice(flat_grad, tok_rows, (0, 0))
    flat_grad = lax.dynamic_update_slice(flat_grad, vectors, (last_row, 0))
    return d_in, flat_grad


def head_step(hidden, labels, small_full, head_full, num_classes, global_b, num_tokens):
    num_chans = hidden.shape[2]
    lnf_g = small_full[:num_chans]
    lnf_b = small_full[num_chans:2 * num_chans]
    head_b = small_full[2 * num_chans:2 * num_chans + num_classes]
    normed = layer_norm(hidden, lnf_g, lnf_b)
    pooled = (jnp.sum(normed[:, :num_tokens], axis=1, dtype=jnp.float32) / num_tokens).astype(jnp.bfloat16)
    is_class = jnp.arange(HEAD_PAD)[None, :] < num_classes
    logits = jnp.dot(pooled, head_full, preferred_element_type=jnp.float32) + jnp.pad(head_b.astype(jnp.float32), (0, HEAD_PAD - num_classes))
    logits = jnp.where(is_class, logits, -jnp.inf)
    log_norm = jax.nn.logsumexp(logits, axis=-1)
    is_label = jnp.arange(HEAD_PAD)[None, :] == labels[:, None]
    picked = jnp.sum(jnp.where(is_label, logits, 0.0), axis=-1)
    loss_sum = jnp.sum(log_norm - picked)
    d_logits = (jnp.exp(logits - log_norm[:, None]) - is_label.astype(jnp.float32)) / global_b
    d_logits_bf = d_logits.astype(jnp.bfloat16)
    g_head_b = jnp.sum(d_logits, axis=0)[:num_classes]
    g_head_w = jnp.einsum('bc,bk->ck', pooled, d_logits_bf, preferred_element_type=jnp.float32)
    d_pooled = jnp.einsum('bk,ck->bc', d_logits_bf, head_full, preferred_element_type=jnp.float32)
    is_token = jnp.arange(hidden.shape[1])[None, :, None] < num_tokens
    d_normed = jnp.where(is_token, (d_pooled / num_tokens)[:, None, :], 0.0)
    d_hidden, g_lnf_g, g_lnf_b = norm_grad(hidden, lnf_g, lnf_b, d_normed)
    g_small = jnp.concatenate([g_lnf_g, g_lnf_b, g_head_b])
    return loss_sum, d_hidden, g_head_w, g_small


def adam_update(master, gradient, moment, second, decay_rate):
    moment_new = BETA_ONE * moment + (1.0 - BETA_ONE) * gradient
    second_new = BETA_TWO * second + (1.0 - BETA_TWO) * gradient * gradient
    m_hat = moment_new / (1.0 - BETA_ONE ** ADAM_STEP)
    v_hat = second_new / (1.0 - BETA_TWO ** ADAM_STEP)
    master_new = master - LEARN_RATE * (m_hat / (jnp.sqrt(v_hat) + ADAM_EPS) + decay_rate * master)
    return master_new, moment_new, second_new


def solution(mesh):
    row_spec = P(AXIS)
    layer_spec = P(None, AXIS)
    in_specs = (row_spec, row_spec, layer_spec, row_spec, row_spec, layer_spec, row_spec, row_spec, layer_spec, row_spec, row_spec)
    out_specs = (P(),) + in_specs[2:]

    def device_step(act_in, labels, layer_p, head_w, small_p, layer_m, head_m, small_m, layer_v, head_v, small_v):
        local_b, num_tokens, num_chans = act_in.shape
        global_b = local_b * GROUP
        num_layers, share_len = layer_p.shape
        flat_len = share_len * GROUP
        head_rows, num_classes = head_w.shape
        small_len = small_p.shape[0]
        mat_len = 2 * num_tokens * (num_chans // 2) + 8 * num_chans * num_chans

        windows = [share_to_window(layer_p[layer_idx].astype(jnp.bfloat16)) for layer_idx in range(num_layers)]
        win_tiles = windows[0].shape[0]
        head_tiles = head_to_tiles(head_w.astype(jnp.bfloat16))
        small_tile = jnp.pad(small_p.astype(jnp.bfloat16).reshape(1, 1, small_len), ((0, 0), (0, ROWS - 1), (0, 0)))
        num_head = head_tiles.shape[0]
        flat0, flat1, extra = gather_shares(windows[0], windows[1], jnp.concatenate([head_tiles, small_tile], axis=0))

        weights = []
        caches = []
        hidden = pad_tokens(act_in, 1, num_tokens)
        for layer_idx, flat in enumerate((flat0, flat1)):
            weights.append(unpack_tiles(flat.reshape(-1, ROWS, LANES), num_tokens, num_chans))
            hidden, cache = layer_forward(hidden, weights[layer_idx], f'f{layer_idx}')
            caches.append(cache)
        head_full = tiles_to_head(extra[:, :num_head], head_rows * GROUP)
        small_full = extra[:, num_head, 0].reshape(-1)
        loss_sum, d_hidden, g_head_w, g_small = head_step(hidden, labels, small_full, head_full, num_classes, global_b, num_tokens)

        head_blocks = head_to_tiles(g_head_w).reshape(GROUP, num_head, ROWS, LANES)
        g_small = jnp.pad(g_small, (0, small_len * GROUP - g_small.shape[0])).reshape(GROUP, 1, 1, small_len)
        small_blocks = jnp.pad(g_small, ((0, 0), (0, 0), (0, ROWS - 1), (0, 0)))
        packed = [None] * num_layers
        for layer_idx in reversed(range(num_layers)):
            d_hidden, flat_grad = layer_backward(d_hidden, weights[layer_idx], caches[layer_idx], f'b{layer_idx}', flat_len, num_tokens)
            packed[layer_idx] = flat_grad.reshape(flat0.shape)
        summed0, summed1 = scatter_grads(packed[0], packed[1], jnp.concatenate([head_blocks, small_blocks], axis=1), win_tiles)
        layer_g = jnp.stack([window_to_share(summed0, share_len), window_to_share(summed1[:win_tiles], share_len)])
        head_g = tiles_to_head(summed1[win_tiles:win_tiles + num_head], head_rows)[:, :num_classes]
        small_g = summed1[win_tiles + num_head, 0]

        sq_local = jnp.sum(jnp.square(layer_g)) + jnp.sum(jnp.square(head_g)) + jnp.sum(jnp.square(small_g))
        loss_total, sq_total = sum_over_devices([loss_sum, sq_local])
        loss_value = loss_total / global_b
        clip_scale = 1.0 / jnp.maximum(1.0, jnp.sqrt(sq_total))
        flat_pos = lax.axis_index(AXIS) * share_len + jnp.arange(share_len)
        layer_decay = jnp.where(flat_pos < mat_len, WEIGHT_DECAY, 0.0)[None, :]
        new_lp, new_lm, new_lv = adam_update(layer_p, layer_g * clip_scale, layer_m, layer_v, layer_decay)
        new_hw, new_hm, new_hv = adam_update(head_w, head_g * clip_scale, head_m, head_v, WEIGHT_DECAY)
        new_sp, new_sm, new_sv = adam_update(small_p, small_g * clip_scale, small_m, small_v, 0.0)
        return (loss_value, new_lp, new_hw, new_sp, new_lm, new_hm, new_sm, new_lv, new_hv, new_sv)

    return jax.shard_map(device_step, mesh=mesh, in_specs=in_specs, out_specs=out_specs, check_vma=False)
```

```python
import functools
import math
import jax
import jax.numpy as jnp
from jax import lax
from jax.experimental import pallas as pl
from jax.experimental.pallas import tpu as pltpu
from jax.sharding import PartitionSpec as P

LN_EPS = 1e-6
LEARN_RATE = 0.003
BETA_ONE = 0.9
BETA_TWO = 0.999
ADAM_EPS = 1e-8
WEIGHT_DECAY = 0.03
ADAM_STEP = 10
AXIS = 'fsdp'
GROUP = 32
ROWS = 8
LANES = 128
TILE = ROWS * LANES
HEAD_PAD = 1024
IMAGE_ROWS = 8

def row_offset(share_rows):
    return (lax.axis_index(AXIS) * share_rows) % ROWS


def share_to_window(share):
    share_rows = share.shape[0] // LANES
    num_tiles = -(-(share_rows + ROWS - 2) // ROWS)
    window = jnp.zeros((num_tiles * ROWS, LANES), share.dtype)
    window = lax.dynamic_update_slice(window, share.reshape(share_rows, LANES), (row_offset(share_rows), 0))
    return window.reshape(num_tiles, ROWS, LANES)


def window_to_share(window, share_len):
    share_rows = share_len // LANES
    rows = window.reshape(-1, LANES)
    return lax.dynamic_slice(rows, (row_offset(share_rows), 0), (share_rows, LANES)).reshape(share_len)


def piece_shapes(num_tokens, num_chans):
    tok_hid = num_chans // 2
    ch_hid = 4 * num_chans
    return [(num_tokens, tok_hid), (tok_hid, num_tokens), (num_chans, ch_hid), (ch_hid, num_chans), (num_chans,), (num_chans,), (tok_hid,), (num_tokens,), (num_chans,), (num_chans,), (ch_hid,), (num_chans,)]


def pad_tokens(val, axis, num_tokens):
    widths = [(0, 0)] * val.ndim
    widths[axis] = (0, -num_tokens % IMAGE_ROWS)
    return jnp.pad(val, widths)


def unpack_tiles(tiles, num_tokens, num_chans):
    pieces = []
    start = 0
    shapes = piece_shapes(num_tokens, num_chans)
    for shape_one in shapes[:4]:
        count = math.prod(shape_one) // TILE
        pieces.append(tiles[start:start + count].reshape(shape_one) if len(pieces) < 2 else None)
        start = start + count
    flat = tiles[start:].reshape(-1)
    start = 0
    for shape_one in shapes[4:]:
        pieces.append(flat[start:start + shape_one[0]])
        start = start + shape_one[0]
    pieces[0] = pad_tokens(pieces[0], 0, num_tokens)
    pieces[1] = pad_tokens(pieces[1], 1, num_tokens)
    tile1 = 2 * math.prod(shapes[0]) // TILE
    pieces[2], pieces[3] = unpack_mats(tiles, shapes[2], shapes[3], tile1, tile1 + math.prod(shapes[2]) // TILE)
    pieces[7] = pad_tokens(pieces[7], 0, num_tokens)
    return pieces


def head_to_tiles(head):
    rows = head.shape[0]
    head = jnp.pad(head, ((0, 0), (0, HEAD_PAD - head.shape[1])))
    return head.reshape(rows // ROWS, ROWS, HEAD_PAD // LANES, LANES).transpose(0, 2, 1, 3).reshape(-1, ROWS, LANES)


def tiles_to_head(tiles, rows):
    tiles = tiles.reshape(rows // ROWS, HEAD_PAD // LANES, ROWS, LANES)
    return tiles.transpose(0, 2, 1, 3).reshape(rows, HEAD_PAD)


MASK_CORE, MASK_X, MASK_Y, MASK_Z = 1, 2, 4, 8
PARTNERS = (MASK_CORE, MASK_X, MASK_Y, MASK_Z, 2 * MASK_Z, 3 * MASK_Z)
PERIOD = 4


class Peers:
    def __init__(self, me):
        self.bits = []
        for bit in range(5):
            val = lax.rem(lax.div(me, 1 << bit), 2)
            self.bits.append((val, 1 - val))
        self.known = {}

    def split(self, rel):
        if rel not in self.known:
            vals = [self.bits[bit][(rel >> bit) & 1] for bit in range(5)]
            pos = vals[0] + 2 * vals[1]
            group = vals[2] + 2 * vals[3] + 4 * vals[4]
            self.known[rel] = (group * PERIOD + pos, group, pos)
        return self.known[rel]

    def device(self, rel):
        return self.split(rel)[0]


def meet_all(me):
    barrier = pltpu.get_barrier_semaphore()
    for step in range(1, GROUP):
        pl.semaphore_signal(barrier, inc=1, device_id=(lax.rem(me + step, GROUP),), device_id_type=pl.DeviceIdType.MESH)
    pl.semaphore_wait(barrier, GROUP - 1)


def meet_partners(peers):
    barrier = pltpu.get_barrier_semaphore()
    for mask in PARTNERS:
        pl.semaphore_signal(barrier, inc=1, device_id=(peers.device(mask),), device_id_type=pl.DeviceIdType.MESH)
    pl.semaphore_wait(barrier, len(PARTNERS))


def gather_kernel(inner0_ref, inner1_ref, misc_ref, flat0_ref, flat1_ref, extra_ref, misc_all, bound, local_sems, send_sems, recv_sems):
    peers = Peers(lax.axis_index(AXIS))
    inner = inner0_ref.shape[0]
    stride = inner + 1
    own_refs = (inner0_ref, inner1_ref, misc_ref)
    colours = ((MASK_Y, MASK_X), (MASK_X, MASK_Y), (MASK_X, MASK_Y))

    def place(arr, rel):
        dev, group, pos = peers.split(rel)
        if arr == 2:
            return misc_all.at[dev]
        flat = (flat0_ref, flat1_ref)[arr]
        return flat.at[group, pl.ds(stride * pos + 1, inner)]

    own_copies = [pltpu.make_async_copy(own_refs[arr], place(arr, 0), local_sems.at[arr]) for arr in range(3)]
    for copy in own_copies:
        copy.start()
    meet_partners(peers)
    sends = []

    def send(arr, rel, mask):
        here = place(arr, rel)
        copy = pltpu.make_async_remote_copy(
            src_ref=own_refs[arr] if rel == 0 else here, dst_ref=here,
            send_sem=send_sems.at[arr, rel ^ mask], recv_sem=recv_sems.at[arr, rel ^ mask],
            device_id=(peers.device(mask),), device_id_type=pl.DeviceIdType.MESH)
        copy.start()
        sends.append(copy)

    def receive(arr, rel):
        here = place(arr, rel)
        pltpu.make_async_remote_copy(
            src_ref=here, dst_ref=here, send_sem=send_sems.at[arr, rel], recv_sem=recv_sems.at[arr, rel],
            device_id=(peers.device(0),), device_id_type=pl.DeviceIdType.MESH).wait_recv()

    for mask_pos in range(6):
        for arr in range(3):
            first, second = colours[arr]
            send(arr, 0, (MASK_Z, first, second, 2 * MASK_Z, 3 * MASK_Z, MASK_CORE)[mask_pos])
    for dist, use_first, use_second in ((0, 1, 0), (1, 0, 0), (0, 0, 1), (1, 1, 0), (0, 1, 1), (2, 0, 0), (1, 0, 1), (2, 1, 0),
                                        (1, 1, 1), (3, 0, 0), (2, 0, 1), (3, 1, 0), (2, 1, 1), (3, 0, 1), (3, 1, 1)):
        for arr in range(3):
            first, second = colours[arr]
            rel = dist * MASK_Z + use_first * first + use_second * second
            receive(arr, rel)
            if not use_second:
                if not use_first:
                    send(arr, rel, first)
                send(arr, rel, second)
            send(arr, rel, MASK_CORE)
    for rel in range(MASK_CORE, GROUP, 2):
        for arr in range(3):
            receive(arr, rel)
    for copy in own_copies:
        copy.wait()
    for copy in sends:
        copy.wait_send()

    for layer_idx in range(2):
        for group in range(GROUP // PERIOD):
            for pos in range(PERIOD + 1):
                tile = None
                if pos < PERIOD:
                    tile = misc_all[group * PERIOD + pos, 2 * layer_idx]
                if pos > 0:
                    left = misc_all[group * PERIOD + pos - 1, 2 * layer_idx + 1]
                    tile = left if tile is None else tile + left
                bound[layer_idx, pos, group, 0] = tile
    extra_ref[...] = misc_all[:, 4:]
    edges = []
    for layer_idx in range(2):
        flat = (flat0_ref, flat1_ref)[layer_idx]
        for pos in range(PERIOD + 1):
            edges.append(pltpu.make_async_copy(bound.at[layer_idx, pos], flat.at[:, pl.ds(stride * pos, 1)], local_sems.at[3 + layer_idx * (PERIOD + 1) + pos]))
    for copy in edges:
        copy.start()
    for copy in edges:
        copy.wait()


def gather_shares(window0, window1, extra):
    num_tiles = window0.shape[0]
    num_extra = extra.shape[0]
    inner = num_tiles - 2
    misc = jnp.concatenate([window0[:1], window0[-1:], window1[:1], window1[-1:], extra], axis=0)
    flat = (GROUP // PERIOD, PERIOD * (num_tiles - 1) + 1, ROWS, LANES)
    vmem = pl.BlockSpec(memory_space=pltpu.VMEM)
    hbm = pl.BlockSpec(memory_space=pl.ANY)
    dtype = window0.dtype
    return pl.pallas_call(
        gather_kernel,
        out_shape=(jax.ShapeDtypeStruct(flat, dtype), jax.ShapeDtypeStruct(flat, dtype), jax.ShapeDtypeStruct((GROUP, num_extra, ROWS, LANES), dtype)),
        in_specs=[vmem] * 3,
        out_specs=(hbm, hbm, vmem),
        scratch_shapes=[
            pltpu.VMEM((GROUP, num_extra + 4, ROWS, LANES), dtype),
            pltpu.VMEM((2, PERIOD + 1, GROUP // PERIOD, 1, ROWS, LANES), dtype),
            pltpu.SemaphoreType.DMA((3 + 2 * (PERIOD + 1),)),
            pltpu.SemaphoreType.DMA((3, GROUP)),
            pltpu.SemaphoreType.DMA((3, GROUP)),
        ],
        compiler_params=pltpu.CompilerParams(collective_id=1, has_side_effects=True),
        name='gather_shares',
    )(window0[1:-1], window1[1:-1], misc)


def scatter_kernel(grad0_ref, grad1_ref, extra_ref, loss_ref, out0_ref, out1_ref, sums_ref, own0, own1, core0, core1, first0, first1, second0, second1, far0, far1,
                   partial, held, load_sems, send_sems, core_sems, first_sems, second_sems, far_sems, sum_load_sem, sum_send_sems, sum_recv_sems, *, share_rows):
    me = lax.axis_index(AXIS)
    peers = Peers(me)
    num_tiles = out0_ref.shape[0]
    num_extra = extra_ref.shape[1]
    own, near, first_in, second_in, far_in = (own0, own1), (core0, core1), (first0, first1), (second0, second1), (far0, far1)
    colours = ((MASK_X, MASK_Y), (MASK_Y, MASK_X))
    dists = (3, 2, 1, 0)
    sends = []

    def source(part, rel):
        dev, group, pos = peers.split(rel)
        if part == 2:
            return extra_ref.at[dev]
        grad = (grad0_ref, grad1_ref)[part]
        return grad.at[group, pl.ds((num_tiles - 1) * pos, num_tiles)]

    def slot(part, buffers, pos):
        if part == 2:
            return buffers[1].at[pos, pl.ds(num_tiles, num_extra)]
        return buffers[part].at[pos, pl.ds(0, num_tiles)]

    def post(src, dst, send_sem, recv_sem, mask):
        copy = pltpu.make_async_remote_copy(src_ref=src, dst_ref=dst, send_sem=send_sem, recv_sem=recv_sem,
                                            device_id=(peers.device(mask),), device_id_type=pl.DeviceIdType.MESH)
        copy.start()
        sends.append(copy)

    def expect(dst, send_sem, recv_sem):
        pltpu.make_async_remote_copy(src_ref=dst, dst_ref=dst, send_sem=send_sem, recv_sem=recv_sem,
                                     device_id=(peers.device(0),), device_id_type=pl.DeviceIdType.MESH).wait_recv()

    def targets(dist):
        return [(dist * 4 + pos, dist * MASK_Z + pos * MASK_X) for pos in (3, 2, 1, 0)]

    loads = {}
    for dist in dists:
        for pos, rel in targets(dist):
            for part in range(3):
                loads[part, pos] = pltpu.make_async_copy(source(part, rel), slot(part, own, pos), load_sems.at[part, pos])
                loads[part, pos].start()
    loss_copy = pltpu.make_async_copy(loss_ref, partial.at[1], sum_load_sem.at[0])
    loss_copy.start()
    meet_all(me)
    for dist in dists:
        for pos, rel in targets(dist):
            for part in range(3):
                post(source(part, rel | MASK_CORE), slot(part, near, pos), send_sems.at[part, pos], core_sems.at[part, pos], MASK_CORE)

    def fold_core(dist):
        for pos, rel in targets(dist):
            for part in range(3):
                loads[part, pos].wait()
                expect(slot(part, near, pos), send_sems.at[part, pos], core_sems.at[part, pos])
            for side in range(2):
                own[side][pos] += near[side][pos]
        for side in range(2):
            mask, other = colours[side]
            for which in (1, 0):
                pos = dist * 4 + (mask + which * other) // MASK_X
                index = dist * 2 + which
                post(own[side].at[pos], first_in[side].at[index], send_sems.at[3 + side, index], first_sems.at[side, index], mask)

    def fold_first(dist):
        for side in range(2):
            mask, other = colours[side]
            for which in (1, 0):
                pos = dist * 4 + which * other // MASK_X
                index = dist * 2 + which
                expect(first_in[side].at[index], send_sems.at[3 + side, index], first_sems.at[side, index])
                own[side][pos] += first_in[side][index]
        for side in range(2):
            mask, other = colours[side]
            post(own[side].at[dist * 4 + other // MASK_X], second_in[side].at[dist], send_sems.at[3 + side, 8 + dist], second_sems.at[side, dist], other)

    def fold_second(dist):
        for side in range(2):
            expect(second_in[side].at[dist], send_sems.at[3 + side, 8 + dist], second_sems.at[side, dist])
            own[side][dist * 4] += second_in[side][dist]
        if dist:
            for side in range(2):
                post(own[side].at[dist * 4], far_in[side].at[dist - 1], send_sems.at[3 + side, 12 + dist], far_sems.at[side, dist - 1], dist * MASK_Z)

    fold_core(3)
    fold_core(2)
    fold_first(3)
    fold_core(1)
    fold_first(2)
    fold_second(3)
    fold_core(0)
    fold_first(1)
    fold_second(2)
    fold_first(0)
    fold_second(1)
    fold_second(0)
    for side in range(2):
        total = own[side][0]
        for dist in (3, 2, 1):
            expect(far_in[side].at[dist - 1], send_sems.at[3 + side, 12 + dist], far_sems.at[side, dist - 1])
            total = total + far_in[side][dist - 1]
        (out0_ref, out1_ref)[side][...] = total

    first_row = 2 * peers.split(0)[2] if share_rows % ROWS == 2 else lax.rem(share_rows * me, ROWS)
    row = lax.broadcasted_iota(jnp.int32, (ROWS, LANES), 0)
    squares = jnp.zeros((ROWS, LANES), jnp.float32)
    for out_ref in (out0_ref, out1_ref):
        head = jnp.where(row >= first_row, out_ref[0], 0.0)
        tail = jnp.where(row < first_row + share_rows % ROWS, out_ref[num_tiles - 1], 0.0)
        inner = out_ref[1:num_tiles - 1]
        squares = squares + head * head + tail * tail + jnp.sum(inner * inner, axis=0)
    rest = out1_ref[num_tiles:]
    partial[0] = squares + jnp.sum(rest * rest, axis=0)
    for copy in sends:
        copy.wait_send()
    loss_copy.wait()
    mine = pltpu.make_async_copy(partial, held.at[me], sum_load_sem.at[1])
    mine.start()
    posts = []
    for step in range(1, GROUP):
        copy = pltpu.make_async_remote_copy(
            src_ref=partial, dst_ref=held.at[me], send_sem=sum_send_sems.at[step], recv_sem=sum_recv_sems.at[me],
            device_id=(lax.rem(me + step, GROUP),), device_id_type=pl.DeviceIdType.MESH)
        copy.start()
        posts.append(copy)
    mine.wait()
    for step in range(1, GROUP):
        peer = lax.rem(me + step, GROUP)
        pltpu.make_async_remote_copy(
            src_ref=partial, dst_ref=held.at[peer], send_sem=sum_send_sems.at[step], recv_sem=sum_recv_sems.at[peer],
            device_id=(peer,), device_id_type=pl.DeviceIdType.MESH).wait_recv()
    for copy in posts:
        copy.wait_send()
    sums_ref[...] = jnp.sum(held[...], axis=0)


def scatter_grads(grad0, grad1, extra, loss_tile, num_tiles, share_rows):
    num_extra = extra.shape[1]
    sizes = (num_tiles, num_tiles + num_extra)
    vmem = pl.BlockSpec(memory_space=pltpu.VMEM)
    hbm = pl.BlockSpec(memory_space=pl.ANY)

    def buffers(count):
        return [pltpu.VMEM((count, size, ROWS, LANES), jnp.float32) for size in sizes]

    return pl.pallas_call(
        functools.partial(scatter_kernel, share_rows=share_rows),
        out_shape=tuple(jax.ShapeDtypeStruct((size, ROWS, LANES), jnp.float32) for size in sizes + (2,)),
        in_specs=[hbm] * 3 + [vmem],
        out_specs=(vmem, vmem, vmem),
        scratch_shapes=buffers(16) + buffers(16) + buffers(8) + buffers(4) + buffers(3) + [
            pltpu.VMEM((2, ROWS, LANES), jnp.float32),
            pltpu.VMEM((GROUP, 2, ROWS, LANES), jnp.float32),
            pltpu.SemaphoreType.DMA((3, 16)),
            pltpu.SemaphoreType.DMA((5, 16)),
            pltpu.SemaphoreType.DMA((3, 16)),
            pltpu.SemaphoreType.DMA((2, 8)),
            pltpu.SemaphoreType.DMA((2, 4)),
            pltpu.SemaphoreType.DMA((2, 3)),
            pltpu.SemaphoreType.DMA((2,)),
            pltpu.SemaphoreType.DMA((GROUP,)),
            pltpu.SemaphoreType.DMA((GROUP,)),
        ],
        compiler_params=pltpu.CompilerParams(collective_id=2, has_side_effects=True),
        name='scatter_grads',
    )(grad0, grad1, extra, loss_tile)


NT_DIMS = (((1,), (1,)), ((), ()))
NN_DIMS = (((1,), (0,)), ((), ()))
HID_CHUNK = 512


def mlp_grad_kernel(d_out_ref, act_ref, slope_ref, normed_ref, w1_ref, w2_ref, d_normed_ref, bias_ref, flat_ref, acc1, acc2, staged, sems, *, row1, row2):
    step = pl.program_id(0)
    chans, hid = acc1.shape

    @pl.when(step == 0)
    def _():
        acc1[...] = jnp.zeros_like(acc1)
        acc2[...] = jnp.zeros_like(acc2)
        bias_ref[...] = jnp.zeros_like(bias_ref)

    d_out = d_out_ref[...]
    d_out_t = d_out.T
    normed_t = normed_ref[...].T
    d_normed = None
    for start in range(0, hid, HID_CHUNK):
        cols = pl.ds(start, HID_CHUNK)
        d_act = lax.dot_general(d_out, w2_ref[cols, :], NT_DIMS, preferred_element_type=jnp.float32)
        acc2[:, cols] += lax.dot_general(d_out_t, act_ref[:, cols], NN_DIMS, preferred_element_type=jnp.float32)
        d_hid = d_act.astype(jnp.bfloat16).astype(jnp.float32) * slope_ref[:, cols]
        bias_ref[:, cols] += jnp.sum(d_hid.reshape(-1, ROWS, HID_CHUNK), axis=0)
        d_hid_bf = d_hid.astype(jnp.bfloat16)
        acc1[:, cols] += lax.dot_general(normed_t, d_hid_bf, NN_DIMS, preferred_element_type=jnp.float32)
        part = lax.dot_general(d_hid_bf, w1_ref[:, cols], NT_DIMS, preferred_element_type=jnp.float32)
        d_normed = part if d_normed is None else d_normed + part
    d_normed_ref[...] = d_normed.astype(d_normed_ref.dtype)

    @pl.when(step == pl.num_programs(0) - 1)
    def _():
        wide = hid // LANES
        for col in range(wide):
            staged[0, pl.ds(col, chans, stride=wide), :] = acc1[:, col * LANES:(col + 1) * LANES]
        first = pltpu.make_async_copy(staged.at[0], flat_ref.at[pl.ds(row1, chans * wide)], sems.at[0])
        first.start()
        narrow = chans // LANES
        for col in range(narrow):
            staged[1, pl.ds(col, hid, stride=narrow), :] = acc2[col * LANES:(col + 1) * LANES, :].T
        second = pltpu.make_async_copy(staged.at[1], flat_ref.at[pl.ds(row2, chans * wide)], sems.at[1])
        second.start()
        first.wait()
        second.wait()


def mlp_grad(d_out, act, slope, normed, w1, w2, flat_rows, row1, row2, block):
    tokens, chans = d_out.shape
    hid = act.shape[1]

    def by_block(width):
        return pl.BlockSpec((block, width), lambda step: (step, 0))

    def whole(shape):
        return pl.BlockSpec(shape, lambda step: (0, 0), pipeline_mode=pl.Buffered(1))

    mat_rows = chans * hid // LANES
    return pl.pallas_call(
        functools.partial(mlp_grad_kernel, row1=row1, row2=row2),
        grid=(tokens // block,),
        out_shape=(
            jax.ShapeDtypeStruct((tokens, chans), jnp.bfloat16),
            jax.ShapeDtypeStruct((ROWS, hid), jnp.float32),
            jax.ShapeDtypeStruct((flat_rows, LANES), jnp.float32),
        ),
        in_specs=[by_block(chans), by_block(hid), by_block(hid), by_block(chans), whole(w1.shape), whole(w2.shape)],
        out_specs=(by_block(chans), pl.BlockSpec((ROWS, hid), lambda step: (0, 0)), pl.BlockSpec(memory_space=pl.ANY)),
        scratch_shapes=[
            pltpu.VMEM((chans, hid), jnp.float32),
            pltpu.VMEM((chans, hid), jnp.float32),
            pltpu.VMEM((2, mat_rows, LANES), jnp.float32),
            pltpu.SemaphoreType.DMA((2,)),
        ],
        compiler_params=pltpu.CompilerParams(dimension_semantics=('arbitrary',), vmem_limit_bytes=60 * 1024 * 1024),
        cost_estimate=pl.CostEstimate(flops=8 * tokens * chans * hid, bytes_accessed=6 * tokens * hid + 6 * tokens * chans + 12 * chans * hid, transcendentals=0),
        name='mlp_grad',
    )(d_out, act, slope, normed, w1, w2)


CHUNK_TILES = 128


def unpack_kernel(flat_ref, w1_ref, w2_ref, raw, spread, sems, *, tile1, tile2):
    chans, hid = w1_ref.shape
    num_chunks = chans * hid // (CHUNK_TILES * TILE)
    copies = []
    for mat, first in enumerate((tile1, tile2)):
        for chunk in range(num_chunks):
            pos = mat * num_chunks + chunk
            copies.append(pltpu.make_async_copy(flat_ref.at[pl.ds(first + chunk * CHUNK_TILES, CHUNK_TILES)], raw.at[pos], sems.at[pos]))
            copies[-1].start()
    for mat, out_ref in enumerate((w1_ref, w2_ref)):
        wide = out_ref.shape[1] // LANES
        count = CHUNK_TILES * ROWS // wide
        for chunk in range(num_chunks):
            pos = mat * num_chunks + chunk
            copies[pos].wait()
            spread[pos % 2] = raw[pos].astype(jnp.float32).reshape(CHUNK_TILES * ROWS, LANES)
            for col in range(wide):
                out_ref[chunk * count:(chunk + 1) * count, col * LANES:(col + 1) * LANES] = spread[pos % 2, pl.ds(col, count, stride=wide), :].astype(out_ref.dtype)


def unpack_mats(flat, shape1, shape2, tile1, tile2):
    vmem = pl.BlockSpec(memory_space=pltpu.VMEM)
    num_chunks = math.prod(shape1) // (CHUNK_TILES * TILE)
    return pl.pallas_call(
        functools.partial(unpack_kernel, tile1=tile1, tile2=tile2),
        out_shape=(jax.ShapeDtypeStruct(shape1, flat.dtype), jax.ShapeDtypeStruct(shape2, flat.dtype)),
        in_specs=[pl.BlockSpec(memory_space=pl.ANY)],
        out_specs=(vmem, vmem),
        scratch_shapes=[
            pltpu.VMEM((2 * num_chunks, CHUNK_TILES, ROWS, LANES), flat.dtype),
            pltpu.VMEM((2, CHUNK_TILES * ROWS, LANES), jnp.float32),
            pltpu.SemaphoreType.DMA((2 * num_chunks,)),
        ],
        cost_estimate=pl.CostEstimate(flops=0, bytes_accessed=8 * math.prod(shape1), transcendentals=0),
        name='unpack_mats',
    )(flat)


def layer_norm(x_in, ln_gain, ln_shift):
    x_f = x_in.astype(jnp.float32)
    mean_val = jnp.mean(x_f, axis=-1, keepdims=True)
    var_val = jnp.mean(jnp.square(x_f - mean_val), axis=-1, keepdims=True)
    normed = (x_f - mean_val) * lax.rsqrt(var_val + LN_EPS)
    return (normed * ln_gain.astype(jnp.float32) + ln_shift.astype(jnp.float32)).astype(jnp.bfloat16)


def gelu_both(hidden):
    scale = math.sqrt(2.0 / math.pi)
    square = hidden * hidden
    tanh_val = jnp.tanh(hidden * (scale + (scale * 0.044715) * square))
    cdf = 0.5 + 0.5 * tanh_val
    slope = cdf + (0.5 * hidden) * (1.0 - tanh_val * tanh_val) * (scale + (3.0 * scale * 0.044715) * square)
    return (hidden * cdf).astype(jnp.bfloat16), slope


def norm_grad(x_in, ln_gain, ln_shift, d_normed):
    _, pullback = jax.vjp(layer_norm, x_in, ln_gain.astype(jnp.float32), ln_shift.astype(jnp.float32))
    d_x, d_gain, d_shift = pullback(d_normed.astype(jnp.bfloat16))
    return d_x.astype(jnp.float32), d_gain, d_shift


def scoped(tag, spec, lhs, rhs, **kwargs):
    with jax.named_scope(tag):
        return jnp.einsum(spec, lhs, rhs, **kwargs)


def layer_forward(x_in, weights, tag):
    w_tok1, w_tok2, w_ch1, w_ch2, ln1_g, ln1_b, b_tok1, b_tok2, ln2_g, ln2_b, b_ch1, b_ch2 = weights
    normed = layer_norm(x_in, ln1_g, ln1_b)
    hid_tok = scoped(tag + '_tok1', 'bsc,sj->bcj', normed, w_tok1, preferred_element_type=jnp.float32) + b_tok1.astype(jnp.float32)
    act_tok, slope_tok = gelu_both(hid_tok)
    with jax.named_scope(tag + '_tok2'):
        tok_out = jnp.einsum('bcj,js->bsc', act_tok, w_tok2, preferred_element_type=jnp.float32) + b_tok2.astype(jnp.float32)[:, None]
        after_tok = (x_in.astype(jnp.float32) + tok_out).astype(jnp.bfloat16)
    normed2 = layer_norm(after_tok, ln2_g, ln2_b)
    hid_ch = scoped(tag + '_ch1', 'bsc,cd->bsd', normed2, w_ch1, preferred_element_type=jnp.float32) + b_ch1.astype(jnp.float32)
    act_ch, slope_ch = gelu_both(hid_ch)
    with jax.named_scope(tag + '_ch2'):
        ch_out = jnp.einsum('bsd,dc->bsc', act_ch, w_ch2, preferred_element_type=jnp.float32) + b_ch2.astype(jnp.float32)
        layer_out = (after_tok.astype(jnp.float32) + ch_out).astype(jnp.bfloat16)
    return layer_out, (x_in, normed, slope_tok, act_tok, after_tok, normed2, slope_ch, act_ch)


def layer_backward(d_out, weights, cache, tag, flat_len, num_tokens):
    num_chans = d_out.shape[2]
    w_tok1, w_tok2, w_ch1, w_ch2, ln1_g, ln1_b, b_tok1, b_tok2, ln2_g, ln2_b, b_ch1, b_ch2 = weights
    x_in, normed, slope_tok, act_tok, after_tok, normed2, slope_ch, act_ch = cache
    d_out_bf = d_out.astype(jnp.bfloat16)
    g_b_ch2 = jnp.sum(d_out, axis=(0, 1))
    tokens = d_out.shape[0] * d_out.shape[1]
    mat_tiles = [math.prod(shape_one) // LANES for shape_one in piece_shapes(num_tokens, num_chans)[:4]]
    row1 = mat_tiles[0] + mat_tiles[1]
    d_normed2, bias_rows, flat_grad = mlp_grad(
        d_out_bf.reshape(tokens, num_chans), act_ch.reshape(tokens, -1), slope_ch.reshape(tokens, -1), normed2.reshape(tokens, num_chans),
        w_ch1, w_ch2, flat_len // LANES, row1, row1 + mat_tiles[2], tokens // 5)
    g_b_ch1 = jnp.sum(bias_rows, axis=0)
    d_normed2 = d_normed2.reshape(d_out.shape)
    with jax.named_scope(tag + '_ln2'):
        d_after_ln, g_ln2_g, g_ln2_b = norm_grad(after_tok, ln2_g, ln2_b, d_normed2)
    d_after = d_after_ln + d_out
    d_after_bf = d_after.astype(jnp.bfloat16)
    g_b_tok2 = jnp.sum(d_after, axis=(0, 2))
    g_w_tok2 = scoped(tag + '_gt2', 'bcj,bsc->js', act_tok, d_after_bf, preferred_element_type=jnp.float32)
    with jax.named_scope(tag + '_dtok'):
        d_act_tok = jnp.einsum('bsc,js->bcj', d_after_bf, w_tok2, preferred_element_type=jnp.float32)
        d_hid_tok = d_act_tok.astype(jnp.bfloat16).astype(jnp.float32) * slope_tok
        d_hid_tok_bf = d_hid_tok.astype(jnp.bfloat16)
        g_b_tok1 = jnp.sum(d_hid_tok, axis=(0, 1))
    g_w_tok1 = scoped(tag + '_gt1', 'bsc,bcj->sj', normed, d_hid_tok_bf, preferred_element_type=jnp.float32)
    d_normed = scoped(tag + '_dnt', 'bcj,sj->bsc', d_hid_tok_bf, w_tok1, preferred_element_type=jnp.float32)
    d_in_ln, g_ln1_g, g_ln1_b = norm_grad(x_in, ln1_g, ln1_b, d_normed)
    d_in = d_in_ln + d_after
    vectors = jnp.concatenate([g_ln1_g, g_ln1_b, g_b_tok1, g_b_tok2[:num_tokens], g_ln2_g, g_ln2_b, g_b_ch1, g_b_ch2])
    last_row = row1 + mat_tiles[2] + mat_tiles[3]
    vectors = jnp.pad(vectors, (0, flat_len - last_row * LANES - vectors.shape[0])).reshape(-1, LANES)
    tok_rows = jnp.concatenate([g_w_tok1[:num_tokens].reshape(-1, LANES), g_w_tok2[:, :num_tokens].reshape(-1, LANES)], axis=0)
    flat_grad = lax.dynamic_update_slice(flat_grad, tok_rows, (0, 0))
    flat_grad = lax.dynamic_update_slice(flat_grad, vectors, (last_row, 0))
    return d_in, flat_grad


def head_step(hidden, labels, small_full, head_full, num_classes, global_b, num_tokens):
    num_chans = hidden.shape[2]
    lnf_g = small_full[:num_chans]
    lnf_b = small_full[num_chans:2 * num_chans]
    head_b = small_full[2 * num_chans:2 * num_chans + num_classes]
    normed = layer_norm(hidden, lnf_g, lnf_b)
    pooled = (jnp.sum(normed[:, :num_tokens], axis=1, dtype=jnp.float32) / num_tokens).astype(jnp.bfloat16)
    is_class = jnp.arange(HEAD_PAD)[None, :] < num_classes
    logits = jnp.dot(pooled, head_full, preferred_element_type=jnp.float32) + jnp.pad(head_b.astype(jnp.float32), (0, HEAD_PAD - num_classes))
    logits = jnp.where(is_class, logits, -jnp.inf)
    log_norm = jax.nn.logsumexp(logits, axis=-1)
    is_label = jnp.arange(HEAD_PAD)[None, :] == labels[:, None]
    picked = jnp.sum(jnp.where(is_label, logits, 0.0), axis=-1)
    loss_sum = jnp.sum(log_norm - picked)
    d_logits = (jnp.exp(logits - log_norm[:, None]) - is_label.astype(jnp.float32)) / global_b
    d_logits_bf = d_logits.astype(jnp.bfloat16)
    g_head_b = jnp.sum(d_logits, axis=0)[:num_classes]
    g_head_w = jnp.einsum('bc,bk->ck', pooled, d_logits_bf, preferred_element_type=jnp.float32)
    d_pooled = jnp.einsum('bk,ck->bc', d_logits_bf, head_full, preferred_element_type=jnp.float32)
    is_token = jnp.arange(hidden.shape[1])[None, :, None] < num_tokens
    d_normed = jnp.where(is_token, (d_pooled / num_tokens)[:, None, :], 0.0)
    d_hidden, g_lnf_g, g_lnf_b = norm_grad(hidden, lnf_g, lnf_b, d_normed)
    g_small = jnp.concatenate([g_lnf_g, g_lnf_b, g_head_b])
    return loss_sum, d_hidden, g_head_w, g_small


def adam_update(master, gradient, moment, second, decay_rate):
    moment_new = BETA_ONE * moment + (1.0 - BETA_ONE) * gradient
    second_new = BETA_TWO * second + (1.0 - BETA_TWO) * gradient * gradient
    m_hat = moment_new / (1.0 - BETA_ONE ** ADAM_STEP)
    v_hat = second_new / (1.0 - BETA_TWO ** ADAM_STEP)
    master_new = master - LEARN_RATE * (m_hat / (jnp.sqrt(v_hat) + ADAM_EPS) + decay_rate * master)
    return master_new, moment_new, second_new


def solution(mesh):
    row_spec = P(AXIS)
    layer_spec = P(None, AXIS)
    in_specs = (row_spec, row_spec, layer_spec, row_spec, row_spec, layer_spec, row_spec, row_spec, layer_spec, row_spec, row_spec)
    out_specs = (P(),) + in_specs[2:]

    def device_step(act_in, labels, layer_p, head_w, small_p, layer_m, head_m, small_m, layer_v, head_v, small_v):
        local_b, num_tokens, num_chans = act_in.shape
        global_b = local_b * GROUP
        num_layers, share_len = layer_p.shape
        flat_len = share_len * GROUP
        head_rows, num_classes = head_w.shape
        small_len = small_p.shape[0]
        mat_len = 2 * num_tokens * (num_chans // 2) + 8 * num_chans * num_chans

        windows = [share_to_window(layer_p[layer_idx].astype(jnp.bfloat16)) for layer_idx in range(num_layers)]
        win_tiles = windows[0].shape[0]
        head_tiles = head_to_tiles(head_w.astype(jnp.bfloat16))
        small_tile = jnp.pad(small_p.astype(jnp.bfloat16).reshape(1, 1, small_len), ((0, 0), (0, ROWS - 1), (0, 0)))
        num_head = head_tiles.shape[0]
        flat0, flat1, extra = gather_shares(windows[0], windows[1], jnp.concatenate([head_tiles, small_tile], axis=0))

        weights = []
        caches = []
        hidden = pad_tokens(act_in, 1, num_tokens)
        for layer_idx, flat in enumerate((flat0, flat1)):
            weights.append(unpack_tiles(flat.reshape(-1, ROWS, LANES), num_tokens, num_chans))
            hidden, cache = layer_forward(hidden, weights[layer_idx], f'f{layer_idx}')
            caches.append(cache)
        head_full = tiles_to_head(extra[:, :num_head], head_rows * GROUP)
        small_full = extra[:, num_head, 0].reshape(-1)
        loss_sum, d_hidden, g_head_w, g_small = head_step(hidden, labels, small_full, head_full, num_classes, global_b, num_tokens)

        head_blocks = head_to_tiles(g_head_w).reshape(GROUP, num_head, ROWS, LANES)
        g_small = jnp.pad(g_small, (0, small_len * GROUP - g_small.shape[0])).reshape(GROUP, 1, 1, small_len)
        small_blocks = jnp.pad(g_small, ((0, 0), (0, 0), (0, ROWS - 1), (0, 0)))
        packed = [None] * num_layers
        for layer_idx in reversed(range(num_layers)):
            d_hidden, flat_grad = layer_backward(d_hidden, weights[layer_idx], caches[layer_idx], f'b{layer_idx}', flat_len, num_tokens)
            packed[layer_idx] = flat_grad.reshape(flat0.shape)
        loss_tile = jnp.pad(loss_sum.reshape(1, 1), ((0, ROWS - 1), (0, LANES - 1)))
        extra_blocks = jnp.concatenate([head_blocks, small_blocks], axis=1)
        summed0, summed1, sums = scatter_grads(packed[0], packed[1], extra_blocks, loss_tile, win_tiles, share_len // LANES)
        layer_g = jnp.stack([window_to_share(summed0, share_len), window_to_share(summed1[:win_tiles], share_len)])
        head_g = tiles_to_head(summed1[win_tiles:win_tiles + num_head], head_rows)[:, :num_classes]
        small_g = summed1[win_tiles + num_head, 0]

        sq_total, loss_total = jnp.sum(sums[0]), jnp.sum(sums[1])
        loss_value = loss_total / global_b
        clip_scale = 1.0 / jnp.maximum(1.0, jnp.sqrt(sq_total))
        flat_pos = lax.axis_index(AXIS) * share_len + jnp.arange(share_len)
        layer_decay = jnp.where(flat_pos < mat_len, WEIGHT_DECAY, 0.0)[None, :]
        new_lp, new_lm, new_lv = adam_update(layer_p, layer_g * clip_scale, layer_m, layer_v, layer_decay)
        new_hw, new_hm, new_hv = adam_update(head_w, head_g * clip_scale, head_m, head_v, WEIGHT_DECAY)
        new_sp, new_sm, new_sv = adam_update(small_p, small_g * clip_scale, small_m, small_v, 0.0)
        return (loss_value, new_lp, new_hw, new_sp, new_lm, new_hm, new_sm, new_lv, new_hv, new_sv)

    return jax.shard_map(device_step, mesh=mesh, in_specs=in_specs, out_specs=out_specs, check_vma=False)
```

```python
import functools
import math
import jax
import jax.numpy as jnp
from jax import lax
from jax.experimental import pallas as pl
from jax.experimental.pallas import tpu as pltpu
from jax.sharding import PartitionSpec as P

LN_EPS = 1e-6
LEARN_RATE = 0.003
BETA_ONE = 0.9
BETA_TWO = 0.999
ADAM_EPS = 1e-8
WEIGHT_DECAY = 0.03
ADAM_STEP = 10
AXIS = 'fsdp'
GROUP = 32
ROWS = 8
LANES = 128
TILE = ROWS * LANES
HEAD_PAD = 1024
IMAGE_ROWS = 8

def row_offset(share_rows):
    return (lax.axis_index(AXIS) * share_rows) % ROWS


def share_to_window(share):
    share_rows = share.shape[0] // LANES
    num_tiles = -(-(share_rows + ROWS - 2) // ROWS)
    window = jnp.zeros((num_tiles * ROWS, LANES), share.dtype)
    window = lax.dynamic_update_slice(window, share.reshape(share_rows, LANES), (row_offset(share_rows), 0))
    return window.reshape(num_tiles, ROWS, LANES)


def window_to_share(window, share_len):
    share_rows = share_len // LANES
    rows = window.reshape(-1, LANES)
    return lax.dynamic_slice(rows, (row_offset(share_rows), 0), (share_rows, LANES)).reshape(share_len)


def piece_shapes(num_tokens, num_chans):
    tok_hid = num_chans // 2
    ch_hid = 4 * num_chans
    return [(num_tokens, tok_hid), (tok_hid, num_tokens), (num_chans, ch_hid), (ch_hid, num_chans), (num_chans,), (num_chans,), (tok_hid,), (num_tokens,), (num_chans,), (num_chans,), (ch_hid,), (num_chans,)]


def pad_tokens(val, axis, num_tokens):
    widths = [(0, 0)] * val.ndim
    widths[axis] = (0, -num_tokens % IMAGE_ROWS)
    return jnp.pad(val, widths)


def unpack_tiles(tiles, num_tokens, num_chans):
    pieces = []
    start = 0
    shapes = piece_shapes(num_tokens, num_chans)
    for shape_one in shapes[:4]:
        count = math.prod(shape_one) // TILE
        pieces.append(tiles[start:start + count].reshape(shape_one) if len(pieces) < 2 else None)
        start = start + count
    flat = tiles[start:].reshape(-1)
    start = 0
    for shape_one in shapes[4:]:
        pieces.append(flat[start:start + shape_one[0]])
        start = start + shape_one[0]
    pieces[0] = pad_tokens(pieces[0], 0, num_tokens)
    pieces[1] = pad_tokens(pieces[1], 1, num_tokens)
    tile1 = 2 * math.prod(shapes[0]) // TILE
    pieces[2], pieces[3] = unpack_mats(tiles, shapes[2], shapes[3], tile1, tile1 + math.prod(shapes[2]) // TILE)
    pieces[7] = pad_tokens(pieces[7], 0, num_tokens)
    return pieces


def head_to_tiles(head):
    rows = head.shape[0]
    head = jnp.pad(head, ((0, 0), (0, HEAD_PAD - head.shape[1])))
    return head.reshape(rows // ROWS, ROWS, HEAD_PAD // LANES, LANES).transpose(0, 2, 1, 3).reshape(-1, ROWS, LANES)


def tiles_to_head(tiles, rows):
    tiles = tiles.reshape(rows // ROWS, HEAD_PAD // LANES, ROWS, LANES)
    return tiles.transpose(0, 2, 1, 3).reshape(rows, HEAD_PAD)


MASK_CORE, MASK_X, MASK_Y, MASK_Z = 1, 2, 4, 8
PARTNERS = (MASK_CORE, MASK_X, MASK_Y, MASK_Z, 2 * MASK_Z, 3 * MASK_Z)
PERIOD = 4


class Peers:
    def __init__(self, me):
        self.bits = []
        for bit in range(5):
            val = lax.rem(lax.div(me, 1 << bit), 2)
            self.bits.append((val, 1 - val))
        self.known = {}

    def split(self, rel):
        if rel not in self.known:
            vals = [self.bits[bit][(rel >> bit) & 1] for bit in range(5)]
            pos = vals[0] + 2 * vals[1]
            group = vals[2] + 2 * vals[3] + 4 * vals[4]
            self.known[rel] = (group * PERIOD + pos, group, pos)
        return self.known[rel]

    def device(self, rel):
        return self.split(rel)[0]


def meet_all(me):
    barrier = pltpu.get_barrier_semaphore()
    for step in range(1, GROUP):
        pl.semaphore_signal(barrier, inc=1, device_id=(lax.rem(me + step, GROUP),), device_id_type=pl.DeviceIdType.MESH)
    pl.semaphore_wait(barrier, GROUP - 1)


def meet_partners(peers):
    barrier = pltpu.get_barrier_semaphore()
    for mask in PARTNERS:
        pl.semaphore_signal(barrier, inc=1, device_id=(peers.device(mask),), device_id_type=pl.DeviceIdType.MESH)
    pl.semaphore_wait(barrier, len(PARTNERS))


def gather_kernel(inner0_ref, inner1_ref, misc_ref, flat0_ref, flat1_ref, extra_ref, misc_all, bound, local_sems, send_sems, recv_sems):
    peers = Peers(lax.axis_index(AXIS))
    inner = inner0_ref.shape[0]
    stride = inner + 1
    own_refs = (inner0_ref, inner1_ref, misc_ref)
    colours = ((MASK_Y, MASK_X), (MASK_X, MASK_Y), (MASK_X, MASK_Y))

    def place(arr, rel):
        dev, group, pos = peers.split(rel)
        if arr == 2:
            return misc_all.at[dev]
        flat = (flat0_ref, flat1_ref)[arr]
        return flat.at[group, pl.ds(stride * pos + 1, inner)]

    own_copies = [pltpu.make_async_copy(own_refs[arr], place(arr, 0), local_sems.at[arr]) for arr in range(3)]
    for copy in own_copies:
        copy.start()
    meet_partners(peers)
    sends = []

    def send(arr, rel, mask):
        here = place(arr, rel)
        copy = pltpu.make_async_remote_copy(
            src_ref=own_refs[arr] if rel == 0 else here, dst_ref=here,
            send_sem=send_sems.at[arr, rel ^ mask], recv_sem=recv_sems.at[arr, rel ^ mask],
            device_id=(peers.device(mask),), device_id_type=pl.DeviceIdType.MESH)
        copy.start()
        sends.append(copy)

    def receive(arr, rel):
        here = place(arr, rel)
        pltpu.make_async_remote_copy(
            src_ref=here, dst_ref=here, send_sem=send_sems.at[arr, rel], recv_sem=recv_sems.at[arr, rel],
            device_id=(peers.device(0),), device_id_type=pl.DeviceIdType.MESH).wait_recv()

    for mask_pos in range(6):
        for arr in range(3):
            first, second = colours[arr]
            send(arr, 0, (MASK_Z, first, second, 2 * MASK_Z, 3 * MASK_Z, MASK_CORE)[mask_pos])
    for dist, use_first, use_second in ((0, 1, 0), (1, 0, 0), (0, 0, 1), (1, 1, 0), (0, 1, 1), (2, 0, 0), (1, 0, 1), (2, 1, 0),
                                        (1, 1, 1), (3, 0, 0), (2, 0, 1), (3, 1, 0), (2, 1, 1), (3, 0, 1), (3, 1, 1)):
        for arr in range(3):
            first, second = colours[arr]
            rel = dist * MASK_Z + use_first * first + use_second * second
            receive(arr, rel)
            if not use_second:
                if not use_first:
                    send(arr, rel, first)
                send(arr, rel, second)
            send(arr, rel, MASK_CORE)
    for rel in range(MASK_CORE, GROUP, 2):
        for arr in range(3):
            receive(arr, rel)
    for copy in own_copies:
        copy.wait()
    for copy in sends:
        copy.wait_send()

    for layer_idx in range(2):
        for group in range(GROUP // PERIOD):
            for pos in range(PERIOD + 1):
                tile = None
                if pos < PERIOD:
                    tile = misc_all[group * PERIOD + pos, 2 * layer_idx]
                if pos > 0:
                    left = misc_all[group * PERIOD + pos - 1, 2 * layer_idx + 1]
                    tile = left if tile is None else tile + left
                bound[layer_idx, pos, group, 0] = tile
    extra_ref[...] = misc_all[:, 4:]
    edges = []
    for layer_idx in range(2):
        flat = (flat0_ref, flat1_ref)[layer_idx]
        for pos in range(PERIOD + 1):
            edges.append(pltpu.make_async_copy(bound.at[layer_idx, pos], flat.at[:, pl.ds(stride * pos, 1)], local_sems.at[3 + layer_idx * (PERIOD + 1) + pos]))
    for copy in edges:
        copy.start()
    for copy in edges:
        copy.wait()


def gather_shares(window0, window1, extra):
    num_tiles = window0.shape[0]
    num_extra = extra.shape[0]
    inner = num_tiles - 2
    misc = jnp.concatenate([window0[:1], window0[-1:], window1[:1], window1[-1:], extra], axis=0)
    flat = (GROUP // PERIOD, PERIOD * (num_tiles - 1) + 1, ROWS, LANES)
    vmem = pl.BlockSpec(memory_space=pltpu.VMEM)
    hbm = pl.BlockSpec(memory_space=pl.ANY)
    dtype = window0.dtype
    return pl.pallas_call(
        gather_kernel,
        out_shape=(jax.ShapeDtypeStruct(flat, dtype), jax.ShapeDtypeStruct(flat, dtype), jax.ShapeDtypeStruct((GROUP, num_extra, ROWS, LANES), dtype)),
        in_specs=[vmem] * 3,
        out_specs=(hbm, hbm, vmem),
        scratch_shapes=[
            pltpu.VMEM((GROUP, num_extra + 4, ROWS, LANES), dtype),
            pltpu.VMEM((2, PERIOD + 1, GROUP // PERIOD, 1, ROWS, LANES), dtype),
            pltpu.SemaphoreType.DMA((3 + 2 * (PERIOD + 1),)),
            pltpu.SemaphoreType.DMA((3, GROUP)),
            pltpu.SemaphoreType.DMA((3, GROUP)),
        ],
        compiler_params=pltpu.CompilerParams(collective_id=1, has_side_effects=True),
        name='gather_shares',
    )(window0[1:-1], window1[1:-1], misc)


def scatter_kernel(grad0_ref, grad1_ref, extra_ref, loss_ref, out0_ref, out1_ref, sums_ref, own0, own1, core0, core1, first0, first1, second0, second1, far0, far1,
                   partial, held, load_sems, send_sems, core_sems, first_sems, second_sems, far_sems, sum_load_sem, sum_send_sems, sum_recv_sems, *, share_rows):
    me = lax.axis_index(AXIS)
    peers = Peers(me)
    num_tiles = out0_ref.shape[0]
    num_extra = extra_ref.shape[1]
    own, near, first_in, second_in, far_in = (own0, own1), (core0, core1), (first0, first1), (second0, second1), (far0, far1)
    colours = ((MASK_X, MASK_Y), (MASK_Y, MASK_X))
    dists = (3, 2, 1, 0)
    sends = []

    def source(part, rel):
        dev, group, pos = peers.split(rel)
        if part == 2:
            return extra_ref.at[dev]
        grad = (grad0_ref, grad1_ref)[part]
        return grad.at[group, pl.ds((num_tiles - 1) * pos, num_tiles)]

    def slot(part, buffers, pos):
        if part == 2:
            return buffers[1].at[pos, pl.ds(num_tiles, num_extra)]
        return buffers[part].at[pos, pl.ds(0, num_tiles)]

    def post(src, dst, send_sem, recv_sem, mask):
        copy = pltpu.make_async_remote_copy(src_ref=src, dst_ref=dst, send_sem=send_sem, recv_sem=recv_sem,
                                            device_id=(peers.device(mask),), device_id_type=pl.DeviceIdType.MESH)
        copy.start()
        sends.append(copy)

    def expect(dst, send_sem, recv_sem):
        pltpu.make_async_remote_copy(src_ref=dst, dst_ref=dst, send_sem=send_sem, recv_sem=recv_sem,
                                     device_id=(peers.device(0),), device_id_type=pl.DeviceIdType.MESH).wait_recv()

    def targets(dist):
        return [(dist * 4 + pos, dist * MASK_Z + pos * MASK_X) for pos in (3, 2, 1, 0)]

    loads = {}
    for dist in dists:
        for pos, rel in targets(dist):
            for part in range(3):
                loads[part, pos] = pltpu.make_async_copy(source(part, rel), slot(part, own, pos), load_sems.at[part, pos])
                loads[part, pos].start()
    loss_copy = pltpu.make_async_copy(loss_ref, partial.at[1], sum_load_sem.at[0])
    loss_copy.start()
    meet_all(me)
    for dist in dists:
        for pos, rel in targets(dist):
            for part in range(3):
                post(source(part, rel | MASK_CORE), slot(part, near, pos), send_sems.at[part, pos], core_sems.at[part, pos], MASK_CORE)

    def fold_core(dist):
        for pos, rel in targets(dist):
            for part in range(3):
                loads[part, pos].wait()
                expect(slot(part, near, pos), send_sems.at[part, pos], core_sems.at[part, pos])
            for side in range(2):
                own[side][pos] += near[side][pos]
        for side in range(2):
            mask, other = colours[side]
            for which in (1, 0):
                pos = dist * 4 + (mask + which * other) // MASK_X
                index = dist * 2 + which
                post(own[side].at[pos], first_in[side].at[index], send_sems.at[3 + side, index], first_sems.at[side, index], mask)

    def fold_first(dist):
        for side in range(2):
            mask, other = colours[side]
            for which in (1, 0):
                pos = dist * 4 + which * other // MASK_X
                index = dist * 2 + which
                expect(first_in[side].at[index], send_sems.at[3 + side, index], first_sems.at[side, index])
                own[side][pos] += first_in[side][index]
        for side in range(2):
            mask, other = colours[side]
            post(own[side].at[dist * 4 + other // MASK_X], second_in[side].at[dist], send_sems.at[3 + side, 8 + dist], second_sems.at[side, dist], other)

    def fold_second(dist):
        for side in range(2):
            expect(second_in[side].at[dist], send_sems.at[3 + side, 8 + dist], second_sems.at[side, dist])
            own[side][dist * 4] += second_in[side][dist]
        if dist:
            for side in range(2):
                post(own[side].at[dist * 4], far_in[side].at[dist - 1], send_sems.at[3 + side, 12 + dist], far_sems.at[side, dist - 1], dist * MASK_Z)

    fold_core(3)
    fold_core(2)
    fold_first(3)
    fold_core(1)
    fold_first(2)
    fold_second(3)
    fold_core(0)
    fold_first(1)
    fold_second(2)
    fold_first(0)
    fold_second(1)
    fold_second(0)
    for side in range(2):
        total = own[side][0]
        for dist in (3, 2, 1):
            expect(far_in[side].at[dist - 1], send_sems.at[3 + side, 12 + dist], far_sems.at[side, dist - 1])
            total = total + far_in[side][dist - 1]
        (out0_ref, out1_ref)[side][...] = total

    first_row = 2 * peers.split(0)[2] if share_rows % ROWS == 2 else lax.rem(share_rows * me, ROWS)
    row = lax.broadcasted_iota(jnp.int32, (ROWS, LANES), 0)
    squares = jnp.zeros((ROWS, LANES), jnp.float32)
    for out_ref in (out0_ref, out1_ref):
        head = jnp.where(row >= first_row, out_ref[0], 0.0)
        tail = jnp.where(row < first_row + share_rows % ROWS, out_ref[num_tiles - 1], 0.0)
        inner = out_ref[1:num_tiles - 1]
        squares = squares + head * head + tail * tail + jnp.sum(inner * inner, axis=0)
    rest = out1_ref[num_tiles:]
    partial[0] = squares + jnp.sum(rest * rest, axis=0)
    for copy in sends:
        copy.wait_send()
    loss_copy.wait()
    mine = pltpu.make_async_copy(partial, held.at[me], sum_load_sem.at[1])
    mine.start()
    posts = []
    for step in range(1, GROUP):
        copy = pltpu.make_async_remote_copy(
            src_ref=partial, dst_ref=held.at[me], send_sem=sum_send_sems.at[step], recv_sem=sum_recv_sems.at[me],
            device_id=(lax.rem(me + step, GROUP),), device_id_type=pl.DeviceIdType.MESH)
        copy.start()
        posts.append(copy)
    mine.wait()
    for step in range(1, GROUP):
        peer = lax.rem(me + step, GROUP)
        pltpu.make_async_remote_copy(
            src_ref=partial, dst_ref=held.at[peer], send_sem=sum_send_sems.at[step], recv_sem=sum_recv_sems.at[peer],
            device_id=(peer,), device_id_type=pl.DeviceIdType.MESH).wait_recv()
    for copy in posts:
        copy.wait_send()
    sums_ref[...] = jnp.sum(held[...], axis=0)


def scatter_grads(grad0, grad1, extra, loss_tile, num_tiles, share_rows):
    num_extra = extra.shape[1]
    sizes = (num_tiles, num_tiles + num_extra)
    vmem = pl.BlockSpec(memory_space=pltpu.VMEM)
    hbm = pl.BlockSpec(memory_space=pl.ANY)

    def buffers(count):
        return [pltpu.VMEM((count, size, ROWS, LANES), jnp.float32) for size in sizes]

    return pl.pallas_call(
        functools.partial(scatter_kernel, share_rows=share_rows),
        out_shape=tuple(jax.ShapeDtypeStruct((size, ROWS, LANES), jnp.float32) for size in sizes + (2,)),
        in_specs=[hbm] * 3 + [vmem],
        out_specs=(vmem, vmem, vmem),
        scratch_shapes=buffers(16) + buffers(16) + buffers(8) + buffers(4) + buffers(3) + [
            pltpu.VMEM((2, ROWS, LANES), jnp.float32),
            pltpu.VMEM((GROUP, 2, ROWS, LANES), jnp.float32),
            pltpu.SemaphoreType.DMA((3, 16)),
            pltpu.SemaphoreType.DMA((5, 16)),
            pltpu.SemaphoreType.DMA((3, 16)),
            pltpu.SemaphoreType.DMA((2, 8)),
            pltpu.SemaphoreType.DMA((2, 4)),
            pltpu.SemaphoreType.DMA((2, 3)),
            pltpu.SemaphoreType.DMA((2,)),
            pltpu.SemaphoreType.DMA((GROUP,)),
            pltpu.SemaphoreType.DMA((GROUP,)),
        ],
        compiler_params=pltpu.CompilerParams(collective_id=2, has_side_effects=True),
        name='scatter_grads',
    )(grad0, grad1, extra, loss_tile)


NT_DIMS = (((1,), (1,)), ((), ()))
NN_DIMS = (((1,), (0,)), ((), ()))
HID_CHUNK = 512


def mlp_grad_kernel(d_out_ref, act_ref, slope_ref, normed_ref, w1_ref, w2_ref, d_normed_ref, bias_ref, flat_ref, acc1, acc2, staged, sems, *, row1, row2):
    step = pl.program_id(0)
    chans, hid = acc1.shape

    @pl.when(step == 0)
    def _():
        acc1[...] = jnp.zeros_like(acc1)
        acc2[...] = jnp.zeros_like(acc2)
        bias_ref[...] = jnp.zeros_like(bias_ref)

    d_out = d_out_ref[...]
    d_out_t = d_out.T
    normed_t = normed_ref[...].T
    d_normed = None
    for start in range(0, hid, HID_CHUNK):
        cols = pl.ds(start, HID_CHUNK)
        d_act = lax.dot_general(d_out, w2_ref[cols, :], NT_DIMS, preferred_element_type=jnp.float32)
        acc2[:, cols] += lax.dot_general(d_out_t, act_ref[:, cols], NN_DIMS, preferred_element_type=jnp.float32)
        d_hid = d_act.astype(jnp.bfloat16).astype(jnp.float32) * slope_ref[:, cols]
        bias_ref[:, cols] += jnp.sum(d_hid.reshape(-1, ROWS, HID_CHUNK), axis=0)
        d_hid_bf = d_hid.astype(jnp.bfloat16)
        acc1[:, cols] += lax.dot_general(normed_t, d_hid_bf, NN_DIMS, preferred_element_type=jnp.float32)
        part = lax.dot_general(d_hid_bf, w1_ref[:, cols], NT_DIMS, preferred_element_type=jnp.float32)
        d_normed = part if d_normed is None else d_normed + part
    d_normed_ref[...] = d_normed.astype(d_normed_ref.dtype)

    @pl.when(step == pl.num_programs(0) - 1)
    def _():
        wide = hid // LANES
        for col in range(wide):
            staged[0, pl.ds(col, chans, stride=wide), :] = acc1[:, col * LANES:(col + 1) * LANES]
        first = pltpu.make_async_copy(staged.at[0], flat_ref.at[pl.ds(row1, chans * wide)], sems.at[0])
        first.start()
        narrow = chans // LANES
        for col in range(narrow):
            staged[1, pl.ds(col, hid, stride=narrow), :] = acc2[col * LANES:(col + 1) * LANES, :].T
        second = pltpu.make_async_copy(staged.at[1], flat_ref.at[pl.ds(row2, chans * wide)], sems.at[1])
        second.start()
        first.wait()
        second.wait()


def mlp_grad(d_out, act, slope, normed, w1, w2, flat_rows, row1, row2, block):
    tokens, chans = d_out.shape
    hid = act.shape[1]

    def by_block(width):
        return pl.BlockSpec((block, width), lambda step: (step, 0))

    def whole(shape):
        return pl.BlockSpec(shape, lambda step: (0, 0), pipeline_mode=pl.Buffered(1))

    mat_rows = chans * hid // LANES
    return pl.pallas_call(
        functools.partial(mlp_grad_kernel, row1=row1, row2=row2),
        grid=(tokens // block,),
        out_shape=(
            jax.ShapeDtypeStruct((tokens, chans), jnp.bfloat16),
            jax.ShapeDtypeStruct((ROWS, hid), jnp.float32),
            jax.ShapeDtypeStruct((flat_rows, LANES), jnp.float32),
        ),
        in_specs=[by_block(chans), by_block(hid), by_block(hid), by_block(chans), whole(w1.shape), whole(w2.shape)],
        out_specs=(by_block(chans), pl.BlockSpec((ROWS, hid), lambda step: (0, 0)), pl.BlockSpec(memory_space=pl.ANY)),
        scratch_shapes=[
            pltpu.VMEM((chans, hid), jnp.float32),
            pltpu.VMEM((chans, hid), jnp.float32),
            pltpu.VMEM((2, mat_rows, LANES), jnp.float32),
            pltpu.SemaphoreType.DMA((2,)),
        ],
        compiler_params=pltpu.CompilerParams(dimension_semantics=('arbitrary',), vmem_limit_bytes=60 * 1024 * 1024),
        cost_estimate=pl.CostEstimate(flops=8 * tokens * chans * hid, bytes_accessed=6 * tokens * hid + 6 * tokens * chans + 12 * chans * hid, transcendentals=0),
        name='mlp_grad',
    )(d_out, act, slope, normed, w1, w2)


CHUNK_TILES = 128


def unpack_kernel(flat_ref, w1_ref, w2_ref, raw, spread, sems, *, tile1, tile2):
    chans, hid = w1_ref.shape
    num_chunks = chans * hid // (CHUNK_TILES * TILE)
    copies = []
    for mat, first in enumerate((tile1, tile2)):
        for chunk in range(num_chunks):
            pos = mat * num_chunks + chunk
            copies.append(pltpu.make_async_copy(flat_ref.at[pl.ds(first + chunk * CHUNK_TILES, CHUNK_TILES)], raw.at[pos], sems.at[pos]))
            copies[-1].start()
    for mat, out_ref in enumerate((w1_ref, w2_ref)):
        wide = out_ref.shape[1] // LANES
        count = CHUNK_TILES * ROWS // wide
        for chunk in range(num_chunks):
            pos = mat * num_chunks + chunk
            copies[pos].wait()
            spread[pos % 2] = raw[pos].astype(jnp.float32).reshape(CHUNK_TILES * ROWS, LANES)
            for col in range(wide):
                out_ref[chunk * count:(chunk + 1) * count, col * LANES:(col + 1) * LANES] = spread[pos % 2, pl.ds(col, count, stride=wide), :].astype(out_ref.dtype)


def unpack_mats(flat, shape1, shape2, tile1, tile2):
    vmem = pl.BlockSpec(memory_space=pltpu.VMEM)
    num_chunks = math.prod(shape1) // (CHUNK_TILES * TILE)
    return pl.pallas_call(
        functools.partial(unpack_kernel, tile1=tile1, tile2=tile2),
        out_shape=(jax.ShapeDtypeStruct(shape1, flat.dtype), jax.ShapeDtypeStruct(shape2, flat.dtype)),
        in_specs=[pl.BlockSpec(memory_space=pl.ANY)],
        out_specs=(vmem, vmem),
        scratch_shapes=[
            pltpu.VMEM((2 * num_chunks, CHUNK_TILES, ROWS, LANES), flat.dtype),
            pltpu.VMEM((2, CHUNK_TILES * ROWS, LANES), jnp.float32),
            pltpu.SemaphoreType.DMA((2 * num_chunks,)),
        ],
        cost_estimate=pl.CostEstimate(flops=0, bytes_accessed=8 * math.prod(shape1), transcendentals=0),
        name='unpack_mats',
    )(flat)


def layer_norm(x_in, ln_gain, ln_shift):
    x_f = x_in.astype(jnp.float32)
    mean_val = jnp.mean(x_f, axis=-1, keepdims=True)
    var_val = jnp.mean(jnp.square(x_f - mean_val), axis=-1, keepdims=True)
    normed = (x_f - mean_val) * lax.rsqrt(var_val + LN_EPS)
    return (normed * ln_gain.astype(jnp.float32) + ln_shift.astype(jnp.float32)).astype(jnp.bfloat16)


def gelu_both(hidden):
    scale = math.sqrt(2.0 / math.pi)
    square = hidden * hidden
    tanh_val = jnp.tanh(hidden * (scale + (scale * 0.044715) * square))
    cdf = 0.5 + 0.5 * tanh_val
    slope = cdf + (0.5 * hidden) * (1.0 - tanh_val * tanh_val) * (scale + (3.0 * scale * 0.044715) * square)
    return (hidden * cdf).astype(jnp.bfloat16), slope


def norm_grad(x_in, ln_gain, ln_shift, d_normed):
    _, pullback = jax.vjp(layer_norm, x_in, ln_gain.astype(jnp.float32), ln_shift.astype(jnp.float32))
    d_x, d_gain, d_shift = pullback(d_normed.astype(jnp.bfloat16))
    return d_x.astype(jnp.float32), d_gain, d_shift


def scoped(tag, spec, lhs, rhs, **kwargs):
    with jax.named_scope(tag):
        return jnp.einsum(spec, lhs, rhs, **kwargs)


def layer_forward(x_in, weights, tag):
    w_tok1, w_tok2, w_ch1, w_ch2, ln1_g, ln1_b, b_tok1, b_tok2, ln2_g, ln2_b, b_ch1, b_ch2 = weights
    normed = layer_norm(x_in, ln1_g, ln1_b)
    hid_tok = scoped(tag + '_tok1', 'bsc,sj->bcj', normed, w_tok1, preferred_element_type=jnp.float32) + b_tok1.astype(jnp.float32)
    act_tok, slope_tok = gelu_both(hid_tok)
    with jax.named_scope(tag + '_tok2'):
        tok_out = jnp.einsum('bcj,js->bsc', act_tok, w_tok2, preferred_element_type=jnp.float32) + b_tok2.astype(jnp.float32)[:, None]
        after_tok = (x_in.astype(jnp.float32) + tok_out).astype(jnp.bfloat16)
    normed2 = layer_norm(after_tok, ln2_g, ln2_b)
    hid_ch = scoped(tag + '_ch1', 'bsc,cd->bsd', normed2, w_ch1, preferred_element_type=jnp.float32) + b_ch1.astype(jnp.float32)
    act_ch, slope_ch = gelu_both(hid_ch)
    with jax.named_scope(tag + '_ch2'):
        ch_out = jnp.einsum('bsd,dc->bsc', act_ch, w_ch2, preferred_element_type=jnp.float32) + b_ch2.astype(jnp.float32)
        layer_out = (after_tok.astype(jnp.float32) + ch_out).astype(jnp.bfloat16)
    return layer_out, (x_in, normed, slope_tok, act_tok, after_tok, normed2, slope_ch, act_ch)


def layer_backward(d_out, weights, cache, tag, flat_len, num_tokens):
    num_chans = d_out.shape[2]
    w_tok1, w_tok2, w_ch1, w_ch2, ln1_g, ln1_b, b_tok1, b_tok2, ln2_g, ln2_b, b_ch1, b_ch2 = weights
    x_in, normed, slope_tok, act_tok, after_tok, normed2, slope_ch, act_ch = cache
    d_out_bf = d_out.astype(jnp.bfloat16)
    g_b_ch2 = jnp.sum(d_out, axis=(0, 1))
    tokens = d_out.shape[0] * d_out.shape[1]
    mat_tiles = [math.prod(shape_one) // LANES for shape_one in piece_shapes(num_tokens, num_chans)[:4]]
    row1 = mat_tiles[0] + mat_tiles[1]
    d_normed2, bias_rows, flat_grad = mlp_grad(
        d_out_bf.reshape(tokens, num_chans), act_ch.reshape(tokens, -1), slope_ch.reshape(tokens, -1), normed2.reshape(tokens, num_chans),
        w_ch1, w_ch2, flat_len // LANES, row1, row1 + mat_tiles[2], tokens // 4)
    g_b_ch1 = jnp.sum(bias_rows, axis=0)
    d_normed2 = d_normed2.reshape(d_out.shape)
    with jax.named_scope(tag + '_ln2'):
        d_after_ln, g_ln2_g, g_ln2_b = norm_grad(after_tok, ln2_g, ln2_b, d_normed2)
    d_after = d_after_ln + d_out
    d_after_bf = d_after.astype(jnp.bfloat16)
    g_b_tok2 = jnp.sum(d_after, axis=(0, 2))
    g_w_tok2 = scoped(tag + '_gt2', 'bcj,bsc->js', act_tok, d_after_bf, preferred_element_type=jnp.float32)
    with jax.named_scope(tag + '_dtok'):
        d_act_tok = jnp.einsum('bsc,js->bcj', d_after_bf, w_tok2, preferred_element_type=jnp.float32)
        d_hid_tok = d_act_tok.astype(jnp.bfloat16).astype(jnp.float32) * slope_tok
        d_hid_tok_bf = d_hid_tok.astype(jnp.bfloat16)
        g_b_tok1 = jnp.sum(d_hid_tok, axis=(0, 1))
    g_w_tok1 = scoped(tag + '_gt1', 'bsc,bcj->sj', normed, d_hid_tok_bf, preferred_element_type=jnp.float32)
    d_normed = scoped(tag + '_dnt', 'bcj,sj->bsc', d_hid_tok_bf, w_tok1, preferred_element_type=jnp.float32)
    d_in_ln, g_ln1_g, g_ln1_b = norm_grad(x_in, ln1_g, ln1_b, d_normed)
    d_in = d_in_ln + d_after
    vectors = jnp.concatenate([g_ln1_g, g_ln1_b, g_b_tok1, g_b_tok2[:num_tokens], g_ln2_g, g_ln2_b, g_b_ch1, g_b_ch2])
    last_row = row1 + mat_tiles[2] + mat_tiles[3]
    vectors = jnp.pad(vectors, (0, flat_len - last_row * LANES - vectors.shape[0])).reshape(-1, LANES)
    tok_rows = jnp.concatenate([g_w_tok1[:num_tokens].reshape(-1, LANES), g_w_tok2[:, :num_tokens].reshape(-1, LANES)], axis=0)
    flat_grad = lax.dynamic_update_slice(flat_grad, tok_rows, (0, 0))
    flat_grad = lax.dynamic_update_slice(flat_grad, vectors, (last_row, 0))
    return d_in, flat_grad


def head_step(hidden, labels, small_full, head_full, num_classes, global_b, num_tokens):
    num_chans = hidden.shape[2]
    lnf_g = small_full[:num_chans]
    lnf_b = small_full[num_chans:2 * num_chans]
    head_b = small_full[2 * num_chans:2 * num_chans + num_classes]
    normed = layer_norm(hidden, lnf_g, lnf_b)
    pooled = (jnp.sum(normed[:, :num_tokens], axis=1, dtype=jnp.float32) / num_tokens).astype(jnp.bfloat16)
    is_class = jnp.arange(HEAD_PAD)[None, :] < num_classes
    logits = jnp.dot(pooled, head_full, preferred_element_type=jnp.float32) + jnp.pad(head_b.astype(jnp.float32), (0, HEAD_PAD - num_classes))
    logits = jnp.where(is_class, logits, -jnp.inf)
    log_norm = jax.nn.logsumexp(logits, axis=-1)
    is_label = jnp.arange(HEAD_PAD)[None, :] == labels[:, None]
    picked = jnp.sum(jnp.where(is_label, logits, 0.0), axis=-1)
    loss_sum = jnp.sum(log_norm - picked)
    d_logits = (jnp.exp(logits - log_norm[:, None]) - is_label.astype(jnp.float32)) / global_b
    d_logits_bf = d_logits.astype(jnp.bfloat16)
    g_head_b = jnp.sum(d_logits, axis=0)[:num_classes]
    g_head_w = jnp.einsum('bc,bk->ck', pooled, d_logits_bf, preferred_element_type=jnp.float32)
    d_pooled = jnp.einsum('bk,ck->bc', d_logits_bf, head_full, preferred_element_type=jnp.float32)
    is_token = jnp.arange(hidden.shape[1])[None, :, None] < num_tokens
    d_normed = jnp.where(is_token, (d_pooled / num_tokens)[:, None, :], 0.0)
    d_hidden, g_lnf_g, g_lnf_b = norm_grad(hidden, lnf_g, lnf_b, d_normed)
    g_small = jnp.concatenate([g_lnf_g, g_lnf_b, g_head_b])
    return loss_sum, d_hidden, g_head_w, g_small


def adam_update(master, gradient, moment, second, decay_rate):
    moment_new = BETA_ONE * moment + (1.0 - BETA_ONE) * gradient
    second_new = BETA_TWO * second + (1.0 - BETA_TWO) * gradient * gradient
    m_hat = moment_new / (1.0 - BETA_ONE ** ADAM_STEP)
    v_hat = second_new / (1.0 - BETA_TWO ** ADAM_STEP)
    master_new = master - LEARN_RATE * (m_hat / (jnp.sqrt(v_hat) + ADAM_EPS) + decay_rate * master)
    return master_new, moment_new, second_new


def solution(mesh):
    row_spec = P(AXIS)
    layer_spec = P(None, AXIS)
    in_specs = (row_spec, row_spec, layer_spec, row_spec, row_spec, layer_spec, row_spec, row_spec, layer_spec, row_spec, row_spec)
    out_specs = (P(),) + in_specs[2:]

    def device_step(act_in, labels, layer_p, head_w, small_p, layer_m, head_m, small_m, layer_v, head_v, small_v):
        local_b, num_tokens, num_chans = act_in.shape
        global_b = local_b * GROUP
        num_layers, share_len = layer_p.shape
        flat_len = share_len * GROUP
        head_rows, num_classes = head_w.shape
        small_len = small_p.shape[0]
        mat_len = 2 * num_tokens * (num_chans // 2) + 8 * num_chans * num_chans

        windows = [share_to_window(layer_p[layer_idx].astype(jnp.bfloat16)) for layer_idx in range(num_layers)]
        win_tiles = windows[0].shape[0]
        head_tiles = head_to_tiles(head_w.astype(jnp.bfloat16))
        small_tile = jnp.pad(small_p.astype(jnp.bfloat16).reshape(1, 1, small_len), ((0, 0), (0, ROWS - 1), (0, 0)))
        num_head = head_tiles.shape[0]
        flat0, flat1, extra = gather_shares(windows[0], windows[1], jnp.concatenate([head_tiles, small_tile], axis=0))

        weights = []
        caches = []
        hidden = pad_tokens(act_in, 1, num_tokens)
        for layer_idx, flat in enumerate((flat0, flat1)):
            weights.append(unpack_tiles(flat.reshape(-1, ROWS, LANES), num_tokens, num_chans))
            hidden, cache = layer_forward(hidden, weights[layer_idx], f'f{layer_idx}')
            caches.append(cache)
        head_full = tiles_to_head(extra[:, :num_head], head_rows * GROUP)
        small_full = extra[:, num_head, 0].reshape(-1)
        loss_sum, d_hidden, g_head_w, g_small = head_step(hidden, labels, small_full, head_full, num_classes, global_b, num_tokens)

        head_blocks = head_to_tiles(g_head_w).reshape(GROUP, num_head, ROWS, LANES)
        g_small = jnp.pad(g_small, (0, small_len * GROUP - g_small.shape[0])).reshape(GROUP, 1, 1, small_len)
        small_blocks = jnp.pad(g_small, ((0, 0), (0, 0), (0, ROWS - 1), (0, 0)))
        packed = [None] * num_layers
        for layer_idx in reversed(range(num_layers)):
            d_hidden, flat_grad = layer_backward(d_hidden, weights[layer_idx], caches[layer_idx], f'b{layer_idx}', flat_len, num_tokens)
            packed[layer_idx] = flat_grad.reshape(flat0.shape)
        loss_tile = jnp.pad(loss_sum.reshape(1, 1), ((0, ROWS - 1), (0, LANES - 1)))
        extra_blocks = jnp.concatenate([head_blocks, small_blocks], axis=1)
        summed0, summed1, sums = scatter_grads(packed[0], packed[1], extra_blocks, loss_tile, win_tiles, share_len // LANES)
        layer_g = jnp.stack([window_to_share(summed0, share_len), window_to_share(summed1[:win_tiles], share_len)])
        head_g = tiles_to_head(summed1[win_tiles:win_tiles + num_head], head_rows)[:, :num_classes]
        small_g = summed1[win_tiles + num_head, 0]

        sq_total, loss_total = jnp.sum(sums[0]), jnp.sum(sums[1])
        loss_value = loss_total / global_b
        clip_scale = 1.0 / jnp.maximum(1.0, jnp.sqrt(sq_total))
        flat_pos = lax.axis_index(AXIS) * share_len + jnp.arange(share_len)
        layer_decay = jnp.where(flat_pos < mat_len, WEIGHT_DECAY, 0.0)[None, :]
        new_lp, new_lm, new_lv = adam_update(layer_p, layer_g * clip_scale, layer_m, layer_v, layer_decay)
        new_hw, new_hm, new_hv = adam_update(head_w, head_g * clip_scale, head_m, head_v, WEIGHT_DECAY)
        new_sp, new_sm, new_sv = adam_update(small_p, small_g * clip_scale, small_m, small_v, 0.0)
        return (loss_value, new_lp, new_hw, new_sp, new_lm, new_hm, new_sm, new_lv, new_hv, new_sv)

    return jax.shard_map(device_step, mesh=mesh, in_specs=in_specs, out_specs=out_specs, check_vma=False)
```
